8 devices in a mesh: tp: 4 (over z, y, x), cp: 2 (over core).
Axes of the slice: x: 2, y: 2, z: 1, core: 2. Of those that a mesh axis runs over, the one named last changes fastest.
Arguments:
- x_in: bfloat16 [32, 256, 4096], P(None, 'cp')
- grad_z: bfloat16 [32, 256, 4096], P(None, 'cp')
- seg_pos: int32 [32, 256], P(None, 'cp')
- norm_scale: bfloat16 [4096], replicated
- w_x: bfloat16 [4096, 4096], P(None, 'tp')
- b_x: bfloat16 [4096], P('tp')
- w_y: bfloat16 [4096, 4096], P(None, 'tp')
- b_y: bfloat16 [4096], P('tp')
- conv_w: bfloat16 [4, 4096], P(None, 'tp')
- conv_b: bfloat16 [4096], P('tp')
- w_a: bfloat16 [32, 128, 128], P('tp')
- b_a: bfloat16 [4096], P('tp')
- w_i: bfloat16 [32, 128, 128], P('tp')
- b_i: bfloat16 [4096], P('tp')
- a_param: float32 [4096], P('tp')
- w_out: bfloat16 [4096, 4096], P('tp')
- b_out: bfloat16 [4096], replicated
Outputs:
- output 1: bfloat16 [32, 256, 4096], P(None, 'cp')
- output 2: bfloat16 [32, 256, 4096], P(None, 'cp')
- output 3: float32 [4096], replicated
- output 4: float32 [4096, 4096], P(None, 'tp')
- output 5: float32 [4096], P('tp')
- output 6: float32 [4096, 4096], P(None, 'tp')
- output 7: float32 [4096], P('tp')
- output 8: float32 [4, 4096], P(None, 'tp')
- output 9: float32 [4096], P('tp')
- output 10: float32 [32, 128, 128], P('tp')
- output 11: float32 [4096], P('tp')
- output 12: float32 [32, 128, 128], P('tp')
- output 13: float32 [4096], P('tp')
- output 14: float32 [4096], P('tp')
- output 15: float32 [4096, 4096], P('tp')
- output 16: float32 [4096], replicated
All inputs are finite; a program needn't handle non-finite values.
Results may differ from the reference program's by a relative error of at most 0.00859572.
Values sent between devices are 32-bit elements.
A program may use at most 1 GiB of HBM per device.

```python
import math
import jax
import jax.numpy as jnp
from jax import lax

BATCH_SEQS = 32
SEQ_LEN = 256
D_MODEL = 4096
D_RNN = 4096
GATE_BLOCKS = 32
DOC_STARTS = 2
CONV_WIDTH = 4
BLOCK_WIDTH = D_RNN // GATE_BLOCKS
NORM_EPS = 1e-6


def doc_positions(pos_key):
    starts = jax.random.randint(pos_key, (BATCH_SEQS, DOC_STARTS), 1, SEQ_LEN)
    step_ids = jnp.arange(SEQ_LEN, dtype=jnp.int32)
    is_start = jnp.any(step_ids[None, :, None] == starts[:, None, :], axis=-1) | (step_ids == 0)[None, :]
    last_start = lax.cummax(jnp.where(is_start, step_ids[None, :], 0), axis=1)
    return (step_ids[None, :] - last_start).astype(jnp.int32)


def setup_inputs(seed: int = 0) -> dict:
    key_list = jax.random.split(jax.random.key(seed), 17)

    def draw_normal(key_index, arr_shape, factor):
        return jax.random.normal(key_list[key_index], arr_shape, jnp.float32) * factor

    tok_shape = (BATCH_SEQS, SEQ_LEN, D_MODEL)
    gate_shape = (GATE_BLOCKS, BLOCK_WIDTH, BLOCK_WIDTH)
    soft_plus = jnp.exp(jax.random.uniform(key_list[14], (D_RNN,), jnp.float32, math.log(2e-5), math.log(2e-4)))
    return {
        "x_in": draw_normal(0, tok_shape, 1.0).astype(jnp.bfloat16),
        "grad_z": draw_normal(1, tok_shape, 1.0).astype(jnp.bfloat16),
        "seg_pos": doc_positions(key_list[2]),
        "norm_scale": draw_normal(3, (D_MODEL,), 0.3).astype(jnp.bfloat16),
        "w_x": draw_normal(4, (D_MODEL, D_RNN), D_MODEL ** -0.5).astype(jnp.bfloat16),
        "b_x": draw_normal(5, (D_RNN,), 0.3).astype(jnp.bfloat16),
        "w_y": draw_normal(6, (D_MODEL, D_RNN), D_MODEL ** -0.5).astype(jnp.bfloat16),
        "b_y": draw_normal(7, (D_RNN,), 0.3).astype(jnp.bfloat16),
        "conv_w": draw_normal(8, (CONV_WIDTH, D_RNN), 0.5).astype(jnp.bfloat16),
        "conv_b": draw_normal(9, (D_RNN,), 0.3).astype(jnp.bfloat16),
        "w_a": draw_normal(10, gate_shape, BLOCK_WIDTH ** -0.5).astype(jnp.bfloat16),
        "b_a": draw_normal(11, (D_RNN,), 0.5).astype(jnp.bfloat16),
        "w_i": draw_normal(12, gate_shape, BLOCK_WIDTH ** -0.5).astype(jnp.bfloat16),
        "b_i": draw_normal(13, (D_RNN,), 0.5).astype(jnp.bfloat16),
        "a_param": jnp.log(jnp.expm1(soft_plus)),
        "w_out": draw_normal(15, (D_RNN, D_MODEL), D_RNN ** -0.5).astype(jnp.bfloat16),
        "b_out": draw_normal(16, (D_MODEL,), 0.3).astype(jnp.bfloat16),
    }


def to_bf16(arr_val):
    return arr_val + lax.stop_gradient(arr_val.astype(jnp.bfloat16).astype(jnp.float32) - arr_val)


def block_forward(x_f, norm_scale, w_x, b_x, w_y, b_y, conv_w, conv_b, w_a, b_a, w_i, b_i, a_param, w_out, b_out, seg_pos):
    mean_sq = jnp.mean(x_f * x_f, axis=-1, keepdims=True)
    normed = to_bf16(x_f * lax.rsqrt(mean_sq + NORM_EPS) * (1.0 + norm_scale))
    y_act = jax.nn.gelu(jnp.dot(normed, w_y, preferred_element_type=jnp.float32) + b_y, approximate=True)
    x_branch = to_bf16(jnp.dot(normed, w_x, preferred_element_type=jnp.float32) + b_x)
    batch_n, seq_n, width_n = x_branch.shape
    conv_sum = x_branch * conv_w[0] + conv_b
    for tap_k in range(1, CONV_WIDTH):
        shifted = jnp.pad(x_branch[:, :seq_n - tap_k], ((0, 0), (tap_k, 0), (0, 0)))
        keep_mask = (seg_pos >= tap_k)[:, :, None]
        conv_sum = conv_sum + jnp.where(keep_mask, shifted, 0.0) * conv_w[tap_k]
    conv_out = to_bf16(conv_sum)
    blocks = conv_out.reshape(batch_n, seq_n, GATE_BLOCKS, BLOCK_WIDTH)
    pre_a = jnp.einsum("bthk,hkj->bthj", blocks, w_a).reshape(batch_n, seq_n, width_n) + b_a
    pre_i = jnp.einsum("bthk,hkj->bthj", blocks, w_i).reshape(batch_n, seq_n, width_n) + b_i
    reset_mask = (seg_pos == 0)[:, :, None]
    log_a = -8.0 * jax.nn.sigmoid(pre_a) * jax.nn.softplus(a_param)
    decays = jnp.where(reset_mask, 0.0, jnp.exp(log_a))
    multiplier = jnp.where(reset_mask, 1.0, jnp.sqrt(-jnp.expm1(2.0 * log_a)))
    drives = multiplier * jax.nn.sigmoid(pre_i) * conv_out

    def scan_step(carry_h, inputs_t):
        next_h = inputs_t[0] * carry_h + inputs_t[1]
        return next_h, next_h

    init_h = jnp.zeros((batch_n, width_n), jnp.float32)
    _, hidden_t = lax.scan(scan_step, init_h, (jnp.swapaxes(decays, 0, 1), jnp.swapaxes(drives, 0, 1)))
    hidden = jnp.swapaxes(hidden_t, 0, 1)
    mixed_v = to_bf16(hidden * y_act)
    out_proj = jnp.dot(mixed_v, w_out, preferred_element_type=jnp.float32) + b_out
    return to_bf16(x_f + out_proj)


def reference(x_in, grad_z, seg_pos, norm_scale, w_x, b_x, w_y, b_y, conv_w, conv_b, w_a, b_a, w_i, b_i, a_param, w_out, b_out):
    primals = [param_arr.astype(jnp.float32) for param_arr in (x_in, norm_scale, w_x, b_x, w_y, b_y, conv_w, conv_b, w_a, b_a, w_i, b_i, a_param, w_out, b_out)]

    def run_block(*params):
        return block_forward(*params, seg_pos)

    z_val, pull_back = jax.vjp(run_block, *primals)
    grad_list = pull_back(grad_z.astype(jnp.float32))
    return (z_val.astype(jnp.bfloat16), grad_list[0].astype(jnp.bfloat16), grad_list[1], grad_list[2], grad_list[3], grad_list[4], grad_list[5], grad_list[6], grad_list[7], grad_list[8], grad_list[9], grad_list[10], grad_list[11], grad_list[12], grad_list[13], grad_list[14])
```

```python
import functools
import jax
import jax.numpy as jnp
from jax import lax
from jax.experimental import pallas as pl
from jax.experimental.pallas import tpu as pltpu
from jax.sharding import PartitionSpec as P

F32 = jnp.float32
BF16 = jnp.bfloat16
TAPS = 4
SUB = 8
LANES = 128
SLOTS = 3
MSG_SLOTS = 4
GELU_K0 = 0.7978845608028654
GELU_K1 = 0.7978845608028654 * 0.044715
N_SUMS = 9


def middle_kernel(n_steps, n_tiles, n_tok, grads, pos_f, pos_b, par_f, par_b, wg_f, wg_b, px, py, dm, *rest):
    if grads:
        mix_o, dpy_o, dbr_o, gw_o, sy_o, sb_o = rest[:6]
        rest = rest[6:]
    else:
        mix_o, dpy_o, dbr_o = rest[:3]
        rest = rest[3:]
    (s_g, s_a, s_h, s_k, s_ra, s_ui, s_mi, s_c16, s_r, s_xb, in_x, in_y, in_d, pre_a, pre_i, out_m, out_y, out_b, d_c, d_16, d_gate, xb_w, send, recv, send_sem, recv_sem) = rest
    pitch = n_tok + SUB
    me = lax.axis_index("cp")
    step = pl.program_id(0)
    f_step = step - me
    b_step = step - 2 + me
    f_on = jnp.logical_and(f_step >= 0, f_step < n_steps)
    b_on = jnp.logical_and(b_step >= 0, b_step < n_steps)
    f_slot = lax.rem(f_step + SLOTS, SLOTS)
    b_slot = lax.rem(b_step + SLOTS, SLOTS)
    f_msg = lax.rem(f_step + MSG_SLOTS, MSG_SLOTS)
    b_msg = lax.rem(b_step + MSG_SLOTS, MSG_SLOTS)
    n_groups = n_tok // SUB

    def message(slot):
        return pltpu.make_async_remote_copy(src_ref=send.at[slot], dst_ref=recv.at[slot], send_sem=send_sem.at[slot], recv_sem=recv_sem.at[slot], device_id={"cp": 1 - me}, device_id_type=pl.DeviceIdType.MESH)

    @pl.when(step == 0)
    def _():
        barrier = pltpu.get_barrier_semaphore()
        pl.semaphore_signal(barrier, inc=1, device_id={"cp": 1 - me}, device_id_type=pl.DeviceIdType.MESH)
        pl.semaphore_wait(barrier, 1)

    def row8(base):
        return pl.ds(pl.multiple_of(base, SUB), SUB)

    def strided(t):
        return pl.ds(t, SUB, stride=pitch)

    @pl.when(jnp.logical_and(f_on, me == 1))
    def _():
        message(f_msg).wait_recv()

    @pl.when(f_on)
    def _():
        for seq in range(SUB):
            for src, dst in ((px, in_x), (py, in_y), (dm, in_d)):
                dst[pl.ds(seq * pitch, n_tok), :] = src[pl.ds(seq * n_tok, n_tok), :]
        b_x = jnp.broadcast_to(par_f[0:1, :], (SUB, LANES))
        b_y = jnp.broadcast_to(par_f[1:2, :], (SUB, LANES))
        taps = [jnp.broadcast_to(par_f[2 + k:3 + k, :], (SUB, LANES)) for k in range(TAPS)]
        c_b = jnp.broadcast_to(par_f[6:7, :], (SUB, LANES))
        b_a = jnp.broadcast_to(par_f[7:8, :], (SUB, LANES))
        b_i = jnp.broadcast_to(par_f[8:9, :], (SUB, LANES))
        nsp = jnp.broadcast_to(par_f[9:10, :], (SUB, LANES))
        first = (me == 0)
        in_msg = recv.at[f_msg]
        halo = [jnp.where(first, 0.0, in_msg[pl.ds(SUB * (1 + j), SUB), :]) for j in range(3)]
        h_in = jnp.where(first, 0.0, in_msg[pl.ds(0, SUB), :])
        xb_r = s_xb.at[f_slot] if grads else xb_w
        if grads:
            for j in range(3):
                xb_r[pl.ds(SUB * j, SUB), :] = halo[j]
        c16_r, g_r, a_r, h_r, k_r = s_c16.at[f_slot], s_g.at[f_slot], s_a.at[f_slot], s_h.at[f_slot], s_k.at[f_slot]
        ra_r, ui_r, mi_r = s_ra.at[f_slot], s_ui.at[f_slot], s_mi.at[f_slot]
        r_r = s_r.at[f_slot] if grads else None

        def conv_body(grp, carry):
            xm3, xm2, xm1 = carry
            pend = None
            for j in range(SUB):
                t = grp * SUB + j
                x0 = (in_x[strided(t), :] + b_x).astype(BF16).astype(F32)
                pos = pos_f[row8(t * SUB), :]
                acc = c_b + x0 * taps[0]
                acc = acc + jnp.where(pos >= 1, xm1, 0.0) * taps[1]
                acc = acc + jnp.where(pos >= 2, xm2, 0.0) * taps[2]
                acc = acc + jnp.where(pos >= 3, xm3, 0.0) * taps[3]
                if grads:
                    xb_r[row8(t * SUB + 3 * SUB), :] = x0
                if pend is None:
                    pend = acc
                else:
                    both = jnp.concatenate([pend, acc], axis=0).astype(BF16)
                    c16_r[pl.ds(pl.multiple_of((t - 1) * SUB, 2 * SUB), 2 * SUB), :] = both
                    pend = None
                xm3, xm2, xm1 = xm2, xm1, x0
            return xm3, xm2, xm1

        last3 = lax.fori_loop(0, n_groups, conv_body, tuple(halo))
        pre = jnp.dot(c16_r[...], wg_f[...], preferred_element_type=F32)
        pre_a[...] = pre[:, :LANES]
        pre_i[...] = pre[:, LANES:]
        h_r[pl.ds(0, SUB), :] = h_in

        def gate_body(grp, carry):
            h, sum_y = carry
            for j in range(SUB):
                t = grp * SUB + j
                rows = row8(t * SUB)
                if j % 2 == 0:
                    c2 = c16_r[pl.ds(pl.multiple_of(t * SUB, 2 * SUB), 2 * SUB), :].astype(F32)
                c = c2[:SUB] if j % 2 == 0 else c2[SUB:]
                reset = pos_f[rows, :] == 0
                r = jax.nn.sigmoid(pre_a[rows, :] + b_a)
                i = jax.nn.sigmoid(pre_i[rows, :] + b_i)
                la = nsp * r
                a = jnp.exp(la)
                y2 = la + la
                poly = -y2 * (1.0 + y2 * (0.5 + y2 * (1.0 / 6.0 + y2 * (1.0 / 24.0))))
                q = jnp.maximum(jnp.where(y2 > -0.0625, poly, 1.0 - a * a), 1e-37)
                rm = lax.rsqrt(q)
                m = jnp.where(reset, 1.0, q * rm)
                ic = i * c
                k = a * ic * rm
                a = jnp.where(reset, 0.0, a)
                u = m * ic
                h = a * h + u
                h_r[row8(t * SUB + SUB), :] = h
                a_r[rows, :] = a
                k_r[rows, :] = k
                ra_r[rows, :] = la - la * r
                ui_r[rows, :] = u - u * i
                mi_r[rows, :] = m * i
                if grads:
                    r_r[rows, :] = r
                v = in_y[strided(t), :] + b_y
                v2 = v * v
                th = jnp.tanh(v * (GELU_K0 + GELU_K1 * v2))
                hv = 0.5 * v
                y = hv + hv * th
                dy = (0.5 + 0.5 * th) + hv * (1.0 - th * th) * (GELU_K0 + (3.0 * GELU_K1) * v2)
                d = in_d[strided(t), :]
                g_r[rows, :] = d * y
                out_m[strided(t), :] = h * y
                d_py = d * h * dy
                out_y[strided(t), :] = d_py
                if grads:
                    sum_y = sum_y + d_py
            return h, sum_y

        h_end, sum_y = lax.fori_loop(0, n_groups, gate_body, (h_in, jnp.zeros((SUB, LANES), F32)))
        if grads:
            @pl.when(lax.rem(f_step, n_tiles) == 0)
            def _():
                sy_o[...] = jnp.zeros_like(sy_o)
            sy_o[...] += sum_y

        @pl.when(me == 0)
        def _():
            out_msg = send.at[f_msg]
            out_msg[pl.ds(0, SUB), :] = h_end
            for j in range(3):
                out_msg[pl.ds(SUB * (1 + j), SUB), :] = last3[j]
        for seq in range(SUB):
            mix_o[pl.ds(seq * n_tok, n_tok), :] = out_m[pl.ds(seq * pitch, n_tok), :].astype(BF16)
            dpy_o[pl.ds(seq * n_tok, n_tok), :] = out_y[pl.ds(seq * pitch, n_tok), :].astype(BF16)

        @pl.when(me == 0)
        def _():
            message(f_msg).start()

    @pl.when(jnp.logical_and(b_on, me == 0))
    def _():
        message(b_msg).wait_recv()

    @pl.when(jnp.logical_and(jnp.logical_and(b_step >= 1, b_step <= n_steps), me == 1))
    def _():
        message(lax.rem(b_step - 1 + MSG_SLOTS, MSG_SLOTS)).wait_send()

    @pl.when(b_on)
    def _():
        taps = [jnp.broadcast_to(par_b[2 + k:3 + k, :], (SUB, LANES)) for k in range(TAPS)]
        last = (me == 1)
        in_msg = recv.at[b_msg]
        carry_in = jnp.where(last, 0.0, in_msg[pl.ds(0, SUB), :])
        tail = [jnp.where(last, 0.0, in_msg[pl.ds(SUB * (1 + j), SUB), :]) for j in range(3)]
        g_r, a_r, h_r, k_r = s_g.at[b_slot], s_a.at[b_slot], s_h.at[b_slot], s_k.at[b_slot]
        ra_r, ui_r, mi_r = s_ra.at[b_slot], s_ui.at[b_slot], s_mi.at[b_slot]
        r_r = s_r.at[b_slot] if grads else None
        xb_r = s_xb.at[b_slot] if grads else None
        zero = jnp.zeros((SUB, LANES), F32)

        def scan_body(back, carry):
            grp = n_groups - 1 - back
            adh, sum_a, sum_i, sum_p = carry
            pend = None
            for j in reversed(range(SUB)):
                t = grp * SUB + j
                rows = row8(t * SUB)
                dh = g_r[rows, :] + adh
                adh = a_r[rows, :] * dh
                dlog = adh * (h_r[rows, :] - k_r[rows, :])
                dpa = dlog * ra_r[rows, :]
                dpi = dh * ui_r[rows, :]
                d_c[rows, :] = dh * mi_r[rows, :]
                if grads:
                    sum_a = sum_a + dpa
                    sum_i = sum_i + dpi
                    sum_p = sum_p + dlog * r_r[rows, :]
                if pend is None:
                    pend = (dpa, dpi)
                else:
                    pair = pl.ds(pl.multiple_of(t * SUB, 2 * SUB), 2 * SUB)
                    d_16[pair, :LANES] = jnp.concatenate([dpa, pend[0]], axis=0).astype(BF16)
                    d_16[pair, LANES:] = jnp.concatenate([dpi, pend[1]], axis=0).astype(BF16)
                    pend = None
            return adh, sum_a, sum_i, sum_p

        adh, sum_a, sum_i, sum_p = lax.fori_loop(0, n_groups, scan_body, (carry_in, zero, zero, zero))
        d_gate[...] = lax.dot_general(d_16[...], wg_b[...], (((1,), (1,)), ((), ())), preferred_element_type=F32)

        def conv_body(grp, carry):
            e3, e2, e1 = carry[:3]
            sums = list(carry[3:])
            for j in range(SUB):
                s = grp * SUB + j
                rows = row8(s * SUB)
                pos = pos_b[rows, :]
                dc = d_c[rows, :] + d_gate[rows, :]
                m1 = jnp.where(pos >= 1, dc, 0.0)
                m2 = jnp.where(pos >= 2, dc, 0.0)
                m3 = jnp.where(pos >= 3, dc, 0.0)
                done = e3 + m3 * taps[3]
                out_b[strided(s + SUB - 3), :] = done
                e3, e2, e1 = e2 + m2 * taps[2], e1 + m1 * taps[1], dc * taps[0]
                if grads:
                    sums[0] = sums[0] + dc * xb_r[row8(s * SUB + 3 * SUB), :]
                    sums[1] = sums[1] + m1 * xb_r[row8(s * SUB + 2 * SUB), :]
                    sums[2] = sums[2] + m2 * xb_r[row8(s * SUB + SUB), :]
                    sums[3] = sums[3] + m3 * xb_r[row8(s * SUB), :]
                    sums[4] = sums[4] + dc
                    sums[5] = sums[5] + done
            return (e3, e2, e1) + tuple(sums)

        res = lax.fori_loop(0, n_groups, conv_body, (zero, zero, zero) + (zero,) * (6 if grads else 0))
        ends = [res[j] + tail[j] for j in range(3)]
        for j in range(3):
            out_b[strided(n_tok + SUB - 3 + j), :] = ends[j]
        heads = [out_b[strided(SUB - 3 + j), :] for j in range(3)]

        @pl.when(me == 1)
        def _():
            out_msg = send.at[b_msg]
            out_msg[pl.ds(0, SUB), :] = adh
            for j in range(3):
                out_msg[pl.ds(SUB * (1 + j), SUB), :] = heads[j]

        for seq in range(SUB):
            dbr_o[pl.ds(seq * n_tok, n_tok), :] = out_b[pl.ds(seq * pitch + SUB, n_tok), :].astype(BF16)
        if grads:
            sums = list(res[3:])
            sum_x = sums[5] + ends[0] + ends[1] + ends[2] - heads[0] - heads[1] - heads[2]

            @pl.when(lax.rem(b_step, n_tiles) == 0)
            def _():
                gw_o[...] = jnp.zeros_like(gw_o)
                sb_o[...] = jnp.zeros_like(sb_o)
            for n, val in enumerate((sum_x, sums[0], sums[1], sums[2], sums[3], sums[4], sum_a, sum_i, sum_p)):
                sb_o[0, pl.ds(n * SUB, SUB), :] += val
            gw_o[0] += lax.dot_general(s_c16[b_slot], d_16[...], (((0,), (0,)), ((), ())), preferred_element_type=F32)

        @pl.when(me == 1)
        def _():
            message(b_msg).start()

    @pl.when(jnp.logical_and(f_on, me == 0))
    def _():
        message(f_msg).wait_send()


def middle(px, py, dm, pos_rep, par, w_gate, grads, collective_id):
    n_rows, width = px.shape
    n_tok = pos_rep.shape[1] // SUB
    tile = SUB * n_tok
    n_tiles, n_chunks = n_rows // tile, width // LANES
    n_steps = n_tiles * n_chunks

    def f_of(s):
        return jnp.clip(s - lax.axis_index("cp"), 0, n_steps - 1)

    def b_of(s):
        return jnp.clip(s - 2 + lax.axis_index("cp"), 0, n_steps - 1)

    def spec(shape, of, index):
        def index_map(s):
            k = of(s)
            return index(k // n_tiles, k % n_tiles)
        return pl.BlockSpec(shape, index_map)

    big = lambda of: spec((tile, LANES), of, lambda c, t: (t, c))
    in_specs = [
        spec((None, tile, LANES), f_of, lambda c, t: (t, 0, 0)), spec((None, tile, LANES), b_of, lambda c, t: (t, 0, 0)),
        spec((16, LANES), f_of, lambda c, t: (0, c)), spec((16, LANES), b_of, lambda c, t: (0, c)),
        spec((None, LANES, 2 * LANES), f_of, lambda c, t: (c, 0, 0)), spec((None, LANES, 2 * LANES), b_of, lambda c, t: (c, 0, 0)),
        big(f_of), big(f_of), big(f_of)]
    out_specs = [big(f_of), big(f_of), big(b_of)]
    out_shape = [jax.ShapeDtypeStruct((n_rows, width), BF16)] * 3
    if grads:
        out_specs += [spec((1, LANES, 2 * LANES), b_of, lambda c, t: (c, 0, 0)), spec((1, SUB, LANES), f_of, lambda c, t: (c, 0, 0)), spec((1, N_SUMS * SUB, LANES), b_of, lambda c, t: (c, 0, 0))]
        out_shape += [jax.ShapeDtypeStruct((n_chunks, LANES, 2 * LANES), F32), jax.ShapeDtypeStruct((n_chunks, SUB, LANES), F32), jax.ShapeDtypeStruct((n_chunks, N_SUMS * SUB, LANES), F32)]
    pitched = pltpu.VMEM((SUB * (n_tok + SUB), LANES), F32)
    flat = pltpu.VMEM((tile, LANES), F32)
    slots = pltpu.VMEM((SLOTS, tile, LANES), F32)
    small = pltpu.VMEM((SLOTS if grads else 1, tile if grads else SUB, LANES), F32)
    scratch = [
        slots, slots, pltpu.VMEM((SLOTS, tile + SUB, LANES), F32), slots, slots, slots, slots, pltpu.VMEM((SLOTS, tile, LANES), BF16), small,
        pltpu.VMEM((SLOTS if grads else 1, tile + 3 * SUB if grads else SUB, LANES), F32),
        pitched, pitched, pitched, flat, flat, pitched, pitched, pltpu.VMEM((SUB * (n_tok + SUB) + SUB, LANES), F32), flat, pltpu.VMEM((tile, 2 * LANES), BF16), flat,
        pltpu.VMEM((SUB, LANES), F32),
        pltpu.VMEM((MSG_SLOTS, 4 * SUB, LANES), F32), pltpu.VMEM((MSG_SLOTS, 4 * SUB, LANES), F32), pltpu.SemaphoreType.DMA((MSG_SLOTS,)), pltpu.SemaphoreType.DMA((MSG_SLOTS,))]
    return pl.pallas_call(
        functools.partial(middle_kernel, n_steps, n_tiles, n_tok, grads),
        grid=(n_steps + 2,), in_specs=in_specs, out_specs=out_specs, out_shape=out_shape, scratch_shapes=scratch,
        name="middle",
        cost_estimate=pl.CostEstimate(flops=n_rows * width * 1500, bytes_accessed=n_rows * width * 18, transcendentals=n_rows * width * 8),
        compiler_params=pltpu.CompilerParams(collective_id=collective_id, has_side_effects=True, vmem_limit_bytes=60 * 1024 * 1024, dimension_semantics=("arbitrary",)),
    )(pos_rep, pos_rep, par, par, w_gate, w_gate, px, py, dm)


NORM_EPS = 1e-6
IN_SPECS = (P(None, "cp", None), P(None, "cp", None), P(None, "cp"), P(), P(None, "tp"), P("tp"), P(None, "tp"), P("tp"), P(None, "tp"), P("tp"), P("tp", None, None), P("tp"), P("tp", None, None), P("tp"), P("tp"), P("tp", None), P())
OUT_SPECS = (P(None, "cp", None), P(None, "cp", None), P(), P(None, "tp"), P("tp"), P(None, "tp"), P("tp"), P(None, "tp"), P("tp"), P("tp", None, None), P("tp"), P("tp", None, None), P("tp"), P("tp"), P("tp", None), P())


def norm_apply(x_f, scale_f):
    mean_sq = jnp.mean(x_f * x_f, axis=-1, keepdims=True)
    return x_f * lax.rsqrt(mean_sq + NORM_EPS) * (1.0 + scale_f)


def spread_positions(seg_pos):
    n_seq, n_tok = seg_pos.shape
    pos = jnp.swapaxes(seg_pos.reshape(n_seq // SUB, SUB, n_tok), 1, 2).reshape(n_seq // SUB, n_tok * SUB, 1)
    return jnp.broadcast_to(pos, (n_seq // SUB, n_tok * SUB, LANES))


def stack_params(b_x, b_y, conv_w, conv_b, b_a, b_i, a_param):
    rows = [b_x, b_y, conv_w[0], conv_w[1], conv_w[2], conv_w[3], conv_b, b_a, b_i]
    rows = [row.astype(F32) for row in rows] + [-8.0 * jax.nn.softplus(a_param)]
    return jnp.concatenate([jnp.stack(rows), jnp.zeros((16 - len(rows), a_param.shape[0]), F32)], axis=0)


def shard_body(x_in, grad_z, seg_pos, norm_scale, w_x, b_x, w_y, b_y, conv_w, conv_b, w_a, b_a, w_i, b_i, a_param, w_out, b_out):
    n_seq, n_tok, d_model = x_in.shape
    x_f = x_in.reshape(n_seq * n_tok, d_model).astype(F32)
    gz = grad_z.reshape(n_seq * n_tok, d_model)
    normed_f, norm_pull = jax.vjp(norm_apply, x_f, norm_scale.astype(F32))
    normed = normed_f.astype(BF16)
    px = jnp.dot(normed, w_x, preferred_element_type=F32)
    py = jnp.dot(normed, w_y, preferred_element_type=F32)
    dm = lax.dot_general(gz, w_out, (((1,), (1,)), ((), ())), preferred_element_type=F32)
    par = stack_params(b_x, b_y, conv_w, conv_b, b_a, b_i, a_param)
    w_gate = jnp.concatenate([w_a, w_i], axis=2)
    mixed, dpy, dbr, g_gate, s_y, s_b = middle(px, py, dm, spread_positions(seg_pos), par, w_gate, True, 0)
    out_part = jnp.dot(mixed, w_out, preferred_element_type=F32)
    out_proj = lax.psum(out_part, "tp") + b_out
    z_out = (x_f + out_proj).astype(BF16).reshape(x_in.shape)
    tok = (((0,), (0,)), ((), ()))
    chan = (((1,), (1,)), ((), ()))
    g_w_out = lax.dot_general(mixed, gz, tok, preferred_element_type=F32)
    g_w_x = lax.dot_general(normed, dbr, tok, preferred_element_type=F32)
    g_w_y = lax.dot_general(normed, dpy, tok, preferred_element_type=F32)
    g_b_out = jnp.sum(grad_z, axis=(0, 1), dtype=F32)
    d_norm_part = lax.dot_general(dbr, w_x, chan, preferred_element_type=F32) + lax.dot_general(dpy, w_y, chan, preferred_element_type=F32)
    d_normed = lax.psum(d_norm_part, "tp")
    d_x_norm, g_scale = norm_pull(d_normed)
    grad_x = (gz.astype(F32) + d_x_norm).astype(BF16).reshape(x_in.shape)
    width = a_param.shape[0]
    s_y = jnp.sum(s_y, axis=1).reshape(width)
    s_b = jnp.sum(s_b.reshape(s_b.shape[0], N_SUMS, SUB, LANES), axis=2)
    s_b = jnp.swapaxes(s_b, 0, 1).reshape(N_SUMS, width)
    g_a = -8.0 * s_b[8] * jax.nn.sigmoid(a_param)
    blk = LANES
    sums = lax.psum((g_scale, g_w_x, s_b[0], g_w_y, s_y, s_b[1:5], s_b[5], g_gate[:, :, :blk], s_b[6], g_gate[:, :, blk:], s_b[7], g_a, g_w_out, g_b_out), "cp")
    return (z_out, grad_x) + tuple(sums)


def solution(mesh):
    return jax.shard_map(shard_body, mesh=mesh, in_specs=IN_SPECS, out_specs=OUT_SPECS, check_vma=False)
```

```python
import functools
import jax
import jax.numpy as jnp
from jax import lax
from jax.experimental import pallas as pl
from jax.experimental.pallas import tpu as pltpu
from jax.sharding import PartitionSpec as P

F32 = jnp.float32
BF16 = jnp.bfloat16
TAPS = 4
SUB = 8
LANES = 128
SLOTS = 3
MSG_SLOTS = 4
GELU_K0 = 0.7978845608028654
GELU_K1 = 0.7978845608028654 * 0.044715
N_SUMS = 9


def middle_kernel(n_steps, n_tiles, n_tok, grads, pos_f, pos_b, par_f, par_b, wg_f, wg_b, px, py, dm, *rest):
    if grads:
        mix_o, dpy_o, dbr_o, gw_o, sy_o, sb_o = rest[:6]
        rest = rest[6:]
    else:
        mix_o, dpy_o, dbr_o = rest[:3]
        rest = rest[3:]
    (s_g, s_a, s_h, s_k, s_ra, s_ui, s_mi, s_c16, s_r, s_xb, in_x, in_y, in_d, pre_a, pre_i, out_m, out_y, out_b, d_c, d_16, d_gate, xb_w, send, recv, send_sem, recv_sem) = rest
    pitch = n_tok + SUB
    me = lax.axis_index("cp")
    step = pl.program_id(0)
    f_step = step - me
    b_step = step - 2 + me
    f_on = jnp.logical_and(f_step >= 0, f_step < n_steps)
    b_on = jnp.logical_and(b_step >= 0, b_step < n_steps)
    f_slot = lax.rem(f_step + SLOTS, SLOTS)
    b_slot = lax.rem(b_step + SLOTS, SLOTS)
    f_msg = lax.rem(f_step + MSG_SLOTS, MSG_SLOTS)
    b_msg = lax.rem(b_step + MSG_SLOTS, MSG_SLOTS)
    n_groups = n_tok // SUB

    def message(slot):
        return pltpu.make_async_remote_copy(src_ref=send.at[slot], dst_ref=recv.at[slot], send_sem=send_sem.at[slot], recv_sem=recv_sem.at[slot], device_id={"cp": 1 - me}, device_id_type=pl.DeviceIdType.MESH)

    @pl.when(step == 0)
    def _():
        barrier = pltpu.get_barrier_semaphore()
        pl.semaphore_signal(barrier, inc=1, device_id={"cp": 1 - me}, device_id_type=pl.DeviceIdType.MESH)
        pl.semaphore_wait(barrier, 1)

    def row8(base):
        return pl.ds(pl.multiple_of(base, SUB), SUB)

    def strided(t):
        return pl.ds(t, SUB, stride=pitch)

    @pl.when(jnp.logical_and(f_on, me == 1))
    def _():
        message(f_msg).wait_recv()

    @pl.when(f_on)
    def _():
        for seq in range(SUB):
            for src, dst in ((px, in_x), (py, in_y), (dm, in_d)):
                dst[pl.ds(seq * pitch, n_tok), :] = src[pl.ds(seq * n_tok, n_tok), :]
        b_x = jnp.broadcast_to(par_f[0:1, :], (SUB, LANES))
        b_y = jnp.broadcast_to(par_f[1:2, :], (SUB, LANES))
        taps = [jnp.broadcast_to(par_f[2 + k:3 + k, :], (SUB, LANES)) for k in range(TAPS)]
        c_b = jnp.broadcast_to(par_f[6:7, :], (SUB, LANES))
        b_a = jnp.broadcast_to(par_f[7:8, :], (SUB, LANES))
        b_i = jnp.broadcast_to(par_f[8:9, :], (SUB, LANES))
        nsp = jnp.broadcast_to(par_f[9:10, :], (SUB, LANES))
        first = (me == 0)
        in_msg = recv.at[f_msg]
        halo = [jnp.where(first, 0.0, in_msg[pl.ds(SUB * (1 + j), SUB), :]) for j in range(3)]
        h_in = jnp.where(first, 0.0, in_msg[pl.ds(0, SUB), :])
        xb_r = s_xb.at[f_slot] if grads else xb_w
        if grads:
            for j in range(3):
                xb_r[pl.ds(SUB * j, SUB), :] = halo[j]
        c16_r, g_r, a_r, h_r, k_r = s_c16.at[f_slot], s_g.at[f_slot], s_a.at[f_slot], s_h.at[f_slot], s_k.at[f_slot]
        ra_r, ui_r, mi_r = s_ra.at[f_slot], s_ui.at[f_slot], s_mi.at[f_slot]
        r_r = s_r.at[f_slot] if grads else None

        def conv_body(grp, carry):
            xm3, xm2, xm1 = carry
            pend = None
            for j in range(SUB):
                t = grp * SUB + j
                x0 = (in_x[strided(t), :] + b_x).astype(BF16).astype(F32)
                pos = pos_f[row8(t * SUB), :]
                acc = c_b + x0 * taps[0]
                acc = acc + jnp.where(pos >= 1, xm1, 0.0) * taps[1]
                acc = acc + jnp.where(pos >= 2, xm2, 0.0) * taps[2]
                acc = acc + jnp.where(pos >= 3, xm3, 0.0) * taps[3]
                if grads:
                    xb_r[row8(t * SUB + 3 * SUB), :] = x0
                if pend is None:
                    pend = acc
                else:
                    both = jnp.concatenate([pend, acc], axis=0).astype(BF16)
                    c16_r[pl.ds(pl.multiple_of((t - 1) * SUB, 2 * SUB), 2 * SUB), :] = both
                    pend = None
                xm3, xm2, xm1 = xm2, xm1, x0
            return xm3, xm2, xm1

        last3 = lax.fori_loop(0, n_groups, conv_body, tuple(halo))
        pre = jnp.dot(c16_r[...], wg_f[...], preferred_element_type=F32)
        pre_a[...] = pre[:, :LANES]
        pre_i[...] = pre[:, LANES:]
        h_r[pl.ds(0, SUB), :] = h_in

        def gate_body(grp, carry):
            h, sum_y = carry
            for j in range(SUB):
                t = grp * SUB + j
                rows = row8(t * SUB)
                if j % 2 == 0:
                    c2 = c16_r[pl.ds(pl.multiple_of(t * SUB, 2 * SUB), 2 * SUB), :].astype(F32)
                c = c2[:SUB] if j % 2 == 0 else c2[SUB:]
                reset = pos_f[rows, :] == 0
                r = jax.nn.sigmoid(pre_a[rows, :] + b_a)
                i = jax.nn.sigmoid(pre_i[rows, :] + b_i)
                la = nsp * r
                a = jnp.exp(la)
                y2 = la + la
                poly = -y2 * (1.0 + y2 * (0.5 + y2 * (1.0 / 6.0 + y2 * (1.0 / 24.0))))
                q = jnp.maximum(jnp.where(y2 > -0.0625, poly, 1.0 - a * a), 1e-37)
                rm = lax.rsqrt(q)
                m = jnp.where(reset, 1.0, q * rm)
                ic = i * c
                k = a * ic * rm
                a = jnp.where(reset, 0.0, a)
                u = m * ic
                h = a * h + u
                h_r[row8(t * SUB + SUB), :] = h
                a_r[rows, :] = a
                k_r[rows, :] = k
                ra_r[rows, :] = la - la * r
                ui_r[rows, :] = u - u * i
                mi_r[rows, :] = m * i
                if grads:
                    r_r[rows, :] = r
                v = in_y[strided(t), :] + b_y
                v2 = v * v
                th = jnp.tanh(v * (GELU_K0 + GELU_K1 * v2))
                hv = 0.5 * v
                y = hv + hv * th
                dy = (0.5 + 0.5 * th) + hv * (1.0 - th * th) * (GELU_K0 + (3.0 * GELU_K1) * v2)
                d = in_d[strided(t), :]
                g_r[rows, :] = d * y
                out_m[strided(t), :] = h * y
                d_py = d * h * dy
                out_y[strided(t), :] = d_py
                if grads:
                    sum_y = sum_y + d_py
            return h, sum_y

        h_end, sum_y = lax.fori_loop(0, n_groups, gate_body, (h_in, jnp.zeros((SUB, LANES), F32)))
        if grads:
            @pl.when(lax.rem(f_step, n_tiles) == 0)
            def _():
                sy_o[...] = jnp.zeros_like(sy_o)
            sy_o[...] += sum_y

        @pl.when(me == 0)
        def _():
            out_msg = send.at[f_msg]
            out_msg[pl.ds(0, SUB), :] = h_end
            for j in range(3):
                out_msg[pl.ds(SUB * (1 + j), SUB), :] = last3[j]
        for seq in range(SUB):
            mix_o[pl.ds(seq * n_tok, n_tok), :] = out_m[pl.ds(seq * pitch, n_tok), :].astype(BF16)
            dpy_o[pl.ds(seq * n_tok, n_tok), :] = out_y[pl.ds(seq * pitch, n_tok), :].astype(BF16)

        @pl.when(me == 0)
        def _():
            message(f_msg).start()

    @pl.when(jnp.logical_and(b_on, me == 0))
    def _():
        message(b_msg).wait_recv()

    @pl.when(jnp.logical_and(jnp.logical_and(b_step >= 1, b_step <= n_steps), me == 1))
    def _():
        message(lax.rem(b_step - 1 + MSG_SLOTS, MSG_SLOTS)).wait_send()

    @pl.when(b_on)
    def _():
        taps = [jnp.broadcast_to(par_b[2 + k:3 + k, :], (SUB, LANES)) for k in range(TAPS)]
        last = (me == 1)
        in_msg = recv.at[b_msg]
        carry_in = jnp.where(last, 0.0, in_msg[pl.ds(0, SUB), :])
        tail = [jnp.where(last, 0.0, in_msg[pl.ds(SUB * (1 + j), SUB), :]) for j in range(3)]
        g_r, a_r, h_r, k_r = s_g.at[b_slot], s_a.at[b_slot], s_h.at[b_slot], s_k.at[b_slot]
        ra_r, ui_r, mi_r = s_ra.at[b_slot], s_ui.at[b_slot], s_mi.at[b_slot]
        r_r = s_r.at[b_slot] if grads else None
        xb_r = s_xb.at[b_slot] if grads else None
        zero = jnp.zeros((SUB, LANES), F32)

        def scan_body(back, carry):
            grp = n_groups - 1 - back
            adh, sum_a, sum_i, sum_p = carry
            pend = None
            for j in reversed(range(SUB)):
                t = grp * SUB + j
                rows = row8(t * SUB)
                dh = g_r[rows, :] + adh
                adh = a_r[rows, :] * dh
                dlog = adh * (h_r[rows, :] - k_r[rows, :])
                dpa = dlog * ra_r[rows, :]
                dpi = dh * ui_r[rows, :]
                d_c[rows, :] = dh * mi_r[rows, :]
                if grads:
                    sum_a = sum_a + dpa
                    sum_i = sum_i + dpi
                    sum_p = sum_p + dlog * r_r[rows, :]
                if pend is None:
                    pend = (dpa, dpi)
                else:
                    pair = pl.ds(pl.multiple_of(t * SUB, 2 * SUB), 2 * SUB)
                    d_16[pair, :LANES] = jnp.concatenate([dpa, pend[0]], axis=0).astype(BF16)
                    d_16[pair, LANES:] = jnp.concatenate([dpi, pend[1]], axis=0).astype(BF16)
                    pend = None
            return adh, sum_a, sum_i, sum_p

        adh, sum_a, sum_i, sum_p = lax.fori_loop(0, n_groups, scan_body, (carry_in, zero, zero, zero))
        d_gate[...] = lax.dot_general(d_16[...], wg_b[...], (((1,), (1,)), ((), ())), preferred_element_type=F32)

        def conv_body(grp, carry):
            e3, e2, e1 = carry[:3]
            sums = list(carry[3:])
            for j in range(SUB):
                s = grp * SUB + j
                rows = row8(s * SUB)
                pos = pos_b[rows, :]
                dc = d_c[rows, :] + d_gate[rows, :]
                m1 = jnp.where(pos >= 1, dc, 0.0)
                m2 = jnp.where(pos >= 2, dc, 0.0)
                m3 = jnp.where(pos >= 3, dc, 0.0)
                done = e3 + m3 * taps[3]
                out_b[strided(s + SUB - 3), :] = done
                e3, e2, e1 = e2 + m2 * taps[2], e1 + m1 * taps[1], dc * taps[0]
                if grads:
                    sums[0] = sums[0] + dc * xb_r[row8(s * SUB + 3 * SUB), :]
                    sums[1] = sums[1] + m1 * xb_r[row8(s * SUB + 2 * SUB), :]
                    sums[2] = sums[2] + m2 * xb_r[row8(s * SUB + SUB), :]
                    sums[3] = sums[3] + m3 * xb_r[row8(s * SUB), :]
                    sums[4] = sums[4] + dc
                    sums[5] = sums[5] + done
            return (e3, e2, e1) + tuple(sums)

        res = lax.fori_loop(0, n_groups, conv_body, (zero, zero, zero) + (zero,) * (6 if grads else 0))
        ends = [res[j] + tail[j] for j in range(3)]
        for j in range(3):
            out_b[strided(n_tok + SUB - 3 + j), :] = ends[j]
        heads = [out_b[strided(SUB - 3 + j), :] for j in range(3)]

        @pl.when(me == 1)
        def _():
            out_msg = send.at[b_msg]
            out_msg[pl.ds(0, SUB), :] = adh
            for j in range(3):
                out_msg[pl.ds(SUB * (1 + j), SUB), :] = heads[j]

        for seq in range(SUB):
            dbr_o[pl.ds(seq * n_tok, n_tok), :] = out_b[pl.ds(seq * pitch + SUB, n_tok), :].astype(BF16)
        if grads:
            sums = list(res[3:])
            sum_x = sums[5] + ends[0] + ends[1] + ends[2] - heads[0] - heads[1] - heads[2]

            @pl.when(lax.rem(b_step, n_tiles) == 0)
            def _():
                gw_o[...] = jnp.zeros_like(gw_o)
                sb_o[...] = jnp.zeros_like(sb_o)
            for n, val in enumerate((sum_x, sums[0], sums[1], sums[2], sums[3], sums[4], sum_a, sum_i, sum_p)):
                sb_o[0, pl.ds(n * SUB, SUB), :] += val
            gw_o[0] += lax.dot_general(s_c16[b_slot], d_16[...], (((0,), (0,)), ((), ())), preferred_element_type=F32)

        @pl.when(me == 1)
        def _():
            message(b_msg).start()

    @pl.when(jnp.logical_and(f_on, me == 0))
    def _():
        message(f_msg).wait_send()


def middle(px, py, dm, pos_rep, par, w_gate, grads, collective_id):
    n_rows, width = px.shape
    n_tok = pos_rep.shape[1] // SUB
    tile = SUB * n_tok
    n_tiles, n_chunks = n_rows // tile, width // LANES
    n_steps = n_tiles * n_chunks

    def f_of(s):
        return jnp.clip(s - lax.axis_index("cp"), 0, n_steps - 1)

    def b_of(s):
        return jnp.clip(s - 2 + lax.axis_index("cp"), 0, n_steps - 1)

    def spec(shape, of, index):
        def index_map(s):
            k = of(s)
            return index(k // n_tiles, k % n_tiles)
        return pl.BlockSpec(shape, index_map)

    big = lambda of: spec((tile, LANES), of, lambda c, t: (t, c))
    in_specs = [
        spec((None, tile, LANES), f_of, lambda c, t: (t, 0, 0)), spec((None, tile, LANES), b_of, lambda c, t: (t, 0, 0)),
        spec((16, LANES), f_of, lambda c, t: (0, c)), spec((16, LANES), b_of, lambda c, t: (0, c)),
        spec((None, LANES, 2 * LANES), f_of, lambda c, t: (c, 0, 0)), spec((None, LANES, 2 * LANES), b_of, lambda c, t: (c, 0, 0)),
        big(f_of), big(f_of), big(f_of)]
    out_specs = [big(f_of), big(f_of), big(b_of)]
    out_shape = [jax.ShapeDtypeStruct((n_rows, width), BF16)] * 3
    if grads:
        out_specs += [spec((1, LANES, 2 * LANES), b_of, lambda c, t: (c, 0, 0)), spec((1, SUB, LANES), f_of, lambda c, t: (c, 0, 0)), spec((1, N_SUMS * SUB, LANES), b_of, lambda c, t: (c, 0, 0))]
        out_shape += [jax.ShapeDtypeStruct((n_chunks, LANES, 2 * LANES), F32), jax.ShapeDtypeStruct((n_chunks, SUB, LANES), F32), jax.ShapeDtypeStruct((n_chunks, N_SUMS * SUB, LANES), F32)]
    pitched = pltpu.VMEM((SUB * (n_tok + SUB), LANES), F32)
    flat = pltpu.VMEM((tile, LANES), F32)
    slots = pltpu.VMEM((SLOTS, tile, LANES), F32)
    small = pltpu.VMEM((SLOTS if grads else 1, tile if grads else SUB, LANES), F32)
    scratch = [
        slots, slots, pltpu.VMEM((SLOTS, tile + SUB, LANES), F32), slots, slots, slots, slots, pltpu.VMEM((SLOTS, tile, LANES), BF16), small,
        pltpu.VMEM((SLOTS if grads else 1, tile + 3 * SUB if grads else SUB, LANES), F32),
        pitched, pitched, pitched, flat, flat, pitched, pitched, pltpu.VMEM((SUB * (n_tok + SUB) + SUB, LANES), F32), flat, pltpu.VMEM((tile, 2 * LANES), BF16), flat,
        pltpu.VMEM((SUB, LANES), F32),
        pltpu.VMEM((MSG_SLOTS, 4 * SUB, LANES), F32), pltpu.VMEM((MSG_SLOTS, 4 * SUB, LANES), F32), pltpu.SemaphoreType.DMA((MSG_SLOTS,)), pltpu.SemaphoreType.DMA((MSG_SLOTS,))]
    return pl.pallas_call(
        functools.partial(middle_kernel, n_steps, n_tiles, n_tok, grads),
        grid=(n_steps + 2,), in_specs=in_specs, out_specs=out_specs, out_shape=out_shape, scratch_shapes=scratch,
        name="middle",
        cost_estimate=pl.CostEstimate(flops=n_rows * width * 1500, bytes_accessed=n_rows * width * 18, transcendentals=n_rows * width * 8),
        compiler_params=pltpu.CompilerParams(collective_id=collective_id, has_side_effects=True, vmem_limit_bytes=60 * 1024 * 1024, dimension_semantics=("arbitrary",)),
    )(pos_rep, pos_rep, par, par, w_gate, w_gate, px, py, dm)


NORM_EPS = 1e-6
VMEM_LIMIT = 60 * 1024 * 1024
ROW = (((1,), (0,)), ((), ()))
CHAN = (((1,), (1,)), ((), ()))
TOK = (((0,), (0,)), ((), ()))
IN_SPECS = (P(None, "cp", None), P(None, "cp", None), P(None, "cp"), P(), P(None, "tp"), P("tp"), P(None, "tp"), P("tp"), P(None, "tp"), P("tp"), P("tp", None, None), P("tp"), P("tp", None, None), P("tp"), P("tp"), P("tp", None), P())
OUT_SPECS = (P(None, "cp", None), P(None, "cp", None), P(), P(None, "tp"), P("tp"), P(None, "tp"), P("tp"), P(None, "tp"), P("tp"), P("tp", None, None), P("tp"), P("tp", None, None), P("tp"), P("tp"), P("tp", None), P())


def params_of(*semantics):
    return pltpu.CompilerParams(vmem_limit_bytes=VMEM_LIMIT, dimension_semantics=semantics)


def norm_kernel(x_ref, scale_ref, n_ref):
    x = x_ref[...].astype(F32)
    inv = lax.rsqrt(jnp.mean(x * x, axis=-1, keepdims=True) + NORM_EPS)
    n_ref[...] = (x * inv * (1.0 + scale_ref[...])).astype(BF16)


def normalize(x, scale):
    rows, width = x.shape
    tile = 256
    return pl.pallas_call(
        norm_kernel, grid=(rows // tile,), name="normalize",
        in_specs=[pl.BlockSpec((tile, width), lambda i: (i, 0)), pl.BlockSpec((1, width), lambda i: (0, 0))],
        out_specs=pl.BlockSpec((tile, width), lambda i: (i, 0)), out_shape=jax.ShapeDtypeStruct(x.shape, BF16),
        cost_estimate=pl.CostEstimate(flops=rows * width * 600, bytes_accessed=4 * rows * width, transcendentals=rows),
        compiler_params=params_of("arbitrary"),
    )(x, scale)


def up_kernel(n_weights, flip, gathered, *refs):
    lhs = refs[0]
    n_in = 4 if gathered else 1
    parts = [refs[1 + n_in * w:1 + n_in * (w + 1)] for w in range(n_weights)]
    outs = refs[1 + n_in * n_weights:]
    me = lax.axis_index("cp")
    if gathered:
        stored = outs[n_weights:]

        @pl.when(pl.program_id(1) == 0)
        def _():
            for part, dst in zip(parts, stored):
                for q, ref in enumerate(part):
                    half = me if q < 2 else 1 - me
                    depth = ref.shape[1] if flip else ref.shape[0]
                    at = pl.ds(pl.multiple_of((half * 2 + q % 2) * depth, depth), depth)
                    if flip:
                        dst[:, at] = ref[...].astype(BF16)
                    else:
                        dst[at, :] = ref[...].astype(BF16)
        weights = stored
    else:
        weights = [part[0] for part in parts]
    for w in range(n_weights):
        outs[w][...] = lax.dot_general(lhs[...], weights[w][...], CHAN if flip else ROW, preferred_element_type=F32)


def up(lhs, weights, flip, n_rows):
    depth = lhs.shape[1]
    gathered = isinstance(weights[0], tuple)
    n = len(weights)
    bm, bn = 1024, 512 if flip else 256
    if gathered:
        width = weights[0][0][0].shape[1 if flip else 2]
        quarter = depth // 4

        def spec(index):
            lead = (None,) * len(index)
            if flip:
                return pl.BlockSpec(lead + (bn, quarter), lambda j, i: index + (j, 0))
            return pl.BlockSpec(lead + (quarter, bn), lambda j, i: index + (0, j))

        w_specs = [spec(index) for w in weights for _, index in w]
        w_args = [array for w in weights for array, _ in w]
    else:
        width = weights[0].shape[0 if flip else 1]
        w_specs = [pl.BlockSpec((bn, depth), lambda j, i: (j, 0)) if flip else pl.BlockSpec((depth, bn), lambda j, i: (0, j))] * n
        w_args = list(weights)
    out_specs = [pl.BlockSpec((bm, bn), lambda j, i: (i, j))] * n
    out_shape = [jax.ShapeDtypeStruct((n_rows, width), F32)] * n
    if gathered:
        out_specs += [pl.BlockSpec((bn, depth), lambda j, i: (j, 0)) if flip else pl.BlockSpec((depth, bn), lambda j, i: (0, j))] * n
        out_shape += [jax.ShapeDtypeStruct((width, depth) if flip else (depth, width), BF16)] * n
    return pl.pallas_call(
        functools.partial(up_kernel, n, flip, gathered), grid=(width // bn, n_rows // bm), name="up",
        in_specs=[pl.BlockSpec((bm, depth), lambda j, i: (i, 0))] + w_specs, out_specs=out_specs, out_shape=out_shape,
        cost_estimate=pl.CostEstimate(flops=2 * n * n_rows * width * depth, bytes_accessed=200000000, transcendentals=0),
        compiler_params=params_of("arbitrary", "arbitrary"),
    )(lhs, *w_args)


def z_kernel(n_pairs, *refs):
    left, right = refs[:n_pairs], refs[n_pairs:2 * n_pairs]
    x_ref, bias_ref, out_ref = refs[2 * n_pairs:]

    def column(c, _):
        cols = pl.ds(pl.multiple_of(c * 256, 256), 256)
        acc = x_ref[:, cols].astype(F32) + bias_ref[:, cols]
        for lhs, rhs in zip(left, right):
            acc = acc + jnp.dot(lhs[...], rhs[:, cols], preferred_element_type=F32)
        out_ref[:, cols] = acc.astype(BF16)
        return 0

    lax.fori_loop(0, out_ref.shape[1] // 256, column, 0)


def project_out(lefts, rights, x, bias, n_rows):
    rows, width = x.shape
    depth = lefts[0].shape[1]
    bm, bn = 1024, 1024
    n = len(lefts)
    return pl.pallas_call(
        functools.partial(z_kernel, n), grid=(n_rows // bm, width // bn), name="project_out",
        in_specs=[pl.BlockSpec((bm, depth), lambda i, j: (i, 0))] * n + [pl.BlockSpec((depth, bn), lambda i, j: (0, j))] * n + [pl.BlockSpec((bm, bn), lambda i, j: (i, j)), pl.BlockSpec((1, bn), lambda i, j: (0, j))],
        out_specs=pl.BlockSpec((bm, bn), lambda i, j: (i, j)), out_shape=jax.ShapeDtypeStruct((rows, width), BF16),
        cost_estimate=pl.CostEstimate(flops=2 * n * rows * width * depth, bytes_accessed=300000000, transcendentals=0),
        compiler_params=params_of("arbitrary", "arbitrary"),
    )(*lefts, *rights, x, bias)


def z_tail_kernel(n_far, own, *refs):
    far, rest = refs[:2 * n_far], refs[2 * n_far:]
    right = rest[:n_far + 1]
    x_ref, bias_ref, _, out_ref = rest[n_far + 1:]
    half = own.shape[0] // 2

    def column(c, _):
        cols = pl.ds(pl.multiple_of(c * 256, 256), 256)
        for h in range(2):
            rows = pl.ds(h * half, half)
            acc = x_ref[rows, cols].astype(F32) + bias_ref[:, cols]
            acc = acc + jnp.dot(own[rows, :], right[0][:, cols], preferred_element_type=F32)
            for j in range(n_far):
                acc = acc + jnp.dot(far[2 * j + h][...].astype(BF16), right[j + 1][:, cols], preferred_element_type=F32)
            out_ref[rows, cols] = acc.astype(BF16)
        return 0

    lax.fori_loop(0, out_ref.shape[1] // 256, column, 0)


def project_out_tail(own, far, rights, x, bias, z, first_row):
    rows, width = x.shape
    depth = own.shape[1]
    bm, bn = rows - first_row, 1024
    skip = first_row // bm
    n = len(far)
    whole = pl.BlockSpec((bm // 2, depth), lambda j: (0, 0))
    tile = pl.BlockSpec((bm, bn), lambda j: (skip, j))
    args = [own] + [v for pair in far for v in pair] + list(rights) + [x, bias, z]
    return pl.pallas_call(
        functools.partial(z_tail_kernel, n), grid=(width // bn,), name="project_out_tail",
        in_specs=[pl.BlockSpec((bm, depth), lambda j: (skip, 0))] + [whole] * (2 * n) + [pl.BlockSpec((depth, bn), lambda j: (0, j))] * (n + 1) + [tile, pl.BlockSpec((1, bn), lambda j: (0, j)), pl.BlockSpec(memory_space=pl.ANY)],
        out_specs=tile, out_shape=jax.ShapeDtypeStruct((rows, width), BF16), input_output_aliases={len(args) - 1: 0},
        cost_estimate=pl.CostEstimate(flops=2 * (n + 1) * bm * width * depth, bytes_accessed=80000000, transcendentals=0),
        compiler_params=params_of("arbitrary"),
    )(*args)


def dn_kernel(n_pairs, *refs):
    left, right, out_ref = refs[:n_pairs], refs[n_pairs:2 * n_pairs], refs[2 * n_pairs]

    def column(c, _):
        cols = pl.ds(pl.multiple_of(c * 256, 256), 256)
        acc = lax.dot_general(left[0][...], right[0][cols, :], CHAN, preferred_element_type=F32)
        for lhs, rhs in zip(left[1:], right[1:]):
            acc = acc + lax.dot_general(lhs[...], rhs[cols, :], CHAN, preferred_element_type=F32)
        out_ref[:, cols] = acc
        return 0

    lax.fori_loop(0, out_ref.shape[1] // 256, column, 0)


def grad_normed(lefts, rights, first_row, rows):
    depth = lefts[0].shape[1]
    width = rights[0].shape[0]
    bm, bn = 1024, 512
    skip = first_row // bm
    n = len(lefts)
    return pl.pallas_call(
        functools.partial(dn_kernel, n), grid=(rows // bm, width // bn), name="grad_normed",
        in_specs=[pl.BlockSpec((bm, depth), lambda i, j: (i + skip, 0))] * n + [pl.BlockSpec((bn, depth), lambda i, j: (j, 0))] * n,
        out_specs=pl.BlockSpec((bm, bn), lambda i, j: (i, j)), out_shape=jax.ShapeDtypeStruct((rows, width), F32),
        cost_estimate=pl.CostEstimate(flops=2 * n * rows * width * depth, bytes_accessed=450000000, transcendentals=0),
        compiler_params=params_of("arbitrary", "arbitrary"),
    )(*lefts, *rights)


def final_kernel(dn_ref, x_ref, gz_ref, scale_ref, *rest):
    out_ref, sum_ref = rest[-2:]

    @pl.when(pl.program_id(0) == 0)
    def _():
        sum_ref[...] = jnp.zeros_like(sum_ref)
    x = x_ref[...].astype(F32)
    gz = gz_ref[...].astype(F32)
    dn = dn_ref[...]
    rows, width = x.shape
    inv = lax.rsqrt(jnp.mean(x * x, axis=-1, keepdims=True) + NORM_EPS)
    xn = x * inv
    part = dn * xn
    g = dn * (1.0 + scale_ref[...])
    mean_gx = jnp.mean(g * xn, axis=-1, keepdims=True)
    out_ref[...] = (gz + inv * (g - xn * mean_gx)).astype(BF16)
    sum_ref[0] += jnp.sum(part.reshape(rows // SUB, SUB, width), axis=0)
    sum_ref[1] += jnp.sum(gz.reshape(rows // SUB, SUB, width), axis=0)


def finish(dn, x, gz, scale, first_row, into):
    rows, width = dn.shape
    tile = 128
    skip = first_row // tile
    row = pl.BlockSpec((tile, width), lambda i: (i + skip, 0))
    args = [dn, x, gz, scale] + ([] if into is None else [into])
    return pl.pallas_call(
        final_kernel, grid=(rows // tile,), name="finish",
        in_specs=[pl.BlockSpec((tile, width), lambda i: (i, 0)), row, row, pl.BlockSpec((1, width), lambda i: (0, 0))] + ([] if into is None else [pl.BlockSpec(memory_space=pl.ANY)]),
        out_specs=[row, pl.BlockSpec((2, SUB, width), lambda i: (0, 0, 0))],
        out_shape=[jax.ShapeDtypeStruct(x.shape, BF16), jax.ShapeDtypeStruct((2, SUB, width), F32)],
        input_output_aliases={} if into is None else {4: 0},
        cost_estimate=pl.CostEstimate(flops=rows * width * 1500, bytes_accessed=rows * width * 10, transcendentals=rows),
        compiler_params=params_of("arbitrary"),
    )(*args)


def spread_positions(seg_pos):
    n_seq, n_tok = seg_pos.shape
    pos = jnp.swapaxes(seg_pos.reshape(n_seq // SUB, SUB, n_tok), 1, 2).reshape(n_seq // SUB, n_tok * SUB, 1)
    return jnp.broadcast_to(pos, (n_seq // SUB, n_tok * SUB, LANES))


def stack_params(b_x, b_y, conv_w, conv_b, b_a, b_i, a_param):
    rows = [b_x, b_y, conv_w[0], conv_w[1], conv_w[2], conv_w[3], conv_b, b_a, b_i]
    rows = [row.astype(F32) for row in rows] + [-8.0 * jax.nn.softplus(a_param)]
    return jnp.concatenate([jnp.stack(rows), jnp.zeros((16 - len(rows), a_param.shape[0]), F32)], axis=0)


def shard_body(x_in, grad_z, seg_pos, norm_scale, w_x, b_x, w_y, b_y, conv_w, conv_b, w_a, b_a, w_i, b_i, a_param, w_out, b_out):
    me = lax.axis_index("cp")
    n_seq, n_tok, d_model = x_in.shape
    n_rows = n_seq * n_tok
    width = a_param.shape[0]
    x = x_in.reshape(n_rows, d_model)
    gz = grad_z.reshape(n_rows, d_model)
    scale = norm_scale.astype(F32).reshape(1, d_model)

    def swap_x(v):
        return lax.ppermute(v, "tp", [(j, j ^ 1) for j in range(4)])

    def swap_y(v):
        return lax.ppermute(v, "tp", [(j, j ^ 2) for j in range(4)])

    def swap_core(v):
        return lax.ppermute(v, "cp", [(0, 1), (1, 0)])

    tile = SUB * n_tok
    shared = n_rows - tile

    par = stack_params(b_x, b_y, conv_w, conv_b, b_a, b_i, a_param)
    w_gate = jnp.concatenate([w_a, w_i], axis=2)
    small = jnp.concatenate([par.reshape(-1), w_gate.astype(F32).reshape(-1)]).reshape(-1, LANES)
    small_x = swap_x(small)
    small_y = swap_y(small)

    def after(values, *before):
        return lax.optimization_barrier((values, before))[0]

    def quarter(w, axis, q):
        size = d_model // 4
        return lax.dynamic_slice_in_dim(w, (me * 2 + q) * size, size, axis).astype(F32)

    def to_neighbours(weights, axis, before):
        weights = after(weights, before)
        sent = [jnp.stack([quarter(w, axis, q) for w in weights]) for q in range(2)]
        return [swap_x(v) for v in sent], [swap_y(v) for v in sent]

    group_a = to_neighbours((w_x, w_y), 0, small)

    def unpack(s):
        flat = s.reshape(-1)
        return flat[:par.size].reshape(par.shape), lax.optimization_barrier(flat[par.size:]).reshape(w_gate.shape).astype(BF16)

    normed = normalize(x, scale)
    pos_rep = spread_positions(seg_pos)
    px, py = up(normed, [w_x, w_y], False, n_rows)
    group_b = to_neighbours((w_out,), 1, px)
    dm, = up(after(gz, px), [w_out], True, n_rows)
    mixed, dpy, dbr, g_gate, s_y, s_b = middle(px, py, dm, pos_rep, par, w_gate, True, 0)
    g_w_out = lax.dot_general(mixed, gz, TOK, preferred_element_type=F32)

    def spread(group, *before):
        from_x, from_y = after(group, *before)
        diag = [swap_y(from_x[0]), swap_x(from_y[1])]
        return (from_x, [swap_core(v) for v in from_x]), (from_y, [swap_core(v) for v in from_y]), diag

    side_x, side_y, diag_a = spread(group_a, g_w_out)
    small_d = swap_y(after(small_x, g_w_out))
    dbr_g, dpy_g = after((dbr, dpy), side_x[0], side_y[0])
    g_w_x = lax.dot_general(normed, dbr_g, TOK, preferred_element_type=F32)
    g_w_y = lax.dot_general(normed, dpy_g, TOK, preferred_element_type=F32)

    def quarters(side, n):
        own, other = side
        return [tuple((v, (k,)) for v in list(own) + list(other)) for k in range(n)]

    px_x, py_x, wx_x, wy_x = up(normed, quarters(side_x, 2), False, shared)
    out_x, out_y, diag_b = spread(group_b, px_x)
    rows_tail = [after(mixed, px_x)[shared + h * (tile // 2):shared + (h + 1) * (tile // 2)].astype(F32) for h in range(2)]
    tail_x, tail_y = [swap_x(v) for v in rows_tail], [swap_y(v) for v in rows_tail]
    px_y, py_y, wx_y, wy_y = up(normed, quarters(side_y, 2), False, shared)
    dm_x, wo_x = up(after(gz, px_y), quarters(out_x, 1), True, shared)
    par_j, gate_j = unpack(small_x)
    mixed_x, dpy_x, dbr_x = middle(px_x, py_x, dm_x, pos_rep, par_j, gate_j, False, 1)
    dm_y, wo_y = up(after(gz, mixed_x), quarters(out_y, 1), True, shared)
    par_j, gate_j = unpack(small_y)
    mixed_y, dpy_y, dbr_y = middle(px_y, py_y, dm_y, pos_rep, par_j, gate_j, False, 1)
    diag_a = after(diag_a, mixed_y)
    diag_a = (diag_a, [swap_core(v) for v in diag_a])
    dn_tail = grad_normed(after([dbr, dpy], diag_a[0]), [w_x, w_y], shared, tile)
    diag_b = after(diag_b, dn_tail)
    diag_b = (diag_b, [swap_core(v) for v in diag_b])
    dn_tail = lax.psum(dn_tail, "tp")
    px_d, py_d, wx_d, wy_d = up(after(normed, diag_b[0]), quarters(diag_a, 2), False, shared)
    dm_d, wo_d = up(after(gz, px_d), quarters(diag_b, 1), True, shared)
    par_j, gate_j = unpack(small_d)
    par_j, far_x, far_y = after((par_j, tail_x, tail_y), dm_d)
    far_d = [swap_y(far_x[0]), swap_x(far_y[1])]
    mixed_d, dpy_d, dbr_d = middle(px_d, py_d, dm_d, pos_rep, par_j, gate_j, False, 1)
    wx_all, wy_all, wo_all = [w_x, wx_x, wx_y, wx_d], [w_y, wy_x, wy_y, wy_d], [w_out, wo_x, wo_y, wo_d]

    dn = grad_normed([dbr, dbr_x, dbr_y, dbr_d, dpy, dpy_x, dpy_y, dpy_d], wx_all + wy_all, 0, shared)
    grad_x, sums_x = finish(dn, x, gz, scale, 0, None)
    grad_x, sums_t = finish(dn_tail, x, gz, scale, shared, grad_x)
    sums_x = jnp.sum(sums_x + sums_t, axis=1)
    bias = b_out.astype(F32).reshape(1, d_model)
    z_out = project_out([mixed, mixed_x, mixed_y, mixed_d], wo_all, x, bias, shared)
    z_out = project_out_tail(mixed, [far_x, far_y, far_d], wo_all, x, bias, z_out, shared).reshape(x_in.shape)

    s_y = jnp.sum(s_y, axis=1).reshape(width)
    s_b = jnp.sum(s_b.reshape(s_b.shape[0], N_SUMS, SUB, LANES), axis=2)
    s_b = jnp.swapaxes(s_b, 0, 1).reshape(N_SUMS, width)
    g_a = -8.0 * s_b[8] * jax.nn.sigmoid(a_param)
    g_scale, g_b_out = lax.psum((sums_x[0], sums_x[1]), "cp")
    sums = lax.psum((g_w_x, s_b[0], g_w_y, s_y, s_b[1:5], s_b[5], g_gate[:, :, :LANES], s_b[6], g_gate[:, :, LANES:], s_b[7], g_a, g_w_out), "cp")
    return (z_out, grad_x.reshape(x_in.shape), g_scale) + tuple(sums) + (g_b_out,)


def solution(mesh):
    return jax.shard_map(shard_body, mesh=mesh, in_specs=IN_SPECS, out_specs=OUT_SPECS, check_vma=False)
```

```python
import functools
import jax
import jax.numpy as jnp
from jax import lax
from jax.experimental import pallas as pl
from jax.experimental.pallas import tpu as pltpu
from jax.sharding import PartitionSpec as P

F32 = jnp.float32
BF16 = jnp.bfloat16
TAPS = 4
SUB = 8
LANES = 128
SLOTS = 3
MSG_SLOTS = 4
VMEM_LIMIT = 60 << 20
ROW = (((1,), (0,)), ((), ()))
CHAN = (((1,), (1,)), ((), ()))
TOK = (((0,), (0,)), ((), ()))
GELU_K0 = 0.7978845608028654
GELU_K1 = 0.7978845608028654 * 0.044715
N_SUMS = 9
N_PAR = 10
BORROW = TAPS - 1


def param_rows(ref):
    return [jnp.broadcast_to(ref[pl.ds(k, 1), :], (SUB, LANES)) for k in range(N_PAR)]


def middle_kernel(n_steps, n_tiles, n_tok, grads, pos_f, pos_b, par_f, par_b, wg_f, wg_b, px, py, dm, *rest):
    if grads:
        mix_o, dpy_o, dbr_o, gw_o, sy_o, sb_o = rest[:6]
        rest = rest[6:]
    else:
        mix_o, dpy_o, dbr_o = rest[:3]
        rest = rest[3:]
    (s_g, s_a, s_h, s_k, s_ra, s_ui, s_mi, s_c16, s_r, s_xb, in_x, in_y, in_d, pre_a, pre_i, out_m, out_y, out_b, d_c, d_16, d_gate, send, recv, send_sem, recv_sem) = rest
    pitch = n_tok + SUB
    me = lax.axis_index("cp")
    step = pl.program_id(0)
    f_step = step - me
    b_step = step - 2 + me
    f_on = jnp.logical_and(f_step >= 0, f_step < n_steps)
    b_on = jnp.logical_and(b_step >= 0, b_step < n_steps)
    f_slot = lax.rem(f_step + SLOTS, SLOTS)
    b_slot = lax.rem(b_step + SLOTS, SLOTS)
    f_msg = lax.rem(f_step + MSG_SLOTS, MSG_SLOTS)
    b_msg = lax.rem(b_step + MSG_SLOTS, MSG_SLOTS)
    n_groups = n_tok // SUB

    def message(slot):
        return pltpu.make_async_remote_copy(src_ref=send.at[slot], dst_ref=recv.at[slot], send_sem=send_sem.at[slot], recv_sem=recv_sem.at[slot], device_id={"cp": 1 - me}, device_id_type=pl.DeviceIdType.MESH)

    @pl.when(step == 0)
    def _():
        barrier = pltpu.get_barrier_semaphore()
        pl.semaphore_signal(barrier, inc=1, device_id={"cp": 1 - me}, device_id_type=pl.DeviceIdType.MESH)
        pl.semaphore_wait(barrier, 1)

    def row8(base):
        return pl.ds(pl.multiple_of(base, SUB), SUB)

    def pair(t):
        return pl.ds(pl.multiple_of(t * SUB, 2 * SUB), 2 * SUB)

    def strided(t):
        return pl.ds(t, SUB, stride=pitch)

    @pl.when(jnp.logical_and(f_on, me == 1))
    def _():
        message(f_msg).wait_recv()

    @pl.when(f_on)
    def _():
        for seq in range(SUB):
            in_x[pl.ds(seq * pitch, n_tok), :] = px[pl.ds(seq * n_tok, n_tok), :]
        b_x, b_y, *taps, c_b, b_a, b_i, nsp = param_rows(par_f)
        h_in, *halo = [jnp.where(me == 0, 0.0, recv[f_msg, pl.ds(SUB * j, SUB), :]) for j in range(TAPS)]
        xb_r = s_xb.at[f_slot] if grads else None
        if grads:
            for j in range(BORROW):
                xb_r[pl.ds(SUB * j, SUB), :] = halo[j]
        c16_r, g_r, a_r, h_r, k_r = s_c16.at[f_slot], s_g.at[f_slot], s_a.at[f_slot], s_h.at[f_slot], s_k.at[f_slot]
        ra_r, ui_r, mi_r = s_ra.at[f_slot], s_ui.at[f_slot], s_mi.at[f_slot]
        r_r = s_r.at[f_slot] if grads else None

        def conv_body(grp, past):
            past = list(past)
            pend = None
            for j in range(SUB):
                t = grp * SUB + j
                now = (in_x[strided(t), :] + b_x).astype(BF16).astype(F32)
                pos = pos_f[row8(t * SUB), :]
                acc = c_b + now * taps[0]
                for k in range(1, TAPS):
                    acc = acc + jnp.where(pos >= k, past[-k], 0.0) * taps[k]
                if grads:
                    xb_r[row8((t + BORROW) * SUB), :] = now
                if pend is None:
                    pend = acc
                else:
                    c16_r[pair(t - 1), :] = jnp.concatenate([pend, acc]).astype(BF16)
                    pend = None
                past = past[1:] + [now]
            return tuple(past)

        last3 = lax.fori_loop(0, n_groups, conv_body, tuple(halo))
        pre = jnp.dot(c16_r[...], wg_f[...], preferred_element_type=F32)
        for seq in range(SUB):
            for src, dst in ((py, in_y), (dm, in_d)):
                dst[pl.ds(seq * pitch, n_tok), :] = src[pl.ds(seq * n_tok, n_tok), :]
        pre_a[...] = pre[:, :LANES]
        pre_i[...] = pre[:, LANES:]
        h_r[pl.ds(0, SUB), :] = h_in

        def gate_body(grp, carry):
            h, sum_y = carry
            for j in range(SUB):
                t = grp * SUB + j
                rows = row8(t * SUB)
                if j % 2:
                    c = both[SUB:]
                else:
                    both = c16_r[pair(t), :].astype(F32)
                    c = both[:SUB]
                reset = pos_f[rows, :] == 0
                r = jax.nn.sigmoid(pre_a[rows, :] + b_a)
                i = jax.nn.sigmoid(pre_i[rows, :] + b_i)
                la = nsp * r
                a = jnp.exp(la)
                y2 = la + la
                poly = -y2 * (1.0 + y2 * (0.5 + y2 * (1.0 / 6.0 + y2 * (1.0 / 24.0))))
                q = jnp.maximum(jnp.where(y2 > -0.0625, poly, 1.0 - a * a), 1e-37)
                rm = lax.rsqrt(q)
                m = jnp.where(reset, 1.0, q * rm)
                ic = i * c
                k = a * ic * rm
                a = jnp.where(reset, 0.0, a)
                u = m * ic
                h = a * h + u
                h_r[row8(t * SUB + SUB), :] = h
                a_r[rows, :] = a
                k_r[rows, :] = k
                ra_r[rows, :] = la - la * r
                ui_r[rows, :] = u - u * i
                mi_r[rows, :] = m * i
                if grads:
                    r_r[rows, :] = r
                v = in_y[strided(t), :] + b_y
                v2 = v * v
                th = jnp.tanh(v * (GELU_K0 + GELU_K1 * v2))
                hv = 0.5 * v
                y = hv + hv * th
                dy = (0.5 + 0.5 * th) + hv * (1.0 - th * th) * (GELU_K0 + (3.0 * GELU_K1) * v2)
                d = in_d[strided(t), :]
                g_r[rows, :] = d * y
                out_m[strided(t), :] = h * y
                d_py = d * h * dy
                out_y[strided(t), :] = d_py
                if grads:
                    sum_y = sum_y + d_py
            return h, sum_y

        h_end, sum_y = lax.fori_loop(0, n_groups, gate_body, (h_in, jnp.zeros((SUB, LANES), F32)))
        if grads:
            @pl.when(lax.rem(f_step, n_tiles) == 0)
            def _():
                sy_o[...] = jnp.zeros_like(sy_o)

            sy_o[...] += sum_y

        @pl.when(me == 0)
        def _():
            for j, val in enumerate((h_end,) + last3):
                send[f_msg, pl.ds(SUB * j, SUB), :] = val

        for seq in range(SUB):
            mix_o[pl.ds(seq * n_tok, n_tok), :] = out_m[pl.ds(seq * pitch, n_tok), :].astype(BF16)
            dpy_o[pl.ds(seq * n_tok, n_tok), :] = out_y[pl.ds(seq * pitch, n_tok), :].astype(BF16)

        @pl.when(me == 0)
        def _():
            message(f_msg).start()

    @pl.when(jnp.logical_and(b_on, me == 0))
    def _():
        message(b_msg).wait_recv()

    @pl.when(jnp.logical_and(jnp.logical_and(b_step >= 1, b_step <= n_steps), me == 1))
    def _():
        message(lax.rem(b_step - 1 + MSG_SLOTS, MSG_SLOTS)).wait_send()

    @pl.when(b_on)
    def _():
        _, _, *taps, _, _, _, _ = param_rows(par_b)
        carry_in, *tail = [jnp.where(me == 1, 0.0, recv[b_msg, pl.ds(SUB * j, SUB), :]) for j in range(TAPS)]
        g_r, a_r, h_r, k_r = s_g.at[b_slot], s_a.at[b_slot], s_h.at[b_slot], s_k.at[b_slot]
        ra_r, ui_r, mi_r = s_ra.at[b_slot], s_ui.at[b_slot], s_mi.at[b_slot]
        r_r = s_r.at[b_slot] if grads else None
        xb_r = s_xb.at[b_slot] if grads else None
        zero = jnp.zeros((SUB, LANES), F32)

        def scan_body(back, carry):
            grp = n_groups - 1 - back
            adh, sum_a, sum_i, sum_p = carry
            pend = None
            for j in reversed(range(SUB)):
                t = grp * SUB + j
                rows = row8(t * SUB)
                dh = g_r[rows, :] + adh
                adh = a_r[rows, :] * dh
                dlog = adh * (h_r[rows, :] - k_r[rows, :])
                dpa = dlog * ra_r[rows, :]
                dpi = dh * ui_r[rows, :]
                d_c[rows, :] = dh * mi_r[rows, :]
                if grads:
                    sum_a = sum_a + dpa
                    sum_i = sum_i + dpi
                    sum_p = sum_p + dlog * r_r[rows, :]
                if pend is None:
                    pend = (dpa, dpi)
                else:
                    d_16[pair(t), :LANES] = jnp.concatenate([dpa, pend[0]]).astype(BF16)
                    d_16[pair(t), LANES:] = jnp.concatenate([dpi, pend[1]]).astype(BF16)
                    pend = None
            return adh, sum_a, sum_i, sum_p

        adh, sum_a, sum_i, sum_p = lax.fori_loop(0, n_groups, scan_body, (carry_in, zero, zero, zero))
        d_gate[...] = lax.dot_general(d_16[...], wg_b[...], CHAN, preferred_element_type=F32)

        def conv_body(grp, carry):
            ahead, sums = list(carry[:BORROW]), list(carry[BORROW:])
            for j in range(SUB):
                s = grp * SUB + j
                rows = row8(s * SUB)
                pos = pos_b[rows, :]
                dc = d_c[rows, :] + d_gate[rows, :]
                masked = [dc] + [jnp.where(pos >= k, dc, 0.0) for k in range(1, TAPS)]
                part = [val * tap for val, tap in zip(masked, taps)]
                done = ahead[0] + part[-1]
                out_b[strided(s + SUB - BORROW), :] = done
                ahead = [ahead[k] + part[-1 - k] for k in range(1, BORROW)] + [part[0]]
                if grads:
                    for k in range(TAPS):
                        sums[k] = sums[k] + masked[k] * xb_r[row8((s + BORROW - k) * SUB), :]
                    sums[TAPS] = sums[TAPS] + dc
                    sums[-1] = sums[-1] + done
            return tuple(ahead + sums)

        res = lax.fori_loop(0, n_groups, conv_body, (zero,) * (BORROW + (TAPS + 2 if grads else 0)))
        ends = [res[j] + tail[j] for j in range(BORROW)]
        for j in range(BORROW):
            out_b[strided(n_tok + SUB - BORROW + j), :] = ends[j]
        heads = [out_b[strided(SUB - BORROW + j), :] for j in range(BORROW)]

        @pl.when(me == 1)
        def _():
            for j, val in enumerate([adh] + heads):
                send[b_msg, pl.ds(SUB * j, SUB), :] = val

        for seq in range(SUB):
            dbr_o[pl.ds(seq * n_tok, n_tok), :] = out_b[pl.ds(seq * pitch + SUB, n_tok), :].astype(BF16)
        if grads:
            *sums, sum_x = res[BORROW:]
            sum_x = sum_x + sum(ends) - sum(heads)

            @pl.when(lax.rem(b_step, n_tiles) == 0)
            def _():
                gw_o[...] = jnp.zeros_like(gw_o)
                sb_o[...] = jnp.zeros_like(sb_o)

            for n, val in enumerate([sum_x] + sums + [sum_a, sum_i, sum_p]):
                sb_o[0, pl.ds(n * SUB, SUB), :] += val
            gw_o[0] += lax.dot_general(s_c16[b_slot], d_16[...], TOK, preferred_element_type=F32)

        @pl.when(me == 1)
        def _():
            message(b_msg).start()

    @pl.when(jnp.logical_and(f_on, me == 0))
    def _():
        message(f_msg).wait_send()


def middle(px, py, dm, pos_rep, par, w_gate, grads, collective_id):
    n_rows, width = px.shape
    n_tok = pos_rep.shape[1] // SUB
    tile = SUB * n_tok
    n_tiles, n_chunks = n_rows // tile, width // LANES
    n_steps = n_tiles * n_chunks

    def f_of(s):
        return jnp.clip(s - lax.axis_index("cp"), 0, n_steps - 1)

    def b_of(s):
        return jnp.clip(s - 2 + lax.axis_index("cp"), 0, n_steps - 1)

    def spec(shape, of, index):
        def index_map(s):
            k = of(s)
            return index(k // n_tiles, k % n_tiles)

        return pl.BlockSpec(shape, index_map)

    big = lambda of: spec((tile, LANES), of, lambda c, t: (t, c))
    both = (f_of, b_of)
    per_chunk = lambda of, *shape: spec((1,) + shape, of, lambda c, t: (c, 0, 0))
    in_specs = [spec((None, tile, LANES), of, lambda c, t: (t, 0, 0)) for of in both]
    in_specs += [spec((par.shape[0], LANES), of, lambda c, t: (0, c)) for of in both]
    in_specs += [spec((None,) + w_gate.shape[1:], of, lambda c, t: (c, 0, 0)) for of in both]
    in_specs += [big(f_of)] * 3
    out_specs = [big(f_of), big(f_of), big(b_of)]
    out_shape = [jax.ShapeDtypeStruct((n_rows, width), BF16)] * 3
    if grads:
        extra = ((b_of, LANES, 2 * LANES), (f_of, SUB, LANES), (b_of, N_SUMS * SUB, LANES))
        out_specs += [per_chunk(*e) for e in extra]
        out_shape += [jax.ShapeDtypeStruct((n_chunks,) + e[1:], F32) for e in extra]
    pitched = pltpu.VMEM((SUB * (n_tok + SUB), LANES), F32)
    flat = pltpu.VMEM((tile, LANES), F32)
    slots = pltpu.VMEM((SLOTS, tile, LANES), F32)
    small = pltpu.VMEM((SLOTS if grads else 1, tile if grads else SUB, LANES), F32)
    scratch = [
        slots, slots, pltpu.VMEM((SLOTS, tile + SUB, LANES), F32), slots, slots, slots, slots, pltpu.VMEM((SLOTS, tile, LANES), BF16), small,
        pltpu.VMEM((SLOTS if grads else 1, tile + BORROW * SUB if grads else SUB, LANES), F32),
        pitched, pitched, pitched, flat, flat, pitched, pitched, pltpu.VMEM((SUB * (n_tok + SUB) + SUB, LANES), F32), flat, pltpu.VMEM((tile, 2 * LANES), BF16), flat,
        *[pltpu.VMEM((MSG_SLOTS, TAPS * SUB, LANES), F32)] * 2, *[pltpu.SemaphoreType.DMA((MSG_SLOTS,))] * 2]
    return pl.pallas_call(
        functools.partial(middle_kernel, n_steps, n_tiles, n_tok, grads),
        grid=(n_steps + 2,), in_specs=in_specs, out_specs=out_specs, out_shape=out_shape, scratch_shapes=scratch,
        name="middle",
        cost_estimate=pl.CostEstimate(flops=n_rows * width * 1500, bytes_accessed=n_rows * width * 18, transcendentals=n_rows * width * 8),
        compiler_params=pltpu.CompilerParams(collective_id=collective_id, has_side_effects=True, vmem_limit_bytes=VMEM_LIMIT, dimension_semantics=("arbitrary",)),
    )(pos_rep, pos_rep, par, par, w_gate, w_gate, px, py, dm)


NORM_EPS = 1e-6
IN_SPECS = (P(None, "cp", None), P(None, "cp", None), P(None, "cp"), P(), P(None, "tp"), P("tp"), P(None, "tp"), P("tp"), P(None, "tp"), P("tp"), P("tp", None, None), P("tp"), P("tp", None, None), P("tp"), P("tp"), P("tp", None), P())
OUT_SPECS = (P(None, "cp", None), P(None, "cp", None), P(), P(None, "tp"), P("tp"), P(None, "tp"), P("tp"), P(None, "tp"), P("tp"), P("tp", None, None), P("tp"), P("tp", None, None), P("tp"), P("tp"), P("tp", None), P())


def params_of(*semantics):
    return pltpu.CompilerParams(vmem_limit_bytes=VMEM_LIMIT, dimension_semantics=semantics)


def norm_kernel(x_ref, scale_ref, n_ref):
    x = x_ref[...].astype(F32)
    inv = lax.rsqrt(jnp.mean(x * x, axis=-1, keepdims=True) + NORM_EPS)
    n_ref[...] = (x * inv * (1.0 + scale_ref[...])).astype(BF16)


def normalize(x, scale):
    rows, width = x.shape
    tile = 256
    return pl.pallas_call(
        norm_kernel, grid=(rows // tile,), name="normalize",
        in_specs=[pl.BlockSpec((tile, width), lambda i: (i, 0)), pl.BlockSpec((1, width), lambda i: (0, 0))],
        out_specs=pl.BlockSpec((tile, width), lambda i: (i, 0)), out_shape=jax.ShapeDtypeStruct(x.shape, BF16),
        cost_estimate=pl.CostEstimate(flops=rows * width * 600, bytes_accessed=4 * rows * width, transcendentals=rows),
        compiler_params=params_of("arbitrary"),
    )(x, scale)


def plain_up_kernel(n_weights, flip, lhs, *refs):
    for w, out in zip(refs[:n_weights], refs[n_weights:]):
        out[...] = lax.dot_general(lhs[...], w[...], CHAN if flip else ROW, preferred_element_type=F32)


def plain_up(lhs, weights, flip):
    rows, depth = lhs.shape
    width = weights[0].shape[0 if flip else 1]
    n = len(weights)
    bm, bn = 1024, 512 // n
    w_spec = pl.BlockSpec((bn, depth), lambda j, i: (j, 0)) if flip else pl.BlockSpec((depth, bn), lambda j, i: (0, j))
    return pl.pallas_call(
        functools.partial(plain_up_kernel, n, flip), grid=(width // bn, rows // bm), name="plain_up",
        in_specs=[pl.BlockSpec((bm, depth), lambda j, i: (i, 0))] + [w_spec] * n,
        out_specs=[pl.BlockSpec((bm, bn), lambda j, i: (i, j))] * n, out_shape=[jax.ShapeDtypeStruct((rows, width), F32)] * n,
        cost_estimate=pl.CostEstimate(flops=2 * n * rows * width * depth, bytes_accessed=4 * rows * depth, transcendentals=0),
        compiler_params=params_of("arbitrary", "arbitrary"),
    )(lhs, *weights)


def up_kernel(n_weights, n_parts, flip, lhs, *refs):
    parts = [refs[n_parts * w:n_parts * (w + 1)] for w in range(n_weights)]
    outs, held = refs[n_parts * n_weights:-1], refs[-1]
    outs, stored = outs[:n_weights], outs[n_weights:]
    me = lax.axis_index("cp")
    j = pl.program_id(1)
    cols = outs[0].shape[1]

    @pl.when(pl.program_id(0) == 0)
    def _():
        for w, part in enumerate(parts):
            mine = pl.ds(w * cols, cols)
            for q, ref in enumerate(part):
                depth = ref.shape[1] if flip else ref.shape[0]
                place = lax.rem(me * 2 + q, n_parts)
                at = pl.ds(pl.multiple_of(place * depth, depth), depth)
                val = ref[...].astype(BF16)
                if flip:
                    held[j, mine, at] = val
                else:
                    held[j, at, mine] = val
                stored[w][(slice(None), at) if flip else (at, slice(None))] = val

    res = lax.dot_general(lhs[...], held[j], CHAN if flip else ROW, preferred_element_type=F32)
    for w, out in enumerate(outs):
        out[...] = res[:, w * cols:(w + 1) * cols]


def up(lhs, weights, flip, n_rows):
    depth = lhs.shape[1]
    n, n_parts = len(weights), len(weights[0])
    width = weights[0][0][0].shape[-2 if flip else -1]
    bm, bn = 1024, 256 // n
    steps = width // bn

    def block(size, lead, of):
        shape = (bn, size) if flip else (size, bn)
        return pl.BlockSpec((None,) * len(lead) + shape, lambda i, j: lead + ((of(i, j), 0) if flip else (0, of(i, j))))

    def once(i, j):
        return jnp.where(i == 0, j, steps - 1)

    out_specs = [pl.BlockSpec((bm, bn), lambda i, j: (i, j))] * n
    out_shape = [jax.ShapeDtypeStruct((n_rows, width), F32)] * n
    out_specs += [block(depth, (), once)] * n
    out_shape += [jax.ShapeDtypeStruct((width, depth) if flip else (depth, width), BF16)] * n
    return pl.pallas_call(
        functools.partial(up_kernel, n, n_parts, flip), grid=(n_rows // bm, steps), name="up",
        in_specs=[pl.BlockSpec((bm, depth), lambda i, j: (i, 0))] + [block(depth // n_parts, lead, once) for part in weights for _, lead in part],
        out_specs=out_specs, out_shape=out_shape,
        scratch_shapes=[pltpu.VMEM((steps, n * bn, depth) if flip else (steps, depth, n * bn), BF16)],
        cost_estimate=pl.CostEstimate(flops=2 * n * n_rows * width * depth, bytes_accessed=4 * n_rows * depth, transcendentals=0),
        compiler_params=params_of("arbitrary", "arbitrary"),
    )(lhs, *[array for part in weights for array, _ in part])


def finish_rows(rows, first, dn_ref, x_ref, gz_ref, scale_ref, grad_ref, sum_ref):
    width = x_ref.shape[1]
    tiles = [pl.ds(n * LANES, LANES) for n in range(width // LANES)]
    here = pl.ds(pl.multiple_of(first, rows), rows)
    square = cross = jnp.zeros((rows, LANES), F32)
    for cols in tiles:
        x = x_ref[here, cols].astype(F32)
        square = square + x * x
        cross = cross + x * (dn_ref[here, cols] * scale_ref[:, cols])
    inv = lax.rsqrt(jnp.sum(square, axis=-1, keepdims=True) / width + NORM_EPS)
    inv_b = jnp.broadcast_to(inv, (rows, LANES))
    pull = jnp.broadcast_to(inv * inv * inv * (jnp.sum(cross, axis=-1, keepdims=True) / width), (rows, LANES))
    for cols in tiles:
        x = x_ref[here, cols].astype(F32)
        gz = gz_ref[here, cols].astype(F32)
        dn = dn_ref[here, cols] * inv_b
        grad_ref[here, cols] = (gz + dn * scale_ref[:, cols] - x * pull).astype(BF16)
        for which, val in enumerate((dn * x, gz)):
            sum_ref[which, :, cols] += sum(val[SUB * r:SUB * (r + 1)] for r in range(rows // SUB))


def z_kernel(n_own, n_far, n_cols, *refs):
    own, far, right = refs[:n_own], refs[n_own:n_own + 2 * n_far], refs[n_own + 2 * n_far:2 * n_own + 3 * n_far]
    x_ref, bias_ref, dn_ref, x_rows, gz_rows, scale_ref = refs[2 * n_own + 3 * n_far:][:6]
    out_ref, grad_ref, sum_ref = refs[-4:-1]
    far_16 = refs[-1]
    unit = 4 * SUB
    turns = out_ref.shape[1] // n_cols
    units = dn_ref.shape[0] // unit // turns

    @pl.when(jnp.logical_and(pl.program_id(0) == 0, pl.program_id(1) == 0))
    def _():
        sum_ref[...] = jnp.zeros_like(sum_ref)
        for k, ref in enumerate(far):
            half = ref.shape[0]
            far_16[k // 2, pl.ds(k % 2 * half, half), :] = ref[...].astype(BF16)

    def column(c, _):
        cols = pl.ds(pl.multiple_of(c * n_cols, n_cols), n_cols)
        acc = x_ref[:, cols].astype(F32) + bias_ref[:, cols]
        for lhs, rhs in zip(list(own) + [far_16.at[k] for k in range(n_far)], right):
            acc = acc + jnp.dot(lhs[...], rhs[:, cols], preferred_element_type=F32)
        out_ref[:, cols] = acc.astype(BF16)
        for u in range(units):
            finish_rows(unit, (c * units + u) * unit, dn_ref, x_rows, gz_rows, scale_ref, grad_ref, sum_ref)
        return 0

    lax.fori_loop(0, turns, column, 0)


def outputs(own, far, rights, x, bias, dn, gz, scale, first_row, into):
    rows, width = dn.shape
    depth = own[0].shape[1]
    bm, bn = 1024, 512
    n_row, n_col = rows // bm, width // bn
    share = rows // (n_row * n_col)
    skip, skip_share = first_row // bm, first_row // share
    tile = pl.BlockSpec((bm, bn), lambda i, j: (i + skip, j))
    part = pl.BlockSpec((share, width), lambda i, j: (i * n_col + j, 0))
    line = pl.BlockSpec((share, width), lambda i, j: (i * n_col + j + skip_share, 0))
    args = list(own) + [v for pair in far for v in pair] + list(rights) + [x, bias, dn, x, gz, scale] + list(into)
    in_specs = [pl.BlockSpec((bm, depth), lambda i, j: (i + skip, 0))] * len(own)
    in_specs += [pl.BlockSpec((bm // 2, depth), lambda i, j: (0, 0))] * (2 * len(far))
    in_specs += [pl.BlockSpec((depth, bn), lambda i, j: (0, j))] * len(rights)
    in_specs += [tile, pl.BlockSpec((1, bn), lambda i, j: (0, j)), part, line, line, pl.BlockSpec((1, width), lambda i, j: (0, 0))]
    in_specs += [pl.BlockSpec(memory_space=pl.ANY)] * len(into)
    return pl.pallas_call(
        functools.partial(z_kernel, len(own), len(far), 256), grid=(n_row, n_col), name="outputs",
        in_specs=in_specs, out_specs=[tile, line, pl.BlockSpec((2, SUB, width), lambda i, j: (0, 0, 0))],
        out_shape=[jax.ShapeDtypeStruct(x.shape, BF16), jax.ShapeDtypeStruct(x.shape, BF16), jax.ShapeDtypeStruct((2, SUB, width), F32)],
        scratch_shapes=[pltpu.VMEM((max(len(far), 1), bm if far else 2 * SUB, depth), BF16)],
        input_output_aliases={len(args) - len(into) + k: k for k in range(len(into))},
        cost_estimate=pl.CostEstimate(flops=2 * len(rights) * rows * width * depth, bytes_accessed=rows * width * 20, transcendentals=rows),
        compiler_params=params_of("arbitrary", "arbitrary"),
    )(*args)


def dn_kernel(n_pairs, *refs):
    left, right, out_ref = refs[:n_pairs], refs[n_pairs:2 * n_pairs], refs[2 * n_pairs]

    def column(c, _):
        cols = pl.ds(pl.multiple_of(c * 256, 256), 256)
        acc = lax.dot_general(left[0][...], right[0][cols, :], CHAN, preferred_element_type=F32)
        for lhs, rhs in zip(left[1:], right[1:]):
            acc = acc + lax.dot_general(lhs[...], rhs[cols, :], CHAN, preferred_element_type=F32)
        out_ref[:, cols] = acc
        return 0

    lax.fori_loop(0, out_ref.shape[1] // 256, column, 0)


def grad_normed(lefts, rights, first_row, rows):
    depth = lefts[0].shape[1]
    width = rights[0].shape[0]
    bm, bn = 1024, 512
    skip = first_row // bm
    n = len(lefts)
    return pl.pallas_call(
        functools.partial(dn_kernel, n), grid=(rows // bm, width // bn), name="grad_normed",
        in_specs=[pl.BlockSpec((bm, depth), lambda i, j: (i + skip, 0))] * n + [pl.BlockSpec((bn, depth), lambda i, j: (j, 0))] * n,
        out_specs=pl.BlockSpec((bm, bn), lambda i, j: (i, j)), out_shape=jax.ShapeDtypeStruct((rows, width), F32),
        cost_estimate=pl.CostEstimate(flops=2 * n * rows * width * depth, bytes_accessed=450000000, transcendentals=0),
        compiler_params=params_of("arbitrary", "arbitrary"),
    )(*lefts, *rights)


def token_product(lhs, rhs):
    return lax.dot_general(lhs, rhs, TOK, preferred_element_type=F32)


def spread_positions(seg_pos):
    n_seq, n_tok = seg_pos.shape
    pos = jnp.swapaxes(seg_pos.reshape(n_seq // SUB, SUB, n_tok), 1, 2).reshape(n_seq // SUB, n_tok * SUB, 1)
    return jnp.broadcast_to(pos, (n_seq // SUB, n_tok * SUB, LANES))


def stack_params(b_x, b_y, conv_w, conv_b, b_a, b_i, a_param):
    rows = [b_x, b_y, conv_w[0], conv_w[1], conv_w[2], conv_w[3], conv_b, b_a, b_i]
    rows = [row.astype(F32) for row in rows] + [-8.0 * jax.nn.softplus(a_param)]
    return jnp.concatenate([jnp.stack(rows), jnp.zeros((16 - len(rows), a_param.shape[0]), F32)], axis=0)


def block_body(x_in, grad_z, seg_pos, norm_scale, w_x, b_x, w_y, b_y, conv_w, conv_b, w_a, b_a, w_i, b_i, a_param, w_out, b_out):
    me = lax.axis_index("cp")
    n_seq, n_tok, d_model = x_in.shape
    n_rows = n_seq * n_tok
    width = a_param.shape[0]
    x = x_in.reshape(n_rows, d_model)
    gz = grad_z.reshape(n_rows, d_model)
    scale = norm_scale.astype(F32).reshape(1, d_model)

    def swap_x(v):
        return lax.ppermute(v, "tp", [(j, j ^ 1) for j in range(4)])

    def swap_y(v):
        return lax.ppermute(v, "tp", [(j, j ^ 2) for j in range(4)])

    def swap_core(v):
        return lax.ppermute(v, "cp", [(0, 1), (1, 0)])

    tile = SUB * n_tok
    shared = n_rows - tile

    par = stack_params(b_x, b_y, conv_w, conv_b, b_a, b_i, a_param)
    w_gate = jnp.concatenate([w_a, w_i], axis=2)
    small = jnp.concatenate([par.reshape(-1), w_gate.astype(F32).reshape(-1)]).reshape(-1, LANES)
    smalls = [lax.ppermute(small, "tp", [(j, j ^ far) for j in range(4)]) for far in range(1, 4)]

    def after(values, *before):
        return lax.optimization_barrier((values, before))[0]

    def quarter(w, axis, q):
        size = d_model // 4
        return lax.dynamic_slice_in_dim(w, (me * 2 + q) * size, size, axis).astype(F32)

    def to_neighbours(weights, axis, before):
        weights = after(weights, before)
        sent = [jnp.stack([quarter(w, axis, q) for w in weights]) for q in range(2)]
        return [swap_x(v) for v in sent], [swap_y(v) for v in sent]

    def cores(values):
        return values, [swap_core(v) for v in values]

    group_a = to_neighbours((w_x, w_y), 0, small)

    def unpack(s):
        flat = s.reshape(-1)
        return flat[:par.size].reshape(par.shape), lax.optimization_barrier(flat[par.size:]).reshape(w_gate.shape).astype(BF16)

    def onward(group):
        return [swap_y(group[0][0]), swap_x(group[1][1])]

    def quarters(side, n):
        own, other = side
        return [tuple((v, (k,)) for v in list(own) + list(other)) for k in range(n)]

    normed = normalize(x, scale)
    pos_rep = spread_positions(seg_pos)
    px, py = plain_up(normed, [w_x, w_y], False)
    group_b = to_neighbours((w_out,), 1, px)
    dm, = plain_up(after(gz, px), [w_out], True)
    mixed, dpy, dbr, g_gate, s_y, s_b = middle(px, py, dm, pos_rep, par, w_gate, True, 0)
    g_w_out = token_product(mixed, gz)
    g_w_y = token_product(normed, dpy)
    group_a = after(group_a, g_w_out, g_w_y)
    side_x, side_y = [cores(values) for values in group_a]
    g_w_x = token_product(normed, after(dbr, g_w_y))
    diag_a = onward(after(group_a, g_w_x))

    px_x, py_x, wx_x, wy_x = up(after(normed, g_w_x), quarters(side_x, 2), False, shared)
    px_y, py_y, wx_y, wy_y = up(after(normed, px_x), quarters(side_y, 2), False, shared)
    group_b, smalls = after((group_b, smalls), px_y)
    out_x, out_y = [cores(values) for values in group_b]
    diag_b = onward(group_b)
    dn_tail = grad_normed(after([dbr, dpy], px_y), [w_x, w_y], shared, tile)
    dm_x, wo_x = up(after(gz, dn_tail), quarters(out_x, 1), True, shared)
    mixed_x, dpy_x, dbr_x = middle(px_x, py_x, dm_x, pos_rep, *unpack(smalls[0]), False, 1)
    dm_y, wo_y = up(after(gz, mixed_x), quarters(out_y, 1), True, shared)
    mixed_y, dpy_y, dbr_y = middle(px_y, py_y, dm_y, pos_rep, *unpack(smalls[1]), False, 1)
    diag_a, diag_b = after((diag_a, diag_b), mixed_y)
    diag_a, diag_b = cores(diag_a), cores(diag_b)
    rows_tail = [after(mixed, mixed_y)[shared + h * (tile // 2):shared + (h + 1) * (tile // 2)].astype(F32) for h in range(2)]
    tail_x, tail_y = [swap_x(v) for v in rows_tail], [swap_y(v) for v in rows_tail]
    px_d, py_d, wx_d, wy_d = up(after(normed, mixed_y), quarters(diag_a, 2), False, shared)
    dn_tail = lax.psum(after(dn_tail, px_d), "tp")
    dm_d, wo_d = up(after(gz, px_d), quarters(diag_b, 1), True, shared)
    mixed_d, dpy_d, dbr_d = middle(px_d, py_d, dm_d, pos_rep, *unpack(smalls[2]), False, 1)

    far_x, far_y = after((tail_x, tail_y), mixed_d)
    far_d = [swap_y(far_x[0]), swap_x(far_y[1])]
    s_y = jnp.sum(s_y, axis=1).reshape(1, width)
    s_b = jnp.swapaxes(jnp.sum(s_b.reshape(s_b.shape[0], N_SUMS, SUB, LANES), axis=2), 0, 1).reshape(N_SUMS, width)
    own_grads = lax.psum(after((g_w_x, g_w_y, g_w_out, g_gate, jnp.concatenate([s_y, s_b])), mixed_d), "cp")
    g_w_x, g_w_y, g_w_out, g_gate, lines = own_grads
    wx_all, wy_all, wo_all = [w_x, wx_x, wx_y, wx_d], [w_y, wy_x, wy_y, wy_d], [w_out, wo_x, wo_y, wo_d]
    dn = grad_normed([dbr, dbr_x, dbr_y, dbr_d, dpy, dpy_x, dpy_y, dpy_d], wx_all + wy_all, 0, shared)
    bias = b_out.astype(F32).reshape(1, d_model)
    z_out, grad_x, sums_x = outputs([mixed, mixed_x, mixed_y, mixed_d], [], wo_all, x, bias, dn, gz, 1.0 + scale, 0, ())
    z_out, grad_x, sums_t = outputs([mixed], [far_x, far_y, far_d], wo_all, x, bias, after(dn_tail, *own_grads), gz, 1.0 + scale, shared, (z_out, grad_x))
    z_out = z_out.reshape(x_in.shape)
    sums_x = jnp.sum(sums_x + sums_t, axis=1)

    sums_x = lax.psum(sums_x, "cp")
    s_y, s_b = lines[0], lines[1:]
    g_a = -8.0 * s_b[8] * jax.nn.sigmoid(a_param)
    return (z_out, grad_x.reshape(x_in.shape), sums_x[0], g_w_x, s_b[0], g_w_y, s_y, s_b[1:5], s_b[5], g_gate[:, :, :LANES], s_b[6], g_gate[:, :, LANES:], s_b[7], g_a, g_w_out, sums_x[1])


def solution(mesh):
    return jax.shard_map(block_body, mesh=mesh, in_specs=IN_SPECS, out_specs=OUT_SPECS, check_vma=False)
```

```python
import functools
import jax
import jax.numpy as jnp
from jax import lax
from jax.experimental import pallas as pl
from jax.experimental.pallas import tpu as pltpu
from jax.sharding import PartitionSpec as P

F32 = jnp.float32
BF16 = jnp.bfloat16
TAPS = 4
SUB = 8
LANES = 128
SLOTS = 3
MSG_SLOTS = 4
VMEM_LIMIT = 60 << 20
ROW = (((1,), (0,)), ((), ()))
CHAN = (((1,), (1,)), ((), ()))
TOK = (((0,), (0,)), ((), ()))
GELU_K0 = 0.7978845608028654
GELU_K1 = 0.7978845608028654 * 0.044715
N_SUMS = 9
SPAN = 32
N_PAR = 10
BORROW = TAPS - 1


def param_rows(ref):
    return [jnp.broadcast_to(ref[pl.ds(k, 1), :], (SUB, LANES)) for k in range(N_PAR)]


def middle_kernel(n_steps, n_tiles, n_tok, grads, pos_w, par_w, wg_w, px, py, dm, *rest):
    if grads:
        mix_o, dpy_o, dbr_o, gw_o, sy_o, sb_o = rest[:6]
        rest = rest[6:]
    else:
        mix_o, dpy_o, dbr_o = rest[:3]
        rest = rest[3:]
    (s_g, s_a, s_h, s_k, s_ra, s_ui, s_mi, s_c16, s_r, s_xb, in_x, in_y, in_d, pre_a, pre_i, out_m, out_y, out_b, d_c, d_16, d_gate, send, recv, send_sem, recv_sem) = rest
    pitch = n_tok + SUB
    me = lax.axis_index("cp")
    step = pl.program_id(0)
    f_step = step - me
    b_step = step - 2 + me
    f_on = jnp.logical_and(f_step >= 0, f_step < n_steps)
    b_on = jnp.logical_and(b_step >= 0, b_step < n_steps)
    f_slot = lax.rem(f_step + SLOTS, SLOTS)
    b_slot = lax.rem(b_step + SLOTS, SLOTS)
    f_msg = lax.rem(f_step + MSG_SLOTS, MSG_SLOTS)
    b_msg = lax.rem(b_step + MSG_SLOTS, MSG_SLOTS)
    n_groups = n_tok // SPAN
    f_at, b_at = [jnp.clip(v, 0, n_steps - 1) for v in (f_step, b_step)]
    pos_f, pos_b = [pos_w.at[lax.rem(v, n_tiles)] for v in (f_at, b_at)]
    par_f, par_b = [par_w.at[:, pl.ds(pl.multiple_of(v // n_tiles * LANES, LANES), LANES)] for v in (f_at, b_at)]
    wg_f, wg_b = [wg_w.at[v // n_tiles] for v in (f_at, b_at)]

    def message(slot):
        return pltpu.make_async_remote_copy(src_ref=send.at[slot], dst_ref=recv.at[slot], send_sem=send_sem.at[slot], recv_sem=recv_sem.at[slot], device_id={"cp": 1 - me}, device_id_type=pl.DeviceIdType.MESH)

    @pl.when(step == 0)
    def _():
        barrier = pltpu.get_barrier_semaphore()
        pl.semaphore_signal(barrier, inc=1, device_id={"cp": 1 - me}, device_id_type=pl.DeviceIdType.MESH)
        pl.semaphore_wait(barrier, 1)

    def row8(base):
        return pl.ds(pl.multiple_of(base, SUB), SUB)

    def pair(t):
        return pl.ds(pl.multiple_of(t * SUB, 2 * SUB), 2 * SUB)

    def strided(t):
        return pl.ds(t, SUB, stride=pitch)

    @pl.when(jnp.logical_and(f_on, me == 1))
    def _():
        message(f_msg).wait_recv()

    @pl.when(f_on)
    def _():
        for seq in range(SUB):
            in_x[pl.ds(seq * pitch, n_tok), :] = px[pl.ds(seq * n_tok, n_tok), :]
        b_x, b_y, *taps, c_b, b_a, b_i, nsp = param_rows(par_f)
        h_in, *halo = [jnp.where(me == 0, 0.0, recv[f_msg, pl.ds(SUB * j, SUB), :]) for j in range(TAPS)]
        xb_r = s_xb.at[f_slot] if grads else None
        if grads:
            for j in range(BORROW):
                xb_r[pl.ds(SUB * j, SUB), :] = halo[j]
        c16_r, g_r, a_r, h_r, k_r = s_c16.at[f_slot], s_g.at[f_slot], s_a.at[f_slot], s_h.at[f_slot], s_k.at[f_slot]
        ra_r, ui_r, mi_r = s_ra.at[f_slot], s_ui.at[f_slot], s_mi.at[f_slot]
        r_r = s_r.at[f_slot] if grads else None

        def conv_body(grp, past):
            past = list(past)
            pend = None
            for j in range(SPAN):
                t = grp * SPAN + j
                now = (in_x[strided(t), :] + b_x).astype(BF16).astype(F32)
                pos = pos_f[row8(t * SUB), :]
                acc = c_b + now * taps[0]
                for k in range(1, TAPS):
                    acc = acc + jnp.where(pos >= k, past[-k], 0.0) * taps[k]
                if grads:
                    xb_r[row8((t + BORROW) * SUB), :] = now
                if pend is None:
                    pend = acc
                else:
                    c16_r[pair(t - 1), :] = jnp.concatenate([pend, acc]).astype(BF16)
                    pend = None
                past = past[1:] + [now]
            return tuple(past)

        last3 = lax.fori_loop(0, n_groups, conv_body, tuple(halo))
        pre = jnp.dot(c16_r[...], wg_f[...], preferred_element_type=F32)
        for seq in range(SUB):
            for src, dst in ((py, in_y), (dm, in_d)):
                dst[pl.ds(seq * pitch, n_tok), :] = src[pl.ds(seq * n_tok, n_tok), :]
        pre_a[...] = pre[:, :LANES]
        pre_i[...] = pre[:, LANES:]
        h_r[pl.ds(0, SUB), :] = h_in

        def gate_body(grp, carry):
            h, sum_y = carry
            for j in range(SPAN):
                t = grp * SPAN + j
                rows = row8(t * SUB)
                if j % 2:
                    c = both[SUB:]
                else:
                    both = c16_r[pair(t), :].astype(F32)
                    c = both[:SUB]
                reset = pos_f[rows, :] == 0
                r = jax.nn.sigmoid(pre_a[rows, :] + b_a)
                i = jax.nn.sigmoid(pre_i[rows, :] + b_i)
                la = nsp * r
                a = jnp.exp(la)
                y2 = la + la
                poly = -y2 * (1.0 + y2 * (0.5 + y2 * (1.0 / 6.0 + y2 * (1.0 / 24.0))))
                q = jnp.maximum(jnp.where(y2 > -0.0625, poly, 1.0 - a * a), 1e-37)
                rm = lax.rsqrt(q)
                m = jnp.where(reset, 1.0, q * rm)
                ic = i * c
                k = a * ic * rm
                a = jnp.where(reset, 0.0, a)
                u = m * ic
                h = a * h + u
                h_r[row8(t * SUB + SUB), :] = h
                a_r[rows, :] = a
                k_r[rows, :] = k
                ra_r[rows, :] = la - la * r
                ui_r[rows, :] = u - u * i
                mi_r[rows, :] = m * i
                if grads:
                    r_r[rows, :] = r
                v = in_y[strided(t), :] + b_y
                v2 = v * v
                th = jnp.tanh(v * (GELU_K0 + GELU_K1 * v2))
                hv = 0.5 * v
                y = hv + hv * th
                dy = (0.5 + 0.5 * th) + hv * (1.0 - th * th) * (GELU_K0 + (3.0 * GELU_K1) * v2)
                d = in_d[strided(t), :]
                g_r[rows, :] = d * y
                out_m[strided(t), :] = h * y
                d_py = d * h * dy
                out_y[strided(t), :] = d_py
                if grads:
                    sum_y = sum_y + d_py
            return h, sum_y

        h_end, sum_y = lax.fori_loop(0, n_groups, gate_body, (h_in, jnp.zeros((SUB, LANES), F32)))
        if grads:
            @pl.when(lax.rem(f_step, n_tiles) == 0)
            def _():
                sy_o[...] = jnp.zeros_like(sy_o)

            sy_o[...] += sum_y

        @pl.when(me == 0)
        def _():
            for j, val in enumerate((h_end,) + last3):
                send[f_msg, pl.ds(SUB * j, SUB), :] = val

        for seq in range(SUB):
            mix_o[pl.ds(seq * n_tok, n_tok), :] = out_m[pl.ds(seq * pitch, n_tok), :].astype(BF16)
            dpy_o[pl.ds(seq * n_tok, n_tok), :] = out_y[pl.ds(seq * pitch, n_tok), :].astype(BF16)

        @pl.when(me == 0)
        def _():
            message(f_msg).start()

    @pl.when(jnp.logical_and(b_on, me == 0))
    def _():
        message(b_msg).wait_recv()

    @pl.when(jnp.logical_and(jnp.logical_and(b_step >= 1, b_step <= n_steps), me == 1))
    def _():
        message(lax.rem(b_step - 1 + MSG_SLOTS, MSG_SLOTS)).wait_send()

    @pl.when(b_on)
    def _():
        _, _, *taps, _, _, _, _ = param_rows(par_b)
        carry_in, *tail = [jnp.where(me == 1, 0.0, recv[b_msg, pl.ds(SUB * j, SUB), :]) for j in range(TAPS)]
        g_r, a_r, h_r, k_r = s_g.at[b_slot], s_a.at[b_slot], s_h.at[b_slot], s_k.at[b_slot]
        ra_r, ui_r, mi_r = s_ra.at[b_slot], s_ui.at[b_slot], s_mi.at[b_slot]
        r_r = s_r.at[b_slot] if grads else None
        xb_r = s_xb.at[b_slot] if grads else None
        zero = jnp.zeros((SUB, LANES), F32)

        def scan_body(back, carry):
            grp = n_groups - 1 - back
            adh, sum_a, sum_i, sum_p = carry
            pend = None
            for j in reversed(range(SPAN)):
                t = grp * SPAN + j
                rows = row8(t * SUB)
                dh = g_r[rows, :] + adh
                adh = a_r[rows, :] * dh
                dlog = adh * (h_r[rows, :] - k_r[rows, :])
                dpa = dlog * ra_r[rows, :]
                dpi = dh * ui_r[rows, :]
                d_c[rows, :] = dh * mi_r[rows, :]
                if grads:
                    sum_a = sum_a + dpa
                    sum_i = sum_i + dpi
                    sum_p = sum_p + dlog * r_r[rows, :]
                if pend is None:
                    pend = (dpa, dpi)
                else:
                    d_16[pair(t), :LANES] = jnp.concatenate([dpa, pend[0]]).astype(BF16)
                    d_16[pair(t), LANES:] = jnp.concatenate([dpi, pend[1]]).astype(BF16)
                    pend = None
            return adh, sum_a, sum_i, sum_p

        adh, sum_a, sum_i, sum_p = lax.fori_loop(0, n_groups, scan_body, (carry_in, zero, zero, zero))
        d_gate[...] = lax.dot_general(d_16[...], wg_b[...], CHAN, preferred_element_type=F32)

        def conv_body(grp, carry):
            ahead, sums = list(carry[:BORROW]), list(carry[BORROW:])
            for j in range(SPAN):
                s = grp * SPAN + j
                rows = row8(s * SUB)
                pos = pos_b[rows, :]
                dc = d_c[rows, :] + d_gate[rows, :]
                masked = [dc] + [jnp.where(pos >= k, dc, 0.0) for k in range(1, TAPS)]
                part = [val * tap for val, tap in zip(masked, taps)]
                done = ahead[0] + part[-1]
                out_b[strided(s + SUB - BORROW), :] = done
                ahead = [ahead[k] + part[-1 - k] for k in range(1, BORROW)] + [part[0]]
                if grads:
                    for k in range(TAPS):
                        sums[k] = sums[k] + masked[k] * xb_r[row8((s + BORROW - k) * SUB), :]
                    sums[TAPS] = sums[TAPS] + dc
                    sums[-1] = sums[-1] + done
            return tuple(ahead + sums)

        res = lax.fori_loop(0, n_groups, conv_body, (zero,) * (BORROW + (TAPS + 2 if grads else 0)))
        ends = [res[j] + tail[j] for j in range(BORROW)]
        for j in range(BORROW):
            out_b[strided(n_tok + SUB - BORROW + j), :] = ends[j]
        heads = [out_b[strided(SUB - BORROW + j), :] for j in range(BORROW)]

        @pl.when(me == 1)
        def _():
            for j, val in enumerate([adh] + heads):
                send[b_msg, pl.ds(SUB * j, SUB), :] = val

        for seq in range(SUB):
            dbr_o[pl.ds(seq * n_tok, n_tok), :] = out_b[pl.ds(seq * pitch + SUB, n_tok), :].astype(BF16)
        if grads:
            *sums, sum_x = res[BORROW:]
            sum_x = sum_x + sum(ends) - sum(heads)

            @pl.when(lax.rem(b_step, n_tiles) == 0)
            def _():
                gw_o[...] = jnp.zeros_like(gw_o)
                sb_o[...] = jnp.zeros_like(sb_o)

            for n, val in enumerate([sum_x] + sums + [sum_a, sum_i, sum_p]):
                sb_o[0, pl.ds(n * SUB, SUB), :] += val
            gw_o[0] += lax.dot_general(s_c16[b_slot], d_16[...], TOK, preferred_element_type=F32)

        @pl.when(me == 1)
        def _():
            message(b_msg).start()

    @pl.when(jnp.logical_and(f_on, me == 0))
    def _():
        message(f_msg).wait_send()


def middle(px, py, dm, pos_rep, par, w_gate, grads, collective_id):
    n_rows, width = px.shape
    n_tok = pos_rep.shape[1] // SUB
    tile = SUB * n_tok
    n_tiles, n_chunks = n_rows // tile, width // LANES
    n_steps = n_tiles * n_chunks

    def f_of(s):
        return jnp.clip(s - lax.axis_index("cp"), 0, n_steps - 1)

    def b_of(s):
        return jnp.clip(s - 2 + lax.axis_index("cp"), 0, n_steps - 1)

    def spec(shape, of, index):
        def index_map(s):
            k = of(s)
            return index(k // n_tiles, k % n_tiles)

        return pl.BlockSpec(shape, index_map)

    big = lambda of: spec((tile, LANES), of, lambda c, t: (t, c))
    per_chunk = lambda of, *shape: spec((1,) + shape, of, lambda c, t: (c, 0, 0))
    in_specs = [pl.BlockSpec((n_tiles,) + pos_rep.shape[1:], lambda s: (0, 0, 0)), pl.BlockSpec(par.shape, lambda s: (0, 0)), pl.BlockSpec(w_gate.shape, lambda s: (0, 0, 0))]
    in_specs += [big(f_of)] * 3
    out_specs = [big(f_of), big(f_of), big(b_of)]
    out_shape = [jax.ShapeDtypeStruct((n_rows, width), BF16)] * 3
    if grads:
        extra = ((b_of, LANES, 2 * LANES), (f_of, SUB, LANES), (b_of, N_SUMS * SUB, LANES))
        out_specs += [per_chunk(*e) for e in extra]
        out_shape += [jax.ShapeDtypeStruct((n_chunks,) + e[1:], F32) for e in extra]
    pitched = pltpu.VMEM((SUB * (n_tok + SUB), LANES), F32)
    flat = pltpu.VMEM((tile, LANES), F32)
    slots = pltpu.VMEM((SLOTS, tile, LANES), F32)
    small = pltpu.VMEM((SLOTS if grads else 1, tile if grads else SUB, LANES), F32)
    scratch = [
        slots, slots, pltpu.VMEM((SLOTS, tile + SUB, LANES), F32), slots, slots, slots, slots, pltpu.VMEM((SLOTS, tile, LANES), BF16), small,
        pltpu.VMEM((SLOTS if grads else 1, tile + BORROW * SUB if grads else SUB, LANES), F32),
        pitched, pitched, pitched, flat, flat, pitched, pitched, pltpu.VMEM((SUB * (n_tok + SUB) + SUB, LANES), F32), flat, pltpu.VMEM((tile, 2 * LANES), BF16), flat,
        *[pltpu.VMEM((MSG_SLOTS, TAPS * SUB, LANES), F32)] * 2, *[pltpu.SemaphoreType.DMA((MSG_SLOTS,))] * 2]
    return pl.pallas_call(
        functools.partial(middle_kernel, n_steps, n_tiles, n_tok, grads),
        grid=(n_steps + 2,), in_specs=in_specs, out_specs=out_specs, out_shape=out_shape, scratch_shapes=scratch,
        name="middle",
        cost_estimate=pl.CostEstimate(flops=n_rows * width * 1500, bytes_accessed=n_rows * width * 18, transcendentals=n_rows * width * 8),
        compiler_params=pltpu.CompilerParams(collective_id=collective_id, has_side_effects=True, vmem_limit_bytes=VMEM_LIMIT, dimension_semantics=("arbitrary",)),
    )(pos_rep, par, w_gate, px, py, dm)


NORM_EPS = 1e-6
IN_SPECS = (P(None, "cp", None), P(None, "cp", None), P(None, "cp"), P(), P(None, "tp"), P("tp"), P(None, "tp"), P("tp"), P(None, "tp"), P("tp"), P("tp", None, None), P("tp"), P("tp", None, None), P("tp"), P("tp"), P("tp", None), P())
OUT_SPECS = (P(None, "cp", None), P(None, "cp", None), P(), P(None, "tp"), P("tp"), P(None, "tp"), P("tp"), P(None, "tp"), P("tp"), P("tp", None, None), P("tp"), P("tp", None, None), P("tp"), P("tp"), P("tp", None), P())


def params_of(*semantics):
    return pltpu.CompilerParams(vmem_limit_bytes=VMEM_LIMIT, dimension_semantics=semantics)


def norm_kernel(x_ref, scale_ref, n_ref):
    x = x_ref[...].astype(F32)
    inv = lax.rsqrt(jnp.mean(x * x, axis=-1, keepdims=True) + NORM_EPS)
    n_ref[...] = (x * inv * (1.0 + scale_ref[...])).astype(BF16)


def normalize(x, scale):
    rows, width = x.shape
    tile = 256
    return pl.pallas_call(
        norm_kernel, grid=(rows // tile,), name="normalize",
        in_specs=[pl.BlockSpec((tile, width), lambda i: (i, 0)), pl.BlockSpec((1, width), lambda i: (0, 0))],
        out_specs=pl.BlockSpec((tile, width), lambda i: (i, 0)), out_shape=jax.ShapeDtypeStruct(x.shape, BF16),
        cost_estimate=pl.CostEstimate(flops=rows * width * 600, bytes_accessed=4 * rows * width, transcendentals=rows),
        compiler_params=params_of("arbitrary"),
    )(x, scale)


def plain_up_kernel(n_weights, flip, lhs, *refs):
    for w, out in zip(refs[:n_weights], refs[n_weights:]):
        out[...] = lax.dot_general(lhs[...], w[...], CHAN if flip else ROW, preferred_element_type=F32)


def plain_up(lhs, weights, flip):
    rows, depth = lhs.shape
    width = weights[0].shape[0 if flip else 1]
    n = len(weights)
    bm, bn = 1024, 512 // n
    w_spec = pl.BlockSpec((bn, depth), lambda j, i: (j, 0)) if flip else pl.BlockSpec((depth, bn), lambda j, i: (0, j))
    return pl.pallas_call(
        functools.partial(plain_up_kernel, n, flip), grid=(width // bn, rows // bm), name="plain_up",
        in_specs=[pl.BlockSpec((bm, depth), lambda j, i: (i, 0))] + [w_spec] * n,
        out_specs=[pl.BlockSpec((bm, bn), lambda j, i: (i, j))] * n, out_shape=[jax.ShapeDtypeStruct((rows, width), F32)] * n,
        cost_estimate=pl.CostEstimate(flops=2 * n * rows * width * depth, bytes_accessed=4 * rows * depth, transcendentals=0),
        compiler_params=params_of("arbitrary", "arbitrary"),
    )(lhs, *weights)


def up_kernel(n_weights, n_parts, flip, lhs, *refs):
    parts = [refs[n_parts * w:n_parts * (w + 1)] for w in range(n_weights)]
    outs, held = refs[n_parts * n_weights:-1], refs[-1]
    outs, stored = outs[:n_weights], outs[n_weights:]
    me = lax.axis_index("cp")
    j = pl.program_id(1)
    cols = outs[0].shape[1]

    @pl.when(pl.program_id(0) == 0)
    def _():
        for w, part in enumerate(parts):
            mine = pl.ds(w * cols, cols)
            for q, ref in enumerate(part):
                depth = ref.shape[1] if flip else ref.shape[0]
                place = lax.rem(me * 2 + q, n_parts)
                at = pl.ds(pl.multiple_of(place * depth, depth), depth)
                val = ref[...].astype(BF16)
                if flip:
                    held[j, mine, at] = val
                else:
                    held[j, at, mine] = val
                stored[w][(slice(None), at) if flip else (at, slice(None))] = val

    res = lax.dot_general(lhs[...], held[j], CHAN if flip else ROW, preferred_element_type=F32)
    for w, out in enumerate(outs):
        out[...] = res[:, w * cols:(w + 1) * cols]


def up(lhs, weights, flip, n_rows):
    depth = lhs.shape[1]
    n, n_parts = len(weights), len(weights[0])
    width = weights[0][0][0].shape[-2 if flip else -1]
    bm, bn = 1024, 256 // n
    steps = width // bn

    def block(size, lead, of):
        shape = (bn, size) if flip else (size, bn)
        return pl.BlockSpec((None,) * len(lead) + shape, lambda i, j: lead + ((of(i, j), 0) if flip else (0, of(i, j))))

    def once(i, j):
        return jnp.where(i == 0, j, steps - 1)

    out_specs = [pl.BlockSpec((bm, bn), lambda i, j: (i, j))] * n
    out_shape = [jax.ShapeDtypeStruct((n_rows, width), F32)] * n
    out_specs += [block(depth, (), once)] * n
    out_shape += [jax.ShapeDtypeStruct((width, depth) if flip else (depth, width), BF16)] * n
    return pl.pallas_call(
        functools.partial(up_kernel, n, n_parts, flip), grid=(n_rows // bm, steps), name="up",
        in_specs=[pl.BlockSpec((bm, depth), lambda i, j: (i, 0))] + [block(depth // n_parts, lead, once) for part in weights for _, lead in part],
        out_specs=out_specs, out_shape=out_shape,
        scratch_shapes=[pltpu.VMEM((steps, n * bn, depth) if flip else (steps, depth, n * bn), BF16)],
        cost_estimate=pl.CostEstimate(flops=2 * n * n_rows * width * depth, bytes_accessed=4 * n_rows * depth, transcendentals=0),
        compiler_params=params_of("arbitrary", "arbitrary"),
    )(lhs, *[array for part in weights for array, _ in part])


def finish_rows(rows, first, dn_ref, x_ref, gz_ref, scale_ref, grad_ref, sum_ref):
    width = x_ref.shape[1]
    tiles = [pl.ds(n * LANES, LANES) for n in range(width // LANES)]
    here = pl.ds(pl.multiple_of(first, rows), rows)
    square = cross = jnp.zeros((rows, LANES), F32)
    for cols in tiles:
        x = x_ref[here, cols].astype(F32)
        square = square + x * x
        cross = cross + x * (dn_ref[here, cols] * scale_ref[:, cols])
    inv = lax.rsqrt(jnp.sum(square, axis=-1, keepdims=True) / width + NORM_EPS)
    inv_b = jnp.broadcast_to(inv, (rows, LANES))
    pull = jnp.broadcast_to(inv * inv * inv * (jnp.sum(cross, axis=-1, keepdims=True) / width), (rows, LANES))
    for cols in tiles:
        x = x_ref[here, cols].astype(F32)
        gz = gz_ref[here, cols].astype(F32)
        dn = dn_ref[here, cols] * inv_b
        grad_ref[here, cols] = (gz + dn * scale_ref[:, cols] - x * pull).astype(BF16)
        for which, val in enumerate((dn * x, gz)):
            sum_ref[which, :, cols] += sum(val[SUB * r:SUB * (r + 1)] for r in range(rows // SUB))


def z_kernel(n_own, n_far, n_into, n_moved, *refs):
    own, far, right = refs[:n_own], refs[n_own:n_own + 2 * n_far], refs[n_own + 2 * n_far:2 * n_own + 3 * n_far]
    x_ref, bias_ref, dn_ref, x_rows, gz_rows, scale_ref = refs[2 * n_own + 3 * n_far:][:6]
    rest = refs[2 * n_own + 3 * n_far + 6 + n_into:]
    moved, (out_ref, grad_ref, sum_ref), placed, far_16 = rest[:n_moved], rest[n_moved:n_moved + 3], rest[n_moved + 3:-1], rest[-1]
    for src, dst in zip(moved, placed):
        dst[...] = src[...]
    unit = 4 * SUB

    @pl.when(jnp.logical_and(pl.program_id(0) == 0, pl.program_id(1) == 0))
    def _():
        sum_ref[...] = jnp.zeros_like(sum_ref)
        for k, ref in enumerate(far):
            half = ref.shape[0]
            far_16[k // 2, pl.ds(k % 2 * half, half), :] = ref[...].astype(BF16)

    acc = x_ref[...].astype(F32) + bias_ref[...]
    for lhs, rhs in zip(list(own) + [far_16.at[k] for k in range(n_far)], right):
        acc = acc + jnp.dot(lhs[...], rhs[...], preferred_element_type=F32)
    out_ref[...] = acc.astype(BF16)
    for first in range(0, dn_ref.shape[0], unit):
        finish_rows(unit, first, dn_ref, x_rows, gz_rows, scale_ref, grad_ref, sum_ref)


def outputs(own, far, rights, x, bias, dn, gz, scale, first_row, into, moved):
    rows, width = dn.shape
    depth = own[0].shape[1]
    bm, bn = 1024, 512
    n_row, n_col = rows // bm, width // bn
    share = rows // (n_row * n_col)
    skip, skip_share = first_row // bm, first_row // share
    tile = pl.BlockSpec((bm, bn), lambda i, j: (i + skip, j))
    part = pl.BlockSpec((share, width), lambda i, j: (i * n_col + j, 0))
    line = pl.BlockSpec((share, width), lambda i, j: (i * n_col + j + skip_share, 0))
    args = list(own) + [v for pair in far for v in pair] + list(rights) + [x, bias, dn, x, gz, scale] + list(into) + list(moved)
    in_specs = [pl.BlockSpec((bm, depth), lambda i, j: (i + skip, 0))] * len(own)
    in_specs += [pl.BlockSpec((bm // 2, depth), lambda i, j: (0, 0))] * (2 * len(far))
    in_specs += [pl.BlockSpec((depth, bn), lambda i, j: (0, j))] * len(rights)
    in_specs += [tile, pl.BlockSpec((1, bn), lambda i, j: (0, j)), part, line, line, pl.BlockSpec((1, width), lambda i, j: (0, 0))]
    in_specs += [pl.BlockSpec(memory_space=pl.ANY)] * len(into)
    n_move = 16
    passing = [pl.BlockSpec((v.shape[0] // n_move, v.shape[1]), lambda i, j: (jnp.minimum(i * n_col + j, n_move - 1), 0)) for v in moved]
    return pl.pallas_call(
        functools.partial(z_kernel, len(own), len(far), len(into), len(moved)), grid=(n_row, n_col), name="outputs",
        in_specs=in_specs + passing, out_specs=[tile, line, pl.BlockSpec((2, SUB, width), lambda i, j: (0, 0, 0))] + passing,
        out_shape=[jax.ShapeDtypeStruct(x.shape, BF16), jax.ShapeDtypeStruct(x.shape, BF16), jax.ShapeDtypeStruct((2, SUB, width), F32)] + [jax.ShapeDtypeStruct(v.shape, v.dtype) for v in moved],
        scratch_shapes=[pltpu.VMEM((max(len(far), 1), bm if far else 2 * SUB, depth), BF16)],
        input_output_aliases={len(args) - len(moved) - len(into) + k: k for k in range(len(into))},
        cost_estimate=pl.CostEstimate(flops=2 * len(rights) * rows * width * depth, bytes_accessed=rows * width * 20, transcendentals=rows),
        compiler_params=params_of("arbitrary", "arbitrary"),
    )(*args)


def dn_kernel(n_pairs, *refs):
    left, right, out_ref = refs[:n_pairs], refs[n_pairs:2 * n_pairs], refs[2 * n_pairs]

    def column(c, _):
        cols = pl.ds(pl.multiple_of(c * 256, 256), 256)
        acc = lax.dot_general(left[0][...], right[0][cols, :], CHAN, preferred_element_type=F32)
        for lhs, rhs in zip(left[1:], right[1:]):
            acc = acc + lax.dot_general(lhs[...], rhs[cols, :], CHAN, preferred_element_type=F32)
        out_ref[:, cols] = acc
        return 0

    lax.fori_loop(0, out_ref.shape[1] // 256, column, 0)


def grad_normed(lefts, rights, first_row, rows):
    depth = lefts[0].shape[1]
    width = rights[0].shape[0]
    bm, bn = 1024, 512
    skip = first_row // bm
    n = len(lefts)
    return pl.pallas_call(
        functools.partial(dn_kernel, n), grid=(rows // bm, width // bn), name="grad_normed",
        in_specs=[pl.BlockSpec((bm, depth), lambda i, j: (i + skip, 0))] * n + [pl.BlockSpec((bn, depth), lambda i, j: (j, 0))] * n,
        out_specs=pl.BlockSpec((bm, bn), lambda i, j: (i, j)), out_shape=jax.ShapeDtypeStruct((rows, width), F32),
        cost_estimate=pl.CostEstimate(flops=2 * n * rows * width * depth, bytes_accessed=450000000, transcendentals=0),
        compiler_params=params_of("arbitrary", "arbitrary"),
    )(*lefts, *rights)


def token_product(lhs, rhs):
    return lax.dot_general(lhs, rhs, TOK, preferred_element_type=F32)


def spread_positions(seg_pos):
    n_seq, n_tok = seg_pos.shape
    pos = jnp.swapaxes(seg_pos.reshape(n_seq // SUB, SUB, n_tok), 1, 2).reshape(n_seq // SUB, n_tok * SUB, 1)
    return jnp.broadcast_to(pos, (n_seq // SUB, n_tok * SUB, LANES))


def stack_params(b_x, b_y, conv_w, conv_b, b_a, b_i, a_param):
    rows = [b_x, b_y, conv_w[0], conv_w[1], conv_w[2], conv_w[3], conv_b, b_a, b_i]
    rows = [row.astype(F32) for row in rows] + [-8.0 * jax.nn.softplus(a_param)]
    return jnp.concatenate([jnp.stack(rows), jnp.zeros((16 - len(rows), a_param.shape[0]), F32)], axis=0)


def block_body(x_in, grad_z, seg_pos, norm_scale, w_x, b_x, w_y, b_y, conv_w, conv_b, w_a, b_a, w_i, b_i, a_param, w_out, b_out):
    me = lax.axis_index("cp")
    n_seq, n_tok, d_model = x_in.shape
    n_rows = n_seq * n_tok
    width = a_param.shape[0]
    x = x_in.reshape(n_rows, d_model)
    gz = grad_z.reshape(n_rows, d_model)
    scale = norm_scale.astype(F32).reshape(1, d_model)

    def swap_x(v):
        return lax.ppermute(v, "tp", [(j, j ^ 1) for j in range(4)])

    def swap_y(v):
        return lax.ppermute(v, "tp", [(j, j ^ 2) for j in range(4)])

    def swap_core(v):
        return lax.ppermute(v, "cp", [(0, 1), (1, 0)])

    tile = SUB * n_tok
    shared = n_rows - tile

    par = stack_params(b_x, b_y, conv_w, conv_b, b_a, b_i, a_param)
    w_gate = jnp.concatenate([w_a, w_i], axis=2)
    small = jnp.concatenate([par.reshape(-1), w_gate.astype(F32).reshape(-1)]).reshape(-1, LANES)
    smalls = [lax.ppermute(small, "tp", [(j, j ^ far) for j in range(4)]) for far in range(1, 4)]

    def after(values, *before):
        return lax.optimization_barrier((values, before))[0]

    def quarter(w, axis, q):
        size = d_model // 4
        return lax.dynamic_slice_in_dim(w, (me * 2 + q) * size, size, axis).astype(F32)

    def to_neighbours(weights, axis, before):
        weights = after(weights, before)
        sent = [jnp.stack([quarter(w, axis, q) for w in weights]) for q in range(2)]
        return [swap_x(v) for v in sent], [swap_y(v) for v in sent]

    def cores(values):
        return values, [swap_core(v) for v in values]

    group_a = to_neighbours((w_x, w_y), 0, small)

    def unpack(s):
        flat = s.reshape(-1)
        return flat[:par.size].reshape(par.shape), lax.optimization_barrier(flat[par.size:]).reshape(w_gate.shape).astype(BF16)

    def onward(group):
        return [swap_y(group[0][0]), swap_x(group[1][1])]

    def quarters(side, n):
        own, other = side
        return [tuple((v, (k,)) for v in list(own) + list(other)) for k in range(n)]

    normed = normalize(x, scale)
    pos_rep = spread_positions(seg_pos)
    px, py = plain_up(normed, [w_x, w_y], False)
    group_b = to_neighbours((w_out,), 1, px)
    dm, = plain_up(after(gz, px), [w_out], True)
    mixed, dpy, dbr, g_gate, s_y, s_b = middle(px, py, dm, pos_rep, par, w_gate, True, 0)
    g_w_out = token_product(mixed, gz)
    g_w_y = token_product(normed, dpy)
    group_a = after(group_a, g_w_out, g_w_y)
    side_x, side_y = [cores(values) for values in group_a]
    g_w_x = token_product(normed, after(dbr, g_w_y))
    diag_a = onward(after(group_a, g_w_x))

    s_y = jnp.sum(s_y, axis=1).reshape(1, width)
    s_b = jnp.swapaxes(jnp.sum(s_b.reshape(s_b.shape[0], N_SUMS, SUB, LANES), axis=2), 0, 1).reshape(N_SUMS, width)
    own_grads = lax.psum((g_w_x, g_w_y, g_w_out, g_gate), "cp")

    px_x, py_x, wx_x, wy_x = up(after(normed, g_w_x), quarters(side_x, 2), False, shared)
    px_y, py_y, wx_y, wy_y = up(after(normed, px_x), quarters(side_y, 2), False, shared)
    group_b, smalls = after((group_b, smalls), px_y)
    out_x, out_y = [cores(values) for values in group_b]
    diag_b = onward(group_b)
    dn_tail = grad_normed(after([dbr, dpy], px_y), [w_x, w_y], shared, tile)
    dm_x, wo_x = up(after(gz, dn_tail), quarters(out_x, 1), True, shared)
    mixed_x, dpy_x, dbr_x = middle(px_x, py_x, dm_x, pos_rep, *unpack(smalls[0]), False, 1)
    dm_y, wo_y = up(after(gz, mixed_x), quarters(out_y, 1), True, shared)
    mixed_y, dpy_y, dbr_y = middle(px_y, py_y, dm_y, pos_rep, *unpack(smalls[1]), False, 1)
    diag_a, diag_b = after((diag_a, diag_b), mixed_y)
    diag_a, diag_b = cores(diag_a), cores(diag_b)
    rows_tail = [after(mixed, mixed_y)[shared + h * (tile // 2):shared + (h + 1) * (tile // 2)].astype(F32) for h in range(2)]
    tail_x, tail_y = [swap_x(v) for v in rows_tail], [swap_y(v) for v in rows_tail]
    px_d, py_d, wx_d, wy_d = up(after(normed, mixed_y), quarters(diag_a, 2), False, shared)
    dn_tail = lax.psum(after(dn_tail, px_d), "tp")
    dm_d, wo_d = up(after(gz, px_d), quarters(diag_b, 1), True, shared)
    mixed_d, dpy_d, dbr_d = middle(px_d, py_d, dm_d, pos_rep, *unpack(smalls[2]), False, 1)

    far_x, far_y = after((tail_x, tail_y), mixed_d)
    far_d = [swap_y(far_x[0]), swap_x(far_y[1])]
    wx_all, wy_all, wo_all = [w_x, wx_x, wx_y, wx_d], [w_y, wy_x, wy_y, wy_d], [w_out, wo_x, wo_y, wo_d]
    dn = grad_normed([dbr, dbr_x, dbr_y, dbr_d, dpy, dpy_x, dpy_y, dpy_d], wx_all + wy_all, 0, shared)
    bias = b_out.astype(F32).reshape(1, d_model)
    *tall, g_gate = own_grads
    lines = lax.psum(after(jnp.concatenate([s_y, s_b]), mixed_d), "cp")
    z_out, grad_x, sums_x, *tall = outputs([mixed, mixed_x, mixed_y, mixed_d], [], wo_all, x, bias, after(dn, lines), gz, 1.0 + scale, 0, (), tall)
    g_w_x, g_w_y, g_w_out = tall
    z_out, grad_x, sums_t = outputs([mixed], [far_x, far_y, far_d], wo_all, x, bias, dn_tail, gz, 1.0 + scale, shared, (z_out, grad_x), ())
    z_out = z_out.reshape(x_in.shape)
    sums_x = jnp.sum(sums_x + sums_t, axis=1)

    sums_x = lax.psum(sums_x, "cp")
    s_y, s_b = lines[0], lines[1:]
    g_a = -8.0 * s_b[8] * jax.nn.sigmoid(a_param)
    return (z_out, grad_x.reshape(x_in.shape), sums_x[0], g_w_x, s_b[0], g_w_y, s_y, s_b[1:5], s_b[5], g_gate[:, :, :LANES], s_b[6], g_gate[:, :, LANES:], s_b[7], g_a, g_w_out, sums_x[1])


def solution(mesh):
    return jax.shard_map(block_body, mesh=mesh, in_specs=IN_SPECS, out_specs=OUT_SPECS, check_vma=False)
```

```python
import functools
import jax
import jax.numpy as jnp
from jax import lax
from jax.experimental import pallas as pl
from jax.experimental.pallas import tpu as pltpu
from jax.sharding import PartitionSpec as P

F32 = jnp.float32
BF16 = jnp.bfloat16
TAPS = 4
SUB = 8
LANES = 128
SLOTS = 3
MSG_SLOTS = 4
VMEM_LIMIT = 60 << 20
ROW = (((1,), (0,)), ((), ()))
CHAN = (((1,), (1,)), ((), ()))
TOK = (((0,), (0,)), ((), ()))
GELU_K0 = 1.5957691216057308
GELU_K1 = GELU_K0 * 0.044715
N_SUMS = 9
SPAN = 64
N_PAR = 10
BORROW = TAPS - 1


def param_rows(ref):
    return [jnp.broadcast_to(ref[pl.ds(k, 1), :], (SUB, LANES)) for k in range(N_PAR)]


def middle_kernel(n_steps, n_tiles, n_tok, grads, pos_w, par_w, wg_w, px, py, dm, *rest):
    if grads:
        mix_o, dpy_o, dbr_o, gw_o, sy_o, sb_o = rest[:6]
        rest = rest[6:]
    else:
        mix_o, dpy_o, dbr_o = rest[:3]
        rest = rest[3:]
    (s_g, s_a, s_h, s_k, s_ra, s_ui, s_mi, s_c16, s_r, s_xb, in_x, in_y, in_d, pre_a, pre_i, out_m, out_y, out_b, d_c, d_16, d_gate, send, recv, send_sem, recv_sem) = rest
    pitch = n_tok + SUB
    me = lax.axis_index("cp")
    step = pl.program_id(0)
    f_step = step - me
    b_step = step - 2 + me
    f_on = jnp.logical_and(f_step >= 0, f_step < n_steps)
    b_on = jnp.logical_and(b_step >= 0, b_step < n_steps)
    f_slot = lax.rem(f_step + SLOTS, SLOTS)
    b_slot = lax.rem(b_step + SLOTS, SLOTS)
    f_msg = lax.rem(f_step + MSG_SLOTS, MSG_SLOTS)
    b_msg = lax.rem(b_step + MSG_SLOTS, MSG_SLOTS)
    n_groups = n_tok // SPAN
    f_at, b_at = [jnp.clip(v, 0, n_steps - 1) for v in (f_step, b_step)]
    pos_f, pos_b = [pos_w.at[lax.rem(v, n_tiles)] for v in (f_at, b_at)]
    par_f, par_b = [par_w.at[:, pl.ds(pl.multiple_of(v // n_tiles * LANES, LANES), LANES)] for v in (f_at, b_at)]
    wg_f, wg_b = [wg_w.at[v // n_tiles] for v in (f_at, b_at)]

    def message(slot):
        return pltpu.make_async_remote_copy(src_ref=send.at[slot], dst_ref=recv.at[slot], send_sem=send_sem.at[slot], recv_sem=recv_sem.at[slot], device_id={"cp": 1 - me}, device_id_type=pl.DeviceIdType.MESH)

    @pl.when(step == 0)
    def _():
        barrier = pltpu.get_barrier_semaphore()
        pl.semaphore_signal(barrier, inc=1, device_id={"cp": 1 - me}, device_id_type=pl.DeviceIdType.MESH)
        pl.semaphore_wait(barrier, 1)

    def row8(base):
        return pl.ds(pl.multiple_of(base, SUB), SUB)

    def pair(t):
        return pl.ds(pl.multiple_of(t * SUB, 2 * SUB), 2 * SUB)

    def strided(t):
        return pl.ds(t, SUB, stride=pitch)

    @pl.when(jnp.logical_and(f_on, me == 1))
    def _():
        message(f_msg).wait_recv()

    @pl.when(f_on)
    def _():
        for seq in range(SUB):
            in_x[pl.ds(seq * pitch, n_tok), :] = px[pl.ds(seq * n_tok, n_tok), :]
        b_x, b_y, *taps, c_b, nb_a, nb_i, nsp = param_rows(par_f)
        h_in, *halo = [jnp.where(me == 0, 0.0, recv[f_msg, pl.ds(SUB * j, SUB), :]) for j in range(TAPS)]
        xb_r = s_xb.at[f_slot] if grads else None
        if grads:
            for j in range(BORROW):
                xb_r[pl.ds(SUB * j, SUB), :] = halo[j]
        c16_r, g_r, a_r, h_r, k_r = s_c16.at[f_slot], s_g.at[f_slot], s_a.at[f_slot], s_h.at[f_slot], s_k.at[f_slot]
        ra_r, ui_r, mi_r = s_ra.at[f_slot], s_ui.at[f_slot], s_mi.at[f_slot]
        r_r = s_r.at[f_slot] if grads else None

        def conv_body(grp, past):
            past = list(past)
            pend = None
            for j in range(SPAN):
                t = grp * SPAN + j
                now = (in_x[strided(t), :] + b_x).astype(BF16).astype(F32)
                pos = pos_f[row8(t * SUB), :]
                acc = c_b + now * taps[0]
                for k in range(1, TAPS):
                    acc = acc + jnp.where(pos >= k, past[-k], 0.0) * taps[k]
                if grads:
                    xb_r[row8((t + BORROW) * SUB), :] = now
                if pend is None:
                    pend = acc
                else:
                    c16_r[pair(t - 1), :] = jnp.concatenate([pend, acc]).astype(BF16)
                    pend = None
                past = past[1:] + [now]
            return tuple(past)

        last3 = lax.fori_loop(0, n_groups, conv_body, tuple(halo))
        pre = jnp.dot(c16_r[...], wg_f[...], preferred_element_type=F32)
        for seq in range(SUB):
            for src, dst in ((py, in_y), (dm, in_d)):
                dst[pl.ds(seq * pitch, n_tok), :] = src[pl.ds(seq * n_tok, n_tok), :]
        pre_a[...] = pre[:, :LANES]
        pre_i[...] = pre[:, LANES:]
        h_r[pl.ds(0, SUB), :] = h_in

        def gate_body(grp, carry):
            h, sum_y = carry
            for j in range(SPAN):
                t = grp * SPAN + j
                rows = row8(t * SUB)
                if j % 2:
                    c = both[SUB:]
                else:
                    both = c16_r[pair(t), :].astype(F32)
                    c = both[:SUB]
                reset = pos_f[rows, :] == 0
                r = 1.0 / (1.0 + jnp.exp(nb_a - pre_a[rows, :]))
                i = 1.0 / (1.0 + jnp.exp(nb_i - pre_i[rows, :]))
                la = nsp * r
                a = jnp.exp(la)
                th = jnp.tanh(jnp.abs(la))
                twice, more = th + th, 1.0 + th
                root = lax.rsqrt(jnp.maximum(twice * more, 1e-37))
                rm = more * root
                m = jnp.where(reset, 1.0, twice * root)
                ic = i * c
                k = a * ic * rm
                a = jnp.where(reset, 0.0, a)
                u = m * ic
                h = a * h + u
                h_r[row8(t * SUB + SUB), :] = h
                a_r[rows, :] = a
                k_r[rows, :] = k
                ra_r[rows, :] = la - la * r
                ui_r[rows, :] = u - u * i
                mi_r[rows, :] = m * i
                if grads:
                    r_r[rows, :] = r
                v = in_y[strided(t), :] + b_y
                v2 = v * v
                cdf = jax.nn.sigmoid(v * (GELU_K0 + GELU_K1 * v2))
                y = v * cdf
                dy = cdf + (y - y * cdf) * (GELU_K0 + (3.0 * GELU_K1) * v2)
                d = in_d[strided(t), :]
                g_r[rows, :] = d * y
                out_m[strided(t), :] = h * y
                d_py = d * h * dy
                out_y[strided(t), :] = d_py
                if grads:
                    sum_y = sum_y + d_py
            return h, sum_y

        h_end, sum_y = lax.fori_loop(0, n_groups, gate_body, (h_in, jnp.zeros((SUB, LANES), F32)))
        if grads:
            @pl.when(lax.rem(f_step, n_tiles) == 0)
            def _():
                sy_o[...] = jnp.zeros_like(sy_o)

            sy_o[...] += sum_y

        @pl.when(me == 0)
        def _():
            for j, val in enumerate((h_end,) + last3):
                send[f_msg, pl.ds(SUB * j, SUB), :] = val

        for seq in range(SUB):
            mix_o[pl.ds(seq * n_tok, n_tok), :] = out_m[pl.ds(seq * pitch, n_tok), :].astype(BF16)
            dpy_o[pl.ds(seq * n_tok, n_tok), :] = out_y[pl.ds(seq * pitch, n_tok), :].astype(BF16)

        @pl.when(me == 0)
        def _():
            message(f_msg).start()

    @pl.when(jnp.logical_and(b_on, me == 0))
    def _():
        message(b_msg).wait_recv()

    @pl.when(jnp.logical_and(jnp.logical_and(b_step >= 1, b_step <= n_steps), me == 1))
    def _():
        message(lax.rem(b_step - 1 + MSG_SLOTS, MSG_SLOTS)).wait_send()

    @pl.when(b_on)
    def _():
        _, _, *taps, _, _, _, _ = param_rows(par_b)
        carry_in, *tail = [jnp.where(me == 1, 0.0, recv[b_msg, pl.ds(SUB * j, SUB), :]) for j in range(TAPS)]
        g_r, a_r, h_r, k_r = s_g.at[b_slot], s_a.at[b_slot], s_h.at[b_slot], s_k.at[b_slot]
        ra_r, ui_r, mi_r = s_ra.at[b_slot], s_ui.at[b_slot], s_mi.at[b_slot]
        r_r = s_r.at[b_slot] if grads else None
        xb_r = s_xb.at[b_slot] if grads else None
        zero = jnp.zeros((SUB, LANES), F32)

        def scan_body(back, carry):
            grp = n_groups - 1 - back
            adh, sum_a, sum_i, sum_p = carry
            pend = None
            for j in reversed(range(SPAN)):
                t = grp * SPAN + j
                rows = row8(t * SUB)
                dh = g_r[rows, :] + adh
                adh = a_r[rows, :] * dh
                dlog = adh * (h_r[rows, :] - k_r[rows, :])
                dpa = dlog * ra_r[rows, :]
                dpi = dh * ui_r[rows, :]
                d_c[rows, :] = dh * mi_r[rows, :]
                if grads:
                    sum_a = sum_a + dpa
                    sum_i = sum_i + dpi
                    sum_p = sum_p + dlog * r_r[rows, :]
                if pend is None:
                    pend = (dpa, dpi)
                else:
                    d_16[pair(t), :LANES] = jnp.concatenate([dpa, pend[0]]).astype(BF16)
                    d_16[pair(t), LANES:] = jnp.concatenate([dpi, pend[1]]).astype(BF16)
                    pend = None
            return adh, sum_a, sum_i, sum_p

        adh, sum_a, sum_i, sum_p = lax.fori_loop(0, n_groups, scan_body, (carry_in, zero, zero, zero))
        d_gate[...] = lax.dot_general(d_16[...], wg_b[...], CHAN, preferred_element_type=F32)

        def conv_body(grp, carry):
            ahead, sums = list(carry[:BORROW]), list(carry[BORROW:])
            for j in range(SPAN):
                s = grp * SPAN + j
                rows = row8(s * SUB)
                pos = pos_b[rows, :]
                dc = d_c[rows, :] + d_gate[rows, :]
                masked = [dc] + [jnp.where(pos >= k, dc, 0.0) for k in range(1, TAPS)]
                part = [val * tap for val, tap in zip(masked, taps)]
                done = ahead[0] + part[-1]
                out_b[strided(s + SUB - BORROW), :] = done
                ahead = [ahead[k] + part[-1 - k] for k in range(1, BORROW)] + [part[0]]
                if grads:
                    for k in range(TAPS):
                        sums[k] = sums[k] + masked[k] * xb_r[row8((s + BORROW - k) * SUB), :]
                    sums[TAPS] = sums[TAPS] + dc
                    sums[-1] = sums[-1] + done
            return tuple(ahead + sums)

        res = lax.fori_loop(0, n_groups, conv_body, (zero,) * (BORROW + (TAPS + 2 if grads else 0)))
        ends = [res[j] + tail[j] for j in range(BORROW)]
        for j in range(BORROW):
            out_b[strided(n_tok + SUB - BORROW + j), :] = ends[j]
        heads = [out_b[strided(SUB - BORROW + j), :] for j in range(BORROW)]

        @pl.when(me == 1)
        def _():
            for j, val in enumerate([adh] + heads):
                send[b_msg, pl.ds(SUB * j, SUB), :] = val

        for seq in range(SUB):
            dbr_o[pl.ds(seq * n_tok, n_tok), :] = out_b[pl.ds(seq * pitch + SUB, n_tok), :].astype(BF16)
        if grads:
            *sums, sum_x = res[BORROW:]
            sum_x = sum_x + sum(ends) - sum(heads)

            @pl.when(lax.rem(b_step, n_tiles) == 0)
            def _():
                gw_o[...] = jnp.zeros_like(gw_o)
                sb_o[...] = jnp.zeros_like(sb_o)

            for n, val in enumerate([sum_x] + sums + [sum_a, sum_i, sum_p]):
                sb_o[0, pl.ds(n * SUB, SUB), :] += val
            gw_o[0] += lax.dot_general(s_c16[b_slot], d_16[...], TOK, preferred_element_type=F32)

        @pl.when(me == 1)
        def _():
            message(b_msg).start()

    @pl.when(jnp.logical_and(f_on, me == 0))
    def _():
        message(f_msg).wait_send()


def middle(px, py, dm, pos_rep, par, w_gate, grads, collective_id):
    n_rows, width = px.shape
    n_tok = pos_rep.shape[1] // SUB
    tile = SUB * n_tok
    n_tiles, n_chunks = n_rows // tile, width // LANES
    n_steps = n_tiles * n_chunks

    def f_of(s):
        return jnp.clip(s - lax.axis_index("cp"), 0, n_steps - 1)

    def b_of(s):
        return jnp.clip(s - 2 + lax.axis_index("cp"), 0, n_steps - 1)

    def spec(shape, of, index):
        def index_map(s):
            k = of(s)
            return index(k // n_tiles, k % n_tiles)

        return pl.BlockSpec(shape, index_map)

    big = lambda of: spec((tile, LANES), of, lambda c, t: (t, c))
    per_chunk = lambda of, *shape: spec((1,) + shape, of, lambda c, t: (c, 0, 0))
    in_specs = [pl.BlockSpec((n_tiles,) + pos_rep.shape[1:], lambda s: (0, 0, 0)), pl.BlockSpec(par.shape, lambda s: (0, 0)), pl.BlockSpec(w_gate.shape, lambda s: (0, 0, 0))]
    in_specs += [big(f_of)] * 3
    out_specs = [big(f_of), big(f_of), big(b_of)]
    out_shape = [jax.ShapeDtypeStruct((n_rows, width), BF16)] * 3
    if grads:
        extra = ((b_of, LANES, 2 * LANES), (f_of, SUB, LANES), (b_of, N_SUMS * SUB, LANES))
        out_specs += [per_chunk(*e) for e in extra]
        out_shape += [jax.ShapeDtypeStruct((n_chunks,) + e[1:], F32) for e in extra]
    pitched = pltpu.VMEM((SUB * (n_tok + SUB), LANES), F32)
    flat = pltpu.VMEM((tile, LANES), F32)
    slots = pltpu.VMEM((SLOTS, tile, LANES), F32)
    small = pltpu.VMEM((SLOTS if grads else 1, tile if grads else SUB, LANES), F32)
    scratch = [
        slots, slots, pltpu.VMEM((SLOTS, tile + SUB, LANES), F32), slots, slots, slots, slots, pltpu.VMEM((SLOTS, tile, LANES), BF16), small,
        pltpu.VMEM((SLOTS if grads else 1, tile + BORROW * SUB if grads else SUB, LANES), F32),
        pitched, pitched, pitched, flat, flat, pitched, pitched, pltpu.VMEM((SUB * (n_tok + SUB) + SUB, LANES), F32), flat, pltpu.VMEM((tile, 2 * LANES), BF16), flat,
        *[pltpu.VMEM((MSG_SLOTS, TAPS * SUB, LANES), F32)] * 2, *[pltpu.SemaphoreType.DMA((MSG_SLOTS,))] * 2]
    return pl.pallas_call(
        functools.partial(middle_kernel, n_steps, n_tiles, n_tok, grads),
        grid=(n_steps + 2,), in_specs=in_specs, out_specs=out_specs, out_shape=out_shape, scratch_shapes=scratch,
        name="middle",
        cost_estimate=pl.CostEstimate(flops=n_rows * width * 1500, bytes_accessed=n_rows * width * 18, transcendentals=n_rows * width * 8),
        compiler_params=pltpu.CompilerParams(collective_id=collective_id, has_side_effects=True, vmem_limit_bytes=VMEM_LIMIT, dimension_semantics=("arbitrary",)),
    )(pos_rep, par, w_gate, px, py, dm)


NORM_EPS = 1e-6
UNIT = 4 * SUB
IN_SPECS = (P(None, "cp", None), P(None, "cp", None), P(None, "cp"), P(), P(None, "tp"), P("tp"), P(None, "tp"), P("tp"), P(None, "tp"), P("tp"), P("tp", None, None), P("tp"), P("tp", None, None), P("tp"), P("tp"), P("tp", None), P())
OUT_SPECS = (P(None, "cp", None), P(None, "cp", None), P(), P(None, "tp"), P("tp"), P(None, "tp"), P("tp"), P(None, "tp"), P("tp"), P("tp", None, None), P("tp"), P("tp", None, None), P("tp"), P("tp"), P("tp", None), P())


def params_of(*semantics):
    return pltpu.CompilerParams(vmem_limit_bytes=VMEM_LIMIT, dimension_semantics=semantics)


def norm_kernel(x_ref, scale_ref, n_ref):
    rows, width = 4 * SUB, x_ref.shape[1]
    tiles = [pl.ds(n * LANES, LANES) for n in range(width // LANES)]

    def unit(u, _):
        here = pl.ds(pl.multiple_of(u * rows, rows), rows)
        square = jnp.zeros((rows, LANES), F32)
        for cols in tiles:
            x = x_ref[here, cols].astype(F32)
            square = square + x * x
        inv = jnp.broadcast_to(lax.rsqrt(jnp.sum(square, axis=-1, keepdims=True) / width + NORM_EPS), (rows, LANES))
        for cols in tiles:
            n_ref[here, cols] = (x_ref[here, cols].astype(F32) * inv * scale_ref[:, cols]).astype(BF16)
        return 0

    lax.fori_loop(0, x_ref.shape[0] // rows, unit, 0)


def normalize(x, scale):
    rows, width = x.shape
    tile = 512
    return pl.pallas_call(
        norm_kernel, grid=(rows // tile,), name="normalize",
        in_specs=[pl.BlockSpec((tile, width), lambda i: (i, 0)), pl.BlockSpec((1, width), lambda i: (0, 0))],
        out_specs=pl.BlockSpec((tile, width), lambda i: (i, 0)), out_shape=jax.ShapeDtypeStruct(x.shape, BF16),
        cost_estimate=pl.CostEstimate(flops=rows * width * 600, bytes_accessed=4 * rows * width, transcendentals=rows),
        compiler_params=params_of("arbitrary"),
    )(x, scale)


def plain_up_kernel(n_weights, flip, lhs, *refs):
    for w, out in zip(refs[:n_weights], refs[n_weights:]):
        out[...] = lax.dot_general(lhs[...], w[...], CHAN if flip else ROW, preferred_element_type=F32)


def plain_up(lhs, weights, flip):
    rows, depth = lhs.shape
    width = weights[0].shape[0 if flip else 1]
    n = len(weights)
    bm, bn = 1024, 512 // n
    w_spec = pl.BlockSpec((bn, depth), lambda j, i: (j, 0)) if flip else pl.BlockSpec((depth, bn), lambda j, i: (0, j))
    return pl.pallas_call(
        functools.partial(plain_up_kernel, n, flip), grid=(width // bn, rows // bm), name="plain_up",
        in_specs=[pl.BlockSpec((bm, depth), lambda j, i: (i, 0))] + [w_spec] * n,
        out_specs=[pl.BlockSpec((bm, bn), lambda j, i: (i, j))] * n, out_shape=[jax.ShapeDtypeStruct((rows, width), F32)] * n,
        cost_estimate=pl.CostEstimate(flops=2 * n * rows * width * depth, bytes_accessed=4 * rows * depth, transcendentals=0),
        compiler_params=params_of("arbitrary", "arbitrary"),
    )(lhs, *weights)


def up_kernel(n_weights, n_parts, flip, lhs, *refs):
    parts = [refs[n_parts * w:n_parts * (w + 1)] for w in range(n_weights)]
    outs, held = refs[n_parts * n_weights:-1], refs[-1]
    outs, stored = outs[:n_weights], outs[n_weights:]
    me = lax.axis_index("cp")
    j = pl.program_id(1)
    cols = outs[0].shape[1]

    @pl.when(pl.program_id(0) == 0)
    def _():
        for w, part in enumerate(parts):
            mine = pl.ds(w * cols, cols)
            for q, ref in enumerate(part):
                depth = ref.shape[1] if flip else ref.shape[0]
                place = lax.rem(me * 2 + q, n_parts)
                at = pl.ds(pl.multiple_of(place * depth, depth), depth)
                val = ref[...].astype(BF16)
                if flip:
                    held[j, mine, at] = val
                else:
                    held[j, at, mine] = val
                stored[w][(slice(None), at) if flip else (at, slice(None))] = val

    res = lax.dot_general(lhs[...], held[j], CHAN if flip else ROW, preferred_element_type=F32)
    for w, out in enumerate(outs):
        out[...] = res[:, w * cols:(w + 1) * cols]


def up(lhs, weights, flip, n_rows):
    depth = lhs.shape[1]
    n, n_parts = len(weights), len(weights[0])
    width = weights[0][0][0].shape[-2 if flip else -1]
    bm, bn = 1024, 256 // n
    steps = width // bn

    def block(size, lead, of):
        shape = (bn, size) if flip else (size, bn)
        return pl.BlockSpec((None,) * len(lead) + shape, lambda i, j: lead + ((of(i, j), 0) if flip else (0, of(i, j))))

    def once(i, j):
        return jnp.where(i == 0, j, steps - 1)

    out_specs = [pl.BlockSpec((bm, bn), lambda i, j: (i, j))] * n
    out_shape = [jax.ShapeDtypeStruct((n_rows, width), F32)] * n
    out_specs += [block(depth, (), once)] * n
    out_shape += [jax.ShapeDtypeStruct((width, depth) if flip else (depth, width), BF16)] * n
    return pl.pallas_call(
        functools.partial(up_kernel, n, n_parts, flip), grid=(n_rows // bm, steps), name="up",
        in_specs=[pl.BlockSpec((bm, depth), lambda i, j: (i, 0))] + [block(depth // n_parts, lead, once) for part in weights for _, lead in part],
        out_specs=out_specs, out_shape=out_shape,
        scratch_shapes=[pltpu.VMEM((steps, n * bn, depth) if flip else (steps, depth, n * bn), BF16)],
        cost_estimate=pl.CostEstimate(flops=2 * n * n_rows * width * depth, bytes_accessed=4 * n_rows * depth, transcendentals=0),
        compiler_params=params_of("arbitrary", "arbitrary"),
    )(lhs, *[array for part in weights for array, _ in part])


def finish_rows(rows, first, dn_ref, x_ref, gz_ref, scale_ref, grad_ref, sum_ref):
    width = x_ref.shape[1]
    tiles = [pl.ds(n * LANES, LANES) for n in range(width // LANES)]
    here = pl.ds(pl.multiple_of(first, rows), rows)
    square = cross = jnp.zeros((rows, LANES), F32)
    for cols in tiles:
        x = x_ref[here, cols].astype(F32)
        square = square + x * x
        cross = cross + x * (dn_ref[here, cols] * scale_ref[:, cols])
    inv = lax.rsqrt(jnp.sum(square, axis=-1, keepdims=True) / width + NORM_EPS)
    inv_b = jnp.broadcast_to(inv, (rows, LANES))
    pull = jnp.broadcast_to(inv * inv * inv * (jnp.sum(cross, axis=-1, keepdims=True) / width), (rows, LANES))
    for cols in tiles:
        x = x_ref[here, cols].astype(F32)
        gz = gz_ref[here, cols].astype(F32)
        dn = dn_ref[here, cols] * inv_b
        grad_ref[here, cols] = (gz + dn * scale_ref[:, cols] - x * pull).astype(BF16)
        for which, val in enumerate((dn * x, gz)):
            sum_ref[which, :, cols] += sum(val[SUB * r:SUB * (r + 1)] for r in range(rows // SUB))


def z_kernel(n_pairs, n_moved, *refs):
    left, right = refs[:n_pairs], refs[n_pairs:2 * n_pairs]
    x_ref, bias_ref, *rows_in = refs[2 * n_pairs:2 * n_pairs + 6]
    moved, (out_ref, *rows_out), placed = refs[2 * n_pairs + 6:-3 - n_moved], refs[-3 - n_moved:len(refs) - n_moved], refs[len(refs) - n_moved:]
    for src, dst in zip(moved, placed):
        dst[...] = src[...]

    @pl.when(jnp.logical_and(pl.program_id(0) == 0, pl.program_id(1) == 0))
    def _():
        rows_out[-1][...] = jnp.zeros_like(rows_out[-1])

    acc = x_ref[...].astype(F32) + bias_ref[...]
    for lhs, rhs in zip(left, right):
        acc = acc + jnp.dot(lhs[...], rhs[...], preferred_element_type=F32)
    out_ref[...] = acc.astype(BF16)
    for first in range(0, rows_in[0].shape[0], UNIT):
        finish_rows(UNIT, first, *rows_in, *rows_out)


def outputs(left, right, x, bias, dn, gz, scale, moved):
    rows, width = dn.shape
    depth = left[0].shape[1]
    bm, bn = 1024, 512
    n_row, n_col = rows // bm, width // bn
    share = rows // (n_row * n_col)
    tile = pl.BlockSpec((bm, bn), lambda i, j: (i, j))
    line = pl.BlockSpec((share, width), lambda i, j: (i * n_col + j, 0))
    in_specs = [pl.BlockSpec((bm, depth), lambda i, j: (i, 0))] * len(left) + [pl.BlockSpec((depth, bn), lambda i, j: (0, j))] * len(right)
    in_specs += [tile, pl.BlockSpec((1, bn), lambda i, j: (0, j)), line, line, line, pl.BlockSpec((1, width), lambda i, j: (0, 0))]
    n_move = 16
    passing = [pl.BlockSpec((v.shape[0] // n_move, v.shape[1]), lambda i, j: (jnp.minimum(i * n_col + j, n_move - 1), 0)) for v in moved]
    return pl.pallas_call(
        functools.partial(z_kernel, len(left), len(moved)), grid=(n_row, n_col), name="outputs",
        in_specs=in_specs + passing, out_specs=[tile, line, pl.BlockSpec((2, SUB, width), lambda i, j: (0, 0, 0))] + passing,
        out_shape=[jax.ShapeDtypeStruct(x.shape, BF16)] * 2 + [jax.ShapeDtypeStruct((2, SUB, width), F32)] + [jax.ShapeDtypeStruct(v.shape, v.dtype) for v in moved],
        cost_estimate=pl.CostEstimate(flops=2 * len(right) * rows * width * depth, bytes_accessed=rows * width * 20, transcendentals=rows),
        compiler_params=params_of("arbitrary", "arbitrary"),
    )(*left, *right, x, bias, dn, x, gz, scale, *moved)


def tail_kernel(z_ref, bias_ref, dn_ref, x_ref, gz_ref, scale_ref, _, __, out_ref, grad_ref, sum_ref):
    @pl.when(pl.program_id(0) == 0)
    def _():
        sum_ref[...] = jnp.zeros_like(sum_ref)

    def unit(u, _):
        here = pl.ds(pl.multiple_of(u * UNIT, UNIT), UNIT)
        for n in range(out_ref.shape[1] // LANES):
            cols = pl.ds(n * LANES, LANES)
            out_ref[here, cols] = (x_ref[here, cols].astype(F32) + (z_ref[here, cols] + bias_ref[:, cols])).astype(BF16)
        finish_rows(UNIT, u * UNIT, dn_ref, x_ref, gz_ref, scale_ref, grad_ref, sum_ref)
        return 0

    lax.fori_loop(0, out_ref.shape[0] // UNIT, unit, 0)


def tail_outputs(z_sum, bias, dn, x, gz, scale, z, grad_x, first_row):
    rows, width = dn.shape
    share = 128
    skip = first_row // share
    near = pl.BlockSpec((share, width), lambda i: (i, 0))
    line = pl.BlockSpec((share, width), lambda i: (i + skip, 0))
    whole = pl.BlockSpec((1, width), lambda i: (0, 0))
    here = pl.BlockSpec(memory_space=pl.ANY)
    return pl.pallas_call(
        tail_kernel, grid=(rows // share,), name="tail_outputs",
        in_specs=[near, whole, near, line, line, whole, here, here], out_specs=[line, line, pl.BlockSpec((2, SUB, width), lambda i: (0, 0, 0))],
        out_shape=[jax.ShapeDtypeStruct(x.shape, BF16)] * 2 + [jax.ShapeDtypeStruct((2, SUB, width), F32)], input_output_aliases={6: 0, 7: 1},
        cost_estimate=pl.CostEstimate(flops=rows * width * 1500, bytes_accessed=rows * width * 16, transcendentals=rows),
        compiler_params=params_of("arbitrary"),
    )(z_sum, bias, dn, x, gz, scale, z, grad_x)


def wide_kernel(n_pairs, flip, *refs):
    left, right, out_ref = refs[:n_pairs], refs[n_pairs:2 * n_pairs], refs[2 * n_pairs]

    def column(c, _):
        cols = pl.ds(pl.multiple_of(c * 256, 256), 256)
        acc = 0.0
        for lhs, rhs in zip(left, right):
            acc = acc + lax.dot_general(lhs[...], rhs[cols, :] if flip else rhs[:, cols], CHAN if flip else ROW, preferred_element_type=F32)
        out_ref[:, cols] = acc
        return 0

    lax.fori_loop(0, out_ref.shape[1] // 256, column, 0)


def wide_product(lefts, rights, flip, first_row, rows):
    depth = lefts[0].shape[1]
    width = rights[0].shape[0 if flip else 1]
    bm, bn = 1024, 512
    skip = first_row // bm
    n = len(lefts)
    return pl.pallas_call(
        functools.partial(wide_kernel, n, flip), grid=(rows // bm, width // bn), name="wide_product",
        in_specs=[pl.BlockSpec((bm, depth), lambda i, j: (i + skip, 0))] * n + [pl.BlockSpec((bn, depth), lambda i, j: (j, 0)) if flip else pl.BlockSpec((depth, bn), lambda i, j: (0, j))] * n,
        out_specs=pl.BlockSpec((bm, bn), lambda i, j: (i, j)), out_shape=jax.ShapeDtypeStruct((rows, width), F32),
        cost_estimate=pl.CostEstimate(flops=2 * n * rows * width * depth, bytes_accessed=450000000, transcendentals=0),
        compiler_params=params_of("arbitrary", "arbitrary"),
    )(*lefts, *rights)


def token_product(lhs, rhs):
    return lax.dot_general(lhs, rhs, TOK, preferred_element_type=F32)


def spread_positions(seg_pos):
    n_seq, n_tok = seg_pos.shape
    pos = jnp.swapaxes(seg_pos.reshape(n_seq // SUB, SUB, n_tok), 1, 2).reshape(n_seq // SUB, n_tok * SUB, 1)
    return jnp.broadcast_to(pos, (n_seq // SUB, n_tok * SUB, LANES))


def stack_params(b_x, b_y, conv_w, conv_b, b_a, b_i, a_param):
    rows = [b_x, b_y, *conv_w, conv_b, -b_a, -b_i]
    rows = [row.astype(F32) for row in rows] + [-8.0 * jax.nn.softplus(a_param)]
    return jnp.concatenate([jnp.stack(rows), jnp.zeros((16 - len(rows), a_param.shape[0]), F32)], axis=0)


def block_body(x_in, grad_z, seg_pos, norm_scale, w_x, b_x, w_y, b_y, conv_w, conv_b, w_a, b_a, w_i, b_i, a_param, w_out, b_out):
    me = lax.axis_index("cp")
    n_seq, n_tok, d_model = x_in.shape
    n_rows = n_seq * n_tok
    width = a_param.shape[0]
    x = x_in.reshape(n_rows, d_model)
    gz = grad_z.reshape(n_rows, d_model)
    scale = norm_scale.astype(F32).reshape(1, d_model)

    def swap_x(v):
        return lax.ppermute(v, "tp", [(j, j ^ 1) for j in range(4)])

    def swap_y(v):
        return lax.ppermute(v, "tp", [(j, j ^ 2) for j in range(4)])

    def swap_core(v):
        return lax.ppermute(v, "cp", [(0, 1), (1, 0)])

    tile = SUB * n_tok
    shared = n_rows - tile

    par = stack_params(b_x, b_y, conv_w, conv_b, b_a, b_i, a_param)
    w_gate = jnp.concatenate([w_a, w_i], axis=2)
    small = jnp.concatenate([par.reshape(-1), w_gate.astype(F32).reshape(-1)]).reshape(-1, LANES)

    def after(values, *before):
        return lax.optimization_barrier((values, before))[0]

    def quarter(w, axis, q):
        size = d_model // 4
        return lax.dynamic_slice_in_dim(w, (me * 2 + q) * size, size, axis).astype(F32)

    def to_neighbours(weights, axis, before):
        weights = after(weights, before)
        sent = [jnp.stack([quarter(w, axis, q) for w in weights]) for q in range(2)]
        return [swap_x(v) for v in sent], [swap_y(v) for v in sent]

    def cores(values):
        return values, [swap_core(v) for v in values]

    group_a = to_neighbours((w_x, w_y), 0, seg_pos)

    def unpack(s):
        flat = s.reshape(-1)
        return flat[:par.size].reshape(par.shape), lax.optimization_barrier(flat[par.size:]).reshape(w_gate.shape).astype(BF16)

    def onward(group):
        return [swap_y(group[0][0]), swap_x(group[1][1])]

    def quarters(side, n):
        own, other = side
        return [tuple((v, (k,)) for v in list(own) + list(other)) for k in range(n)]

    normed = normalize(x, 1.0 + scale)
    pos_rep = spread_positions(seg_pos)
    px, py = plain_up(normed, [w_x, w_y], False)
    group_b = to_neighbours((w_out,), 1, px)
    smalls = [lax.ppermute(after(small, px), "tp", [(j, j ^ far) for j in range(4)]) for far in range(1, 4)]
    dm, = plain_up(after(gz, px), [w_out], True)
    mixed, dpy, dbr, g_gate, s_y, s_b = middle(px, py, dm, pos_rep, par, w_gate, True, 0)
    g_w_out = token_product(mixed, gz)
    g_w_y = token_product(normed, dpy)
    group_a = after(group_a, g_w_out, g_w_y)
    side_x, side_y = [cores(values) for values in group_a]
    g_w_x = token_product(normed, after(dbr, g_w_y))
    diag_a = onward(after(group_a, g_w_x))

    s_y = jnp.sum(s_y, axis=1).reshape(1, width)
    s_b = jnp.swapaxes(jnp.sum(s_b.reshape(s_b.shape[0], N_SUMS, SUB, LANES), axis=2), 0, 1).reshape(N_SUMS, width)
    own_grads = lax.psum((g_w_x, g_w_y, g_w_out, g_gate), "cp")

    px_x, py_x, wx_x, wy_x = up(after(normed, g_w_x), quarters(side_x, 2), False, shared)
    px_y, py_y, wx_y, wy_y = up(after(normed, px_x), quarters(side_y, 2), False, shared)
    group_b = after(group_b, px_y)
    out_x, out_y = [cores(values) for values in group_b]
    diag_b = onward(group_b)
    dn_tail = wide_product(after([dbr, dpy], px_y), [w_x, w_y], True, shared, tile)
    smalls = after(smalls, dn_tail)
    dm_x, wo_x = up(after(gz, dn_tail), quarters(out_x, 1), True, shared)
    mixed_x, dpy_x, dbr_x = middle(px_x, py_x, dm_x, pos_rep, *unpack(smalls[0]), False, 1)
    dm_y, wo_y = up(after(gz, mixed_x), quarters(out_y, 1), True, shared)
    mixed_y, dpy_y, dbr_y = middle(px_y, py_y, dm_y, pos_rep, *unpack(smalls[1]), False, 1)
    diag_a, diag_b = after((diag_a, diag_b), mixed_y)
    diag_a, diag_b = cores(diag_a), cores(diag_b)
    z_tail = wide_product(after([mixed], mixed_y), [w_out], False, shared, tile)
    dn_sum, z_sum = lax.psum((dn_tail, z_tail), "tp")
    px_d, py_d, wx_d, wy_d = up(after(normed, z_tail), quarters(diag_a, 2), False, shared)
    dm_d, wo_d = up(after(gz, px_d), quarters(diag_b, 1), True, shared)
    mixed_d, dpy_d, dbr_d = middle(px_d, py_d, dm_d, pos_rep, *unpack(smalls[2]), False, 1)

    wx_all, wy_all, wo_all = [w_x, wx_x, wx_y, wx_d], [w_y, wy_x, wy_y, wy_d], [w_out, wo_x, wo_y, wo_d]
    dn = wide_product([dbr, dbr_x, dbr_y, dbr_d, dpy, dpy_x, dpy_y, dpy_d], wx_all + wy_all, True, 0, shared)
    bias = b_out.astype(F32).reshape(1, d_model)
    *tall, g_gate = own_grads
    lines = lax.psum(after(jnp.concatenate([s_y, s_b]), mixed_d), "cp")
    z_out, grad_x, sums_x, *tall = outputs([mixed, mixed_x, mixed_y, mixed_d], wo_all, x, bias, after(dn, lines), gz, 1.0 + scale, tall)
    g_w_x, g_w_y, g_w_out = tall
    z_out, grad_x, sums_t = tail_outputs(z_sum, bias, dn_sum, x, gz, 1.0 + scale, z_out, grad_x, shared)
    z_out = z_out.reshape(x_in.shape)
    sums_x = jnp.sum(sums_x + sums_t, axis=1)

    sums_x = lax.psum(sums_x, "cp")
    s_y, s_b = lines[0], lines[1:]
    g_a = -8.0 * s_b[8] * jax.nn.sigmoid(a_param)
    return (z_out, grad_x.reshape(x_in.shape), sums_x[0], g_w_x, s_b[0], g_w_y, s_y, s_b[1:5], s_b[5], g_gate[:, :, :LANES], s_b[6], g_gate[:, :, LANES:], s_b[7], g_a, g_w_out, sums_x[1])


def solution(mesh):
    return jax.shard_map(block_body, mesh=mesh, in_specs=IN_SPECS, out_specs=OUT_SPECS, check_vma=False)
```

```python
import functools
import jax
import jax.numpy as jnp
from jax import lax
from jax.experimental import pallas as pl
from jax.experimental.pallas import tpu as pltpu
from jax.sharding import PartitionSpec as P

F32 = jnp.float32
BF16 = jnp.bfloat16
TAPS = 4
SUB = 8
LANES = 128
SLOTS = 3
MSG_SLOTS = 4
VMEM_LIMIT = 60 << 20
ROW = (((1,), (0,)), ((), ()))
CHAN = (((1,), (1,)), ((), ()))
TOK = (((0,), (0,)), ((), ()))
GELU_K0 = 1.5957691216057308
GELU_K1 = GELU_K0 * 0.044715
N_SUMS = 9
SPAN = 64
N_PAR = 10
BORROW = TAPS - 1


def param_rows(ref):
    return [jnp.broadcast_to(ref[pl.ds(k, 1), :], (SUB, LANES)) for k in range(N_PAR)]


def middle_kernel(n_steps, n_tiles, n_tok, grads, pos_w, par_w, wg_w, px, py, dm, *rest):
    if grads:
        mix_o, dpy_o, dbr_o, gw_o, sy_o, sb_o = rest[:6]
        rest = rest[6:]
    else:
        mix_o, dpy_o, dbr_o = rest[:3]
        rest = rest[3:]
    (s_g, s_a, s_h, s_k, s_ra, s_ui, s_mi, s_c16, s_r, s_xb, in_x, in_y, in_d, pre_a, pre_i, out_m, out_y, out_b, d_c, d_16, d_gate, send, recv, send_sem, recv_sem) = rest
    pitch = n_tok + SUB
    me = lax.axis_index("cp")
    step = pl.program_id(0)
    f_step = step - me
    b_step = step - 2 + me
    f_on = jnp.logical_and(f_step >= 0, f_step < n_steps)
    b_on = jnp.logical_and(b_step >= 0, b_step < n_steps)
    f_slot = lax.rem(f_step + SLOTS, SLOTS)
    b_slot = lax.rem(b_step + SLOTS, SLOTS)
    f_msg = lax.rem(f_step + MSG_SLOTS, MSG_SLOTS)
    b_msg = lax.rem(b_step + MSG_SLOTS, MSG_SLOTS)
    n_groups = n_tok // SPAN
    f_at, b_at = [jnp.clip(v, 0, n_steps - 1) for v in (f_step, b_step)]
    pos_f, pos_b = [pos_w.at[lax.rem(v, n_tiles)] for v in (f_at, b_at)]
    par_f, par_b = [par_w.at[:, pl.ds(pl.multiple_of(v // n_tiles * LANES, LANES), LANES)] for v in (f_at, b_at)]
    wg_f, wg_b = [wg_w.at[v // n_tiles] for v in (f_at, b_at)]

    def message(slot):
        return pltpu.make_async_remote_copy(src_ref=send.at[slot], dst_ref=recv.at[slot], send_sem=send_sem.at[slot], recv_sem=recv_sem.at[slot], device_id={"cp": 1 - me}, device_id_type=pl.DeviceIdType.MESH)

    @pl.when(step == 0)
    def _():
        barrier = pltpu.get_barrier_semaphore()
        pl.semaphore_signal(barrier, inc=1, device_id={"cp": 1 - me}, device_id_type=pl.DeviceIdType.MESH)
        pl.semaphore_wait(barrier, 1)

    def row8(base):
        return pl.ds(pl.multiple_of(base, SUB), SUB)

    def pair(t):
        return pl.ds(pl.multiple_of(t * SUB, 2 * SUB), 2 * SUB)

    def strided(t):
        return pl.ds(t, SUB, stride=pitch)

    @pl.when(jnp.logical_and(f_on, me == 1))
    def _():
        message(f_msg).wait_recv()

    @pl.when(f_on)
    def _():
        for seq in range(SUB):
            in_x[pl.ds(seq * pitch, n_tok), :] = px[pl.ds(seq * n_tok, n_tok), :]
        b_x, b_y, *taps, c_b, nb_a, nb_i, nsp = param_rows(par_f)
        h_in, *halo = [jnp.where(me == 0, 0.0, recv[f_msg, pl.ds(SUB * j, SUB), :]) for j in range(TAPS)]
        xb_r = s_xb.at[f_slot] if grads else None
        if grads:
            for j in range(BORROW):
                xb_r[pl.ds(SUB * j, SUB), :] = halo[j]
        c16_r, g_r, a_r, h_r, k_r = s_c16.at[f_slot], s_g.at[f_slot], s_a.at[f_slot], s_h.at[f_slot], s_k.at[f_slot]
        ra_r, ui_r, mi_r = s_ra.at[f_slot], s_ui.at[f_slot], s_mi.at[f_slot]
        r_r = s_r.at[f_slot] if grads else None

        def conv_body(grp, past):
            past = list(past)
            pend = None
            for j in range(SPAN):
                t = grp * SPAN + j
                now = (in_x[strided(t), :] + b_x).astype(BF16).astype(F32)
                pos = pos_f[row8(t * SUB), :]
                acc = c_b + now * taps[0]
                for k in range(1, TAPS):
                    acc = acc + jnp.where(pos >= k, past[-k], 0.0) * taps[k]
                if grads:
                    xb_r[row8((t + BORROW) * SUB), :] = now
                if pend is None:
                    pend = acc
                else:
                    c16_r[pair(t - 1), :] = jnp.concatenate([pend, acc]).astype(BF16)
                    pend = None
                past = past[1:] + [now]
            return tuple(past)

        last3 = lax.fori_loop(0, n_groups, conv_body, tuple(halo))
        pre = jnp.dot(c16_r[...], wg_f[...], preferred_element_type=F32)
        for seq in range(SUB):
            for src, dst in ((py, in_y), (dm, in_d)):
                dst[pl.ds(seq * pitch, n_tok), :] = src[pl.ds(seq * n_tok, n_tok), :]
        pre_a[...] = pre[:, :LANES]
        pre_i[...] = pre[:, LANES:]
        h_r[pl.ds(0, SUB), :] = h_in

        def gate_body(grp, carry):
            h, sum_y = carry
            for j in range(SPAN):
                t = grp * SPAN + j
                rows = row8(t * SUB)
                if j % 2:
                    c = both[SUB:]
                else:
                    both = c16_r[pair(t), :].astype(F32)
                    c = both[:SUB]
                reset = pos_f[rows, :] == 0
                r = 1.0 / (1.0 + jnp.exp(nb_a - pre_a[rows, :]))
                i = 1.0 / (1.0 + jnp.exp(nb_i - pre_i[rows, :]))
                la = nsp * r
                a = jnp.exp(la)
                th = jnp.tanh(jnp.abs(la))
                twice, more = th + th, 1.0 + th
                root = lax.rsqrt(jnp.maximum(twice * more, 1e-37))
                rm = more * root
                m = jnp.where(reset, 1.0, twice * root)
                ic = i * c
                k = a * ic * rm
                a = jnp.where(reset, 0.0, a)
                u = m * ic
                h = a * h + u
                h_r[row8(t * SUB + SUB), :] = h
                a_r[rows, :] = a
                k_r[rows, :] = k
                ra_r[rows, :] = la - la * r
                ui_r[rows, :] = u - u * i
                mi_r[rows, :] = m * i
                if grads:
                    r_r[rows, :] = r
                v = in_y[strided(t), :] + b_y
                v2 = v * v
                cdf = jax.nn.sigmoid(v * (GELU_K0 + GELU_K1 * v2))
                y = v * cdf
                dy = cdf + (y - y * cdf) * (GELU_K0 + (3.0 * GELU_K1) * v2)
                d = in_d[strided(t), :]
                g_r[rows, :] = d * y
                out_m[strided(t), :] = h * y
                d_py = d * h * dy
                out_y[strided(t), :] = d_py
                if grads:
                    sum_y = sum_y + d_py
            return h, sum_y

        h_end, sum_y = lax.fori_loop(0, n_groups, gate_body, (h_in, jnp.zeros((SUB, LANES), F32)))
        if grads:
            @pl.when(lax.rem(f_step, n_tiles) == 0)
            def _():
                sy_o[...] = jnp.zeros_like(sy_o)

            sy_o[...] += sum_y

        @pl.when(me == 0)
        def _():
            for j, val in enumerate((h_end,) + last3):
                send[f_msg, pl.ds(SUB * j, SUB), :] = val

        for seq in range(SUB):
            mix_o[pl.ds(seq * n_tok, n_tok), :] = out_m[pl.ds(seq * pitch, n_tok), :].astype(BF16)
            dpy_o[pl.ds(seq * n_tok, n_tok), :] = out_y[pl.ds(seq * pitch, n_tok), :].astype(BF16)

        @pl.when(me == 0)
        def _():
            message(f_msg).start()

    @pl.when(jnp.logical_and(b_on, me == 0))
    def _():
        message(b_msg).wait_recv()

    @pl.when(jnp.logical_and(jnp.logical_and(b_step >= 1, b_step <= n_steps), me == 1))
    def _():
        message(lax.rem(b_step - 1 + MSG_SLOTS, MSG_SLOTS)).wait_send()

    @pl.when(b_on)
    def _():
        _, _, *taps, _, _, _, _ = param_rows(par_b)
        carry_in, *tail = [jnp.where(me == 1, 0.0, recv[b_msg, pl.ds(SUB * j, SUB), :]) for j in range(TAPS)]
        g_r, a_r, h_r, k_r = s_g.at[b_slot], s_a.at[b_slot], s_h.at[b_slot], s_k.at[b_slot]
        ra_r, ui_r, mi_r = s_ra.at[b_slot], s_ui.at[b_slot], s_mi.at[b_slot]
        r_r = s_r.at[b_slot] if grads else None
        xb_r = s_xb.at[b_slot] if grads else None
        zero = jnp.zeros((SUB, LANES), F32)

        def scan_body(back, carry):
            grp = n_groups - 1 - back
            adh, sum_a, sum_i, sum_p = carry
            pend = None
            for j in reversed(range(SPAN)):
                t = grp * SPAN + j
                rows = row8(t * SUB)
                dh = g_r[rows, :] + adh
                adh = a_r[rows, :] * dh
                dlog = adh * (h_r[rows, :] - k_r[rows, :])
                dpa = dlog * ra_r[rows, :]
                dpi = dh * ui_r[rows, :]
                d_c[rows, :] = dh * mi_r[rows, :]
                if grads:
                    sum_a = sum_a + dpa
                    sum_i = sum_i + dpi
                    sum_p = sum_p + dlog * r_r[rows, :]
                if pend is None:
                    pend = (dpa, dpi)
                else:
                    d_16[pair(t), :LANES] = jnp.concatenate([dpa, pend[0]]).astype(BF16)
                    d_16[pair(t), LANES:] = jnp.concatenate([dpi, pend[1]]).astype(BF16)
                    pend = None
            return adh, sum_a, sum_i, sum_p

        adh, sum_a, sum_i, sum_p = lax.fori_loop(0, n_groups, scan_body, (carry_in, zero, zero, zero))
        d_gate[...] = lax.dot_general(d_16[...], wg_b[...], CHAN, preferred_element_type=F32)

        def conv_body(grp, carry):
            ahead, sums = list(carry[:BORROW]), list(carry[BORROW:])
            for j in range(SPAN):
                s = grp * SPAN + j
                rows = row8(s * SUB)
                pos = pos_b[rows, :]
                dc = d_c[rows, :] + d_gate[rows, :]
                masked = [dc] + [jnp.where(pos >= k, dc, 0.0) for k in range(1, TAPS)]
                part = [val * tap for val, tap in zip(masked, taps)]
                done = ahead[0] + part[-1]
                out_b[strided(s + SUB - BORROW), :] = done
                ahead = [ahead[k] + part[-1 - k] for k in range(1, BORROW)] + [part[0]]
                if grads:
                    for k in range(TAPS):
                        sums[k] = sums[k] + masked[k] * xb_r[row8((s + BORROW - k) * SUB), :]
                    sums[TAPS] = sums[TAPS] + dc
                    sums[-1] = sums[-1] + done
            return tuple(ahead + sums)

        res = lax.fori_loop(0, n_groups, conv_body, (zero,) * (BORROW + (TAPS + 2 if grads else 0)))
        ends = [res[j] + tail[j] for j in range(BORROW)]
        for j in range(BORROW):
            out_b[strided(n_tok + SUB - BORROW + j), :] = ends[j]
        heads = [out_b[strided(SUB - BORROW + j), :] for j in range(BORROW)]

        @pl.when(me == 1)
        def _():
            for j, val in enumerate([adh] + heads):
                send[b_msg, pl.ds(SUB * j, SUB), :] = val

        for seq in range(SUB):
            dbr_o[pl.ds(seq * n_tok, n_tok), :] = out_b[pl.ds(seq * pitch + SUB, n_tok), :].astype(BF16)
        if grads:
            *sums, sum_x = res[BORROW:]
            sum_x = sum_x + sum(ends) - sum(heads)

            @pl.when(lax.rem(b_step, n_tiles) == 0)
            def _():
                gw_o[...] = jnp.zeros_like(gw_o)
                sb_o[...] = jnp.zeros_like(sb_o)

            for n, val in enumerate([sum_x] + sums + [sum_a, sum_i, sum_p]):
                sb_o[0, pl.ds(n * SUB, SUB), :] += val
            gw_o[0] += lax.dot_general(s_c16[b_slot], d_16[...], TOK, preferred_element_type=F32)

        @pl.when(me == 1)
        def _():
            message(b_msg).start()

    @pl.when(jnp.logical_and(f_on, me == 0))
    def _():
        message(f_msg).wait_send()


def middle(px, py, dm, pos_rep, par, w_gate, grads, collective_id):
    n_rows, width = px.shape
    n_tok = pos_rep.shape[1] // SUB
    tile = SUB * n_tok
    n_tiles, n_chunks = n_rows // tile, width // LANES
    n_steps = n_tiles * n_chunks

    def f_of(s):
        return jnp.clip(s - lax.axis_index("cp"), 0, n_steps - 1)

    def b_of(s):
        return jnp.clip(s - 2 + lax.axis_index("cp"), 0, n_steps - 1)

    def spec(shape, of, index):
        def index_map(s):
            k = of(s)
            return index(k // n_tiles, k % n_tiles)

        return pl.BlockSpec(shape, index_map)

    big = lambda of: spec((tile, LANES), of, lambda c, t: (t, c))
    per_chunk = lambda of, *shape: spec((1,) + shape, of, lambda c, t: (c, 0, 0))
    in_specs = [pl.BlockSpec((n_tiles,) + pos_rep.shape[1:], lambda s: (0, 0, 0)), pl.BlockSpec(par.shape, lambda s: (0, 0)), pl.BlockSpec(w_gate.shape, lambda s: (0, 0, 0))]
    in_specs += [big(f_of)] * 3
    out_specs = [big(f_of), big(f_of), big(b_of)]
    out_shape = [jax.ShapeDtypeStruct((n_rows, width), BF16)] * 3
    if grads:
        extra = ((b_of, LANES, 2 * LANES), (f_of, SUB, LANES), (b_of, N_SUMS * SUB, LANES))
        out_specs += [per_chunk(*e) for e in extra]
        out_shape += [jax.ShapeDtypeStruct((n_chunks,) + e[1:], F32) for e in extra]
    pitched = pltpu.VMEM((SUB * (n_tok + SUB), LANES), F32)
    flat = pltpu.VMEM((tile, LANES), F32)
    slots = pltpu.VMEM((SLOTS, tile, LANES), F32)
    small = pltpu.VMEM((SLOTS if grads else 1, tile if grads else SUB, LANES), F32)
    scratch = [
        slots, slots, pltpu.VMEM((SLOTS, tile + SUB, LANES), F32), slots, slots, slots, slots, pltpu.VMEM((SLOTS, tile, LANES), BF16), small,
        pltpu.VMEM((SLOTS if grads else 1, tile + BORROW * SUB if grads else SUB, LANES), F32),
        pitched, pitched, pitched, flat, flat, pitched, pitched, pltpu.VMEM((SUB * (n_tok + SUB) + SUB, LANES), F32), flat, pltpu.VMEM((tile, 2 * LANES), BF16), flat,
        *[pltpu.VMEM((MSG_SLOTS, TAPS * SUB, LANES), F32)] * 2, *[pltpu.SemaphoreType.DMA((MSG_SLOTS,))] * 2]
    return pl.pallas_call(
        functools.partial(middle_kernel, n_steps, n_tiles, n_tok, grads),
        grid=(n_steps + 2,), in_specs=in_specs, out_specs=out_specs, out_shape=out_shape, scratch_shapes=scratch,
        name="middle",
        cost_estimate=pl.CostEstimate(flops=n_rows * width * 1500, bytes_accessed=n_rows * width * 18, transcendentals=n_rows * width * 8),
        compiler_params=pltpu.CompilerParams(collective_id=collective_id, has_side_effects=True, vmem_limit_bytes=VMEM_LIMIT, dimension_semantics=("arbitrary",)),
    )(pos_rep, par, w_gate, px, py, dm)


NORM_EPS = 1e-6
UNIT = 4 * SUB
IN_SPECS = (P(None, "cp", None), P(None, "cp", None), P(None, "cp"), P(), P(None, "tp"), P("tp"), P(None, "tp"), P("tp"), P(None, "tp"), P("tp"), P("tp", None, None), P("tp"), P("tp", None, None), P("tp"), P("tp"), P("tp", None), P())
OUT_SPECS = (P(None, "cp", None), P(None, "cp", None), P(), P(None, "tp"), P("tp"), P(None, "tp"), P("tp"), P(None, "tp"), P("tp"), P("tp", None, None), P("tp"), P("tp", None, None), P("tp"), P("tp"), P("tp", None), P())


def params_of(*semantics):
    return pltpu.CompilerParams(vmem_limit_bytes=VMEM_LIMIT, dimension_semantics=semantics)


def norm_kernel(x_ref, scale_ref, n_ref):
    rows, width = 4 * SUB, x_ref.shape[1]
    tiles = [pl.ds(n * LANES, LANES) for n in range(width // LANES)]

    def unit(u, _):
        here = pl.ds(pl.multiple_of(u * rows, rows), rows)
        square = jnp.zeros((rows, LANES), F32)
        for cols in tiles:
            x = x_ref[here, cols].astype(F32)
            square = square + x * x
        inv = jnp.broadcast_to(lax.rsqrt(jnp.sum(square, axis=-1, keepdims=True) / width + NORM_EPS), (rows, LANES))
        for cols in tiles:
            n_ref[here, cols] = (x_ref[here, cols].astype(F32) * inv * scale_ref[:, cols]).astype(BF16)
        return 0

    lax.fori_loop(0, x_ref.shape[0] // rows, unit, 0)


def normalize(x, scale):
    rows, width = x.shape
    tile = 512
    return pl.pallas_call(
        norm_kernel, grid=(rows // tile,), name="normalize",
        in_specs=[pl.BlockSpec((tile, width), lambda i: (i, 0)), pl.BlockSpec((1, width), lambda i: (0, 0))],
        out_specs=pl.BlockSpec((tile, width), lambda i: (i, 0)), out_shape=jax.ShapeDtypeStruct(x.shape, BF16),
        cost_estimate=pl.CostEstimate(flops=rows * width * 600, bytes_accessed=4 * rows * width, transcendentals=rows),
        compiler_params=params_of("arbitrary"),
    )(x, scale)


def plain_up_kernel(n_weights, flip, lhs, *refs):
    for w, out in zip(refs[:n_weights], refs[n_weights:]):
        out[...] = lax.dot_general(lhs[...], w[...], CHAN if flip else ROW, preferred_element_type=F32)


def plain_up(lhs, weights, flip):
    rows, depth = lhs.shape
    width = weights[0].shape[0 if flip else 1]
    n = len(weights)
    bm, bn = 1024, 512 // n
    w_spec = pl.BlockSpec((bn, depth), lambda j, i: (j, 0)) if flip else pl.BlockSpec((depth, bn), lambda j, i: (0, j))
    return pl.pallas_call(
        functools.partial(plain_up_kernel, n, flip), grid=(width // bn, rows // bm), name="plain_up",
        in_specs=[pl.BlockSpec((bm, depth), lambda j, i: (i, 0))] + [w_spec] * n,
        out_specs=[pl.BlockSpec((bm, bn), lambda j, i: (i, j))] * n, out_shape=[jax.ShapeDtypeStruct((rows, width), F32)] * n,
        cost_estimate=pl.CostEstimate(flops=2 * n * rows * width * depth, bytes_accessed=4 * rows * depth, transcendentals=0),
        compiler_params=params_of("arbitrary", "arbitrary"),
    )(lhs, *weights)


def up_kernel(n_weights, n_parts, flip, lhs, *refs):
    parts = [refs[n_parts * w:n_parts * (w + 1)] for w in range(n_weights)]
    outs, held = refs[n_parts * n_weights:-1], refs[-1]
    outs, stored = outs[:n_weights], outs[n_weights:]
    me = lax.axis_index("cp")
    j = pl.program_id(1)
    cols = outs[0].shape[1]

    @pl.when(pl.program_id(0) == 0)
    def _():
        for w, part in enumerate(parts):
            mine = pl.ds(w * cols, cols)
            for q, ref in enumerate(part):
                depth = ref.shape[1] if flip else ref.shape[0]
                place = lax.rem(me * 2 + q, n_parts)
                at = pl.ds(pl.multiple_of(place * depth, depth), depth)
                val = ref[...].astype(BF16)
                if flip:
                    held[j, mine, at] = val
                else:
                    held[j, at, mine] = val
                stored[w][(slice(None), at) if flip else (at, slice(None))] = val

    res = lax.dot_general(lhs[...], held[j], CHAN if flip else ROW, preferred_element_type=F32)
    for w, out in enumerate(outs):
        out[...] = res[:, w * cols:(w + 1) * cols]


def up(lhs, weights, flip, n_rows):
    depth = lhs.shape[1]
    n, n_parts = len(weights), len(weights[0])
    width = weights[0][0][0].shape[-2 if flip else -1]
    bm, bn = 1024, 256 // n
    steps = width // bn

    def block(size, lead, of):
        shape = (bn, size) if flip else (size, bn)
        return pl.BlockSpec((None,) * len(lead) + shape, lambda i, j: lead + ((of(i, j), 0) if flip else (0, of(i, j))))

    def once(i, j):
        return jnp.where(i == 0, j, steps - 1)

    out_specs = [pl.BlockSpec((bm, bn), lambda i, j: (i, j))] * n
    out_shape = [jax.ShapeDtypeStruct((n_rows, width), F32)] * n
    out_specs += [block(depth, (), once)] * n
    out_shape += [jax.ShapeDtypeStruct((width, depth) if flip else (depth, width), BF16)] * n
    return pl.pallas_call(
        functools.partial(up_kernel, n, n_parts, flip), grid=(n_rows // bm, steps), name="up",
        in_specs=[pl.BlockSpec((bm, depth), lambda i, j: (i, 0))] + [block(depth // n_parts, lead, once) for part in weights for _, lead in part],
        out_specs=out_specs, out_shape=out_shape,
        scratch_shapes=[pltpu.VMEM((steps, n * bn, depth) if flip else (steps, depth, n * bn), BF16)],
        cost_estimate=pl.CostEstimate(flops=2 * n * n_rows * width * depth, bytes_accessed=4 * n_rows * depth, transcendentals=0),
        compiler_params=params_of("arbitrary", "arbitrary"),
    )(lhs, *[array for part in weights for array, _ in part])


def finish_rows(rows, first, dn_ref, x_ref, gz_ref, scale_ref, grad_ref, sum_ref):
    width = x_ref.shape[1]
    tiles = [pl.ds(n * LANES, LANES) for n in range(width // LANES)]
    here = pl.ds(pl.multiple_of(first, rows), rows)
    square = cross = jnp.zeros((rows, LANES), F32)
    for cols in tiles:
        x = x_ref[here, cols].astype(F32)
        square = square + x * x
        cross = cross + x * (dn_ref[here, cols] * scale_ref[:, cols])
    inv = lax.rsqrt(jnp.sum(square, axis=-1, keepdims=True) / width + NORM_EPS)
    inv_b = jnp.broadcast_to(inv, (rows, LANES))
    pull = jnp.broadcast_to(inv * inv * inv * (jnp.sum(cross, axis=-1, keepdims=True) / width), (rows, LANES))
    for cols in tiles:
        x = x_ref[here, cols].astype(F32)
        gz = gz_ref[here, cols].astype(F32)
        dn = dn_ref[here, cols] * inv_b
        grad_ref[here, cols] = (gz + dn * scale_ref[:, cols] - x * pull).astype(BF16)
        for which, val in enumerate((dn * x, gz)):
            sum_ref[which, :, cols] += sum(val[SUB * r:SUB * (r + 1)] for r in range(rows // SUB))


def z_kernel(n_pairs, n_moved, *refs):
    left, right = refs[:n_pairs], refs[n_pairs:2 * n_pairs]
    x_ref, bias_ref, *rows_in = refs[2 * n_pairs:2 * n_pairs + 6]
    moved, (out_ref, *rows_out), placed = refs[2 * n_pairs + 6:-3 - n_moved], refs[-3 - n_moved:len(refs) - n_moved], refs[len(refs) - n_moved:]
    for src, dst in zip(moved, placed):
        dst[...] = src[...]

    @pl.when(jnp.logical_and(pl.program_id(0) == 0, pl.program_id(1) == 0))
    def _():
        rows_out[-1][...] = jnp.zeros_like(rows_out[-1])

    acc = x_ref[...].astype(F32) + bias_ref[...]
    for lhs, rhs in zip(left, right):
        acc = acc + jnp.dot(lhs[...], rhs[...], preferred_element_type=F32)
    out_ref[...] = acc.astype(BF16)
    for first in range(0, rows_in[0].shape[0], UNIT):
        finish_rows(UNIT, first, *rows_in, *rows_out)


def outputs(left, right, x, bias, dn, gz, scale, moved):
    rows, width = dn.shape
    depth = left[0].shape[1]
    bm, bn = 1024, 512
    n_row, n_col = rows // bm, width // bn
    share = rows // (n_row * n_col)
    tile = pl.BlockSpec((bm, bn), lambda i, j: (i, j))
    line = pl.BlockSpec((share, width), lambda i, j: (i * n_col + j, 0))
    in_specs = [pl.BlockSpec((bm, depth), lambda i, j: (i, 0))] * len(left) + [pl.BlockSpec((depth, bn), lambda i, j: (0, j))] * len(right)
    in_specs += [tile, pl.BlockSpec((1, bn), lambda i, j: (0, j)), line, line, line, pl.BlockSpec((1, width), lambda i, j: (0, 0))]
    n_move = 16
    passing = [pl.BlockSpec((v.shape[0] // n_move, v.shape[1]), lambda i, j: (jnp.minimum(i * n_col + j, n_move - 1), 0)) for v in moved]
    return pl.pallas_call(
        functools.partial(z_kernel, len(left), len(moved)), grid=(n_row, n_col), name="outputs",
        in_specs=in_specs + passing, out_specs=[tile, line, pl.BlockSpec((2, SUB, width), lambda i, j: (0, 0, 0))] + passing,
        out_shape=[jax.ShapeDtypeStruct(x.shape, BF16)] * 2 + [jax.ShapeDtypeStruct((2, SUB, width), F32)] + [jax.ShapeDtypeStruct(v.shape, v.dtype) for v in moved],
        cost_estimate=pl.CostEstimate(flops=2 * len(right) * rows * width * depth, bytes_accessed=rows * width * 20, transcendentals=rows),
        compiler_params=params_of("arbitrary", "arbitrary"),
    )(*left, *right, x, bias, dn, x, gz, scale, *moved)


def tail_kernel(z_ref, bias_ref, dn_ref, x_ref, gz_ref, scale_ref, _, __, out_ref, grad_ref, sum_ref):
    @pl.when(pl.program_id(0) == 0)
    def _():
        sum_ref[...] = jnp.zeros_like(sum_ref)

    def unit(u, _):
        here = pl.ds(pl.multiple_of(u * UNIT, UNIT), UNIT)
        for n in range(out_ref.shape[1] // LANES):
            cols = pl.ds(n * LANES, LANES)
            out_ref[here, cols] = (x_ref[here, cols].astype(F32) + (z_ref[here, cols] + bias_ref[:, cols])).astype(BF16)
        finish_rows(UNIT, u * UNIT, dn_ref, x_ref, gz_ref, scale_ref, grad_ref, sum_ref)
        return 0

    lax.fori_loop(0, out_ref.shape[0] // UNIT, unit, 0)


def tail_outputs(z_sum, bias, dn, x, gz, scale, z, grad_x, first_row):
    rows, width = dn.shape
    share = 128
    skip = first_row // share
    near = pl.BlockSpec((share, width), lambda i: (i, 0))
    line = pl.BlockSpec((share, width), lambda i: (i + skip, 0))
    whole = pl.BlockSpec((1, width), lambda i: (0, 0))
    here = pl.BlockSpec(memory_space=pl.ANY)
    return pl.pallas_call(
        tail_kernel, grid=(rows // share,), name="tail_outputs",
        in_specs=[near, whole, near, line, line, whole, here, here], out_specs=[line, line, pl.BlockSpec((2, SUB, width), lambda i: (0, 0, 0))],
        out_shape=[jax.ShapeDtypeStruct(x.shape, BF16)] * 2 + [jax.ShapeDtypeStruct((2, SUB, width), F32)], input_output_aliases={6: 0, 7: 1},
        cost_estimate=pl.CostEstimate(flops=rows * width * 1500, bytes_accessed=rows * width * 16, transcendentals=rows),
        compiler_params=params_of("arbitrary"),
    )(z_sum, bias, dn, x, gz, scale, z, grad_x)


def wide_kernel(n_pairs, flip, *refs):
    left, right, out_ref = refs[:n_pairs], refs[n_pairs:2 * n_pairs], refs[2 * n_pairs]
    acc = 0.0
    for lhs, rhs in zip(left, right):
        acc = acc + lax.dot_general(lhs[...], rhs[...], CHAN if flip else ROW, preferred_element_type=F32)
    out_ref[...] = acc


def wide_product(lefts, rights, flip, first_row, rows):
    depth = lefts[0].shape[1]
    width = rights[0].shape[0 if flip else 1]
    bm, bn = 1024, 512
    skip = first_row // bm
    n = len(lefts)
    return pl.pallas_call(
        functools.partial(wide_kernel, n, flip), grid=(rows // bm, width // bn), name="wide_product",
        in_specs=[pl.BlockSpec((bm, depth), lambda i, j: (i + skip, 0))] * n + [pl.BlockSpec((bn, depth), lambda i, j: (j, 0)) if flip else pl.BlockSpec((depth, bn), lambda i, j: (0, j))] * n,
        out_specs=pl.BlockSpec((bm, bn), lambda i, j: (i, j)), out_shape=jax.ShapeDtypeStruct((rows, width), F32),
        cost_estimate=pl.CostEstimate(flops=2 * n * rows * width * depth, bytes_accessed=450000000, transcendentals=0),
        compiler_params=params_of("arbitrary", "arbitrary"),
    )(*lefts, *rights)


def token_product(lhs, rhs):
    return lax.dot_general(lhs, rhs, TOK, preferred_element_type=F32)


def spread_positions(seg_pos):
    n_seq, n_tok = seg_pos.shape
    pos = jnp.swapaxes(seg_pos.reshape(n_seq // SUB, SUB, n_tok), 1, 2).reshape(n_seq // SUB, n_tok * SUB, 1)
    return jnp.broadcast_to(pos, (n_seq // SUB, n_tok * SUB, LANES))


def stack_params(b_x, b_y, conv_w, conv_b, b_a, b_i, a_param):
    rows = [b_x, b_y, *conv_w, conv_b, -b_a, -b_i]
    rows = [row.astype(F32) for row in rows] + [-8.0 * jax.nn.softplus(a_param)]
    return jnp.concatenate([jnp.stack(rows), jnp.zeros((16 - len(rows), a_param.shape[0]), F32)], axis=0)


def block_body(x_in, grad_z, seg_pos, norm_scale, w_x, b_x, w_y, b_y, conv_w, conv_b, w_a, b_a, w_i, b_i, a_param, w_out, b_out):
    me = lax.axis_index("cp")
    n_seq, n_tok, d_model = x_in.shape
    n_rows = n_seq * n_tok
    width = a_param.shape[0]
    x = x_in.reshape(n_rows, d_model)
    gz = grad_z.reshape(n_rows, d_model)
    scale = norm_scale.astype(F32).reshape(1, d_model)

    def swap_x(v):
        return lax.ppermute(v, "tp", [(j, j ^ 1) for j in range(4)])

    def swap_y(v):
        return lax.ppermute(v, "tp", [(j, j ^ 2) for j in range(4)])

    def swap_core(v):
        return lax.ppermute(v, "cp", [(0, 1), (1, 0)])

    tile = SUB * n_tok
    shared = n_rows - tile

    par = stack_params(b_x, b_y, conv_w, conv_b, b_a, b_i, a_param)
    w_gate = jnp.concatenate([w_a, w_i], axis=2)
    small = jnp.concatenate([par.reshape(-1), w_gate.astype(F32).reshape(-1)]).reshape(-1, LANES)

    def after(values, *before):
        return lax.optimization_barrier((values, before))[0]

    def quarter(w, axis, q):
        size = d_model // 4
        return lax.dynamic_slice_in_dim(w, (me * 2 + q) * size, size, axis).astype(F32)

    def to_neighbours(weights, axis, before):
        weights = after(weights, before)
        sent = [jnp.stack([quarter(w, axis, q) for w in weights]) for q in range(2)]
        return [swap_x(v) for v in sent], [swap_y(v) for v in sent]

    def cores(values):
        return values, [swap_core(v) for v in values]

    group_a = to_neighbours((w_x, w_y), 0, seg_pos)

    def unpack(s):
        flat = s.reshape(-1)
        return flat[:par.size].reshape(par.shape), lax.optimization_barrier(flat[par.size:]).reshape(w_gate.shape).astype(BF16)

    def onward(group):
        return [swap_y(group[0][0]), swap_x(group[1][1])]

    def quarters(side, n):
        own, other = side
        return [tuple((v, (k,)) for v in list(own) + list(other)) for k in range(n)]

    normed = normalize(x, 1.0 + scale)
    pos_rep = spread_positions(seg_pos)
    px, py = plain_up(normed, [w_x, w_y], False)
    group_b = to_neighbours((w_out,), 1, px)
    smalls = [lax.ppermute(after(small, px), "tp", [(j, j ^ far) for j in range(4)]) for far in range(1, 4)]
    dm, = plain_up(after(gz, px), [w_out], True)
    mixed, dpy, dbr, g_gate, s_y, s_b = middle(px, py, dm, pos_rep, par, w_gate, True, 0)
    g_w_out = token_product(mixed, gz)
    g_w_y = token_product(normed, dpy)
    group_a = after(group_a, g_w_out, g_w_y)
    side_x, side_y = [cores(values) for values in group_a]
    g_w_x = token_product(normed, after(dbr, g_w_y))
    diag_a = onward(after(group_a, g_w_x))

    s_y = jnp.sum(s_y, axis=1).reshape(1, width)
    s_b = jnp.swapaxes(jnp.sum(s_b.reshape(s_b.shape[0], N_SUMS, SUB, LANES), axis=2), 0, 1).reshape(N_SUMS, width)
    own_grads = lax.psum((g_w_x, g_w_y, g_w_out, g_gate), "cp")

    px_x, py_x, wx_x, wy_x = up(after(normed, g_w_x), quarters(side_x, 2), False, shared)
    px_y, py_y, wx_y, wy_y = up(after(normed, px_x), quarters(side_y, 2), False, shared)
    group_b = after(group_b, px_y)
    out_x, out_y = [cores(values) for values in group_b]
    diag_b = onward(group_b)
    dn_tail = wide_product(after([dbr, dpy], px_y), [w_x, w_y], True, shared, tile)
    smalls = after(smalls, dn_tail)
    dm_x, wo_x = up(after(gz, dn_tail), quarters(out_x, 1), True, shared)
    mixed_x, dpy_x, dbr_x = middle(px_x, py_x, dm_x, pos_rep, *unpack(smalls[0]), False, 1)
    dm_y, wo_y = up(after(gz, mixed_x), quarters(out_y, 1), True, shared)
    mixed_y, dpy_y, dbr_y = middle(px_y, py_y, dm_y, pos_rep, *unpack(smalls[1]), False, 1)
    diag_a, diag_b = after((diag_a, diag_b), mixed_y)
    diag_a, diag_b = cores(diag_a), cores(diag_b)
    z_tail = wide_product(after([mixed], mixed_y), [w_out], False, shared, tile)
    dn_sum, z_sum = lax.psum((dn_tail, z_tail), "tp")
    px_d, py_d, wx_d, wy_d = up(after(normed, z_tail), quarters(diag_a, 2), False, shared)
    dm_d, wo_d = up(after(gz, px_d), quarters(diag_b, 1), True, shared)
    mixed_d, dpy_d, dbr_d = middle(px_d, py_d, dm_d, pos_rep, *unpack(smalls[2]), False, 1)

    wx_all, wy_all, wo_all = [w_x, wx_x, wx_y, wx_d], [w_y, wy_x, wy_y, wy_d], [w_out, wo_x, wo_y, wo_d]
    dn = wide_product([dbr, dbr_x, dbr_y, dbr_d, dpy, dpy_x, dpy_y, dpy_d], wx_all + wy_all, True, 0, shared)
    bias = b_out.astype(F32).reshape(1, d_model)
    *tall, g_gate = own_grads
    lines = lax.psum(after(jnp.concatenate([s_y, s_b]), mixed_d), "cp")
    z_out, grad_x, sums_x, *tall = outputs([mixed, mixed_x, mixed_y, mixed_d], wo_all, x, bias, after(dn, lines), gz, 1.0 + scale, tall)
    g_w_x, g_w_y, g_w_out = tall
    z_out, grad_x, sums_t = tail_outputs(z_sum, bias, dn_sum, x, gz, 1.0 + scale, z_out, grad_x, shared)
    z_out = z_out.reshape(x_in.shape)
    sums_x = jnp.sum(sums_x + sums_t, axis=1)

    sums_x = lax.psum(sums_x, "cp")
    s_y, s_b = lines[0], lines[1:]
    g_a = -8.0 * s_b[8] * jax.nn.sigmoid(a_param)
    return (z_out, grad_x.reshape(x_in.shape), sums_x[0], g_w_x, s_b[0], g_w_y, s_y, s_b[1:5], s_b[5], g_gate[:, :, :LANES], s_b[6], g_gate[:, :, LANES:], s_b[7], g_a, g_w_out, sums_x[1])


def solution(mesh):
    return jax.shard_map(block_body, mesh=mesh, in_specs=IN_SPECS, out_specs=OUT_SPECS, check_vma=False)
```
